128 devices in a mesh: lat: 8 (over x, core), lon: 16 (over y, z).
Axes of the slice: x: 4, y: 4, z: 4, core: 2. Of those that a mesh axis runs over, the one named last changes fastest.
Arguments:
- spectra: bfloat16 [393216, 616], P(('lat', 'lon')), may hold values from -6 to 6
- block_target: int32 [3072], P(('lat', 'lon')), may hold values from 0 to 15, as said below
- block_patch: int32 [3072], P(('lat', 'lon')), may hold values from 0 to 11
- block_kernel: int32 [3072], P(('lat', 'lon')), may hold values from 0 to 15
- encoder_weight: bfloat16 [616, 512], replicated, may hold values from -0.25 to 0.25
- kernels: bfloat16 [16, 128, 128], replicated, may hold values from 0.049804688 to 1
- gain: float32 [512], replicated, may hold values from 0.1 to 1.9
- conv_weight: bfloat16 [3, 3, 512, 512], replicated, may hold values from -0.09375 to 0.09375
- cotangent: bfloat16 [192, 1024, 512], P('lat', 'lon'), may hold values from -6 to 6
Outputs:
- conv_out: bfloat16 [192, 1024, 512], P('lat', 'lon')
- conv_grad: float32 [3, 3, 512, 512], replicated
- encoder_grad: float32 [616, 512], replicated
- gain_grad: float32 [512], replicated
The draws below stay inside these ranges and needn't reach their ends.
Inputs may be any that keep to these rules, and one draw needn't show every extreme that they name: `block_target`: within one device's 24 blocks no tile is named more than 3 times; in every latitude band one tile is named exactly 3 times by every device of the band.
All inputs are finite; a program needn't handle non-finite values.
Results may differ from the reference program's by a relative error of at most 0.0059.
Values may be sent and summed in bfloat16 or wider, within the bound.
A program may use at most 192 MiB of HBM per device.

```python
import math
import jax
import jax.numpy as jnp
from jax import lax

CH = 616
D = 512
BLK = 128
PH = 8
PW = 16
NKER = 16
BLOCKS = 24
TH = 24
TW = 64
MOST = 3
NOBS = 393216
NBLK = 3072
NLAT = 192
NLON = 1024
PATCH = 128
PATCHES = 12
N_LAT = 8
N_LON = 16


def draw_block_target(key, part):
    other_slots = (N_LON - 1) * MOST
    spare_blocks = BLOCKS - MOST

    def one_device(device):
        lat_band = device // N_LON
        hot_key = jax.random.fold_in(jax.random.fold_in(key, 101), lat_band)
        hottest = jax.random.randint(hot_key, (), 0, N_LON)
        own_key = jax.random.fold_in(jax.random.fold_in(key, 202), device)
        first_key, second_key = jax.random.split(own_key)
        others = (hottest + 1 + jnp.arange(other_slots) // MOST) % N_LON
        scores = jax.random.permutation(first_key, other_slots)
        _, chosen = lax.top_k(scores, spare_blocks)
        targets = jnp.concatenate([jnp.full((MOST,), hottest, jnp.int32), others[chosen].astype(jnp.int32)])
        return targets[jax.random.permutation(second_key, BLOCKS)]
    return jax.vmap(one_device)(jnp.arange(NBLK // BLOCKS)).reshape(-1).astype(jnp.int32)


def with_ends(values, key, smallest, largest):
    shape = values.shape
    index_at = [jax.random.randint(jax.random.fold_in(key, axis), (), 0, shape[axis]) for axis in range(len(shape))]
    values = values.at[tuple(index_at)].set(smallest)
    longest = shape.index(max(shape))
    index_at[longest] = (index_at[longest] + 1) % shape[longest]
    return values.at[tuple(index_at)].set(largest)


def block_levels(key, shape, cuts, smallest, top_value):
    level = 1.0
    for position, parts in cuts:
        heights = jax.random.uniform(jax.random.fold_in(jax.random.fold_in(key, 6), position), (parts,), jnp.float32, smallest / len(cuts), top_value / len(cuts))
        level = level * jnp.repeat(jnp.exp(heights), shape[position] // parts).reshape((-1,) + (1,) * (len(shape) - 1 - position))
    return level


def gaussian(key, extent, width, limit, pieces=(), held_as=jnp.bfloat16):
    values = jax.random.normal(key, extent, jnp.float32) * width
    if len(pieces) > 0:
        values = block_levels(key, extent, pieces, -0.22, 0.18) * values
    return jnp.clip(values, min=-limit, max=limit).astype(held_as)


def setup_inputs(seed: int = 0) -> dict:
    seeds = jax.random.split(jax.random.key(seed), 10)
    return {
        "spectra": gaussian(seeds[0], (NOBS, CH), 1.0, 6.0, ((0, 128),)),
        "block_target": draw_block_target(jax.random.fold_in(seeds[9], 71), 0),
        "block_patch": with_ends(jax.random.randint(seeds[2], (NBLK,), 0, PATCHES), jax.random.fold_in(seeds[2], 1), 0, PATCHES - 1).astype(jnp.int32),
        "block_kernel": with_ends(jax.random.randint(seeds[3], (NBLK,), 0, NKER), jax.random.fold_in(seeds[3], 1), 0, NKER - 1).astype(jnp.int32),
        "encoder_weight": gaussian(seeds[4], (CH, D), CH ** -0.5, 0.25),
        "kernels": jnp.clip(jax.random.uniform(seeds[5], (NKER, BLK, PATCH), jnp.float32, 0.049804688, 1.0), 0.049804688, 1.0).astype(jnp.bfloat16),
        "gain": jnp.clip(1.0 + 0.18 * jax.random.normal(seeds[6], (D,), jnp.float32), 0.1, 1.9),
        "conv_weight": gaussian(seeds[7], (3, 3, D, D), (9 * D) ** -0.5, 0.09375),
        "cotangent": gaussian(seeds[8], (NLAT, NLON, D), 1.0, 6.0, ((0, 8), (1, 16))),
    }


def normalise(field, gain):
    meansq = lax.optimization_barrier(jnp.mean(field * field, axis=-1, keepdims=True))
    return field * lax.rsqrt(meansq + 1e-06) * gain

def silu_slope(preact):
    logistic = jax.nn.sigmoid(preact)
    return logistic * (1.0 + preact * (1.0 - logistic))

def widen_global(field):
    beside_all = jnp.concatenate([field[:, -1:], field, field[:, :1]], axis=1)
    return jnp.pad(beside_all, ((1, 1), (0, 0), (0, 0)))

def reference(spectra, block_target, block_patch, block_kernel, encoder_weight, kernels, gain, conv_weight, cotangent):
    block_count = block_target.shape[0]
    preact = jnp.dot(spectra, encoder_weight, preferred_element_type=jnp.float32)
    encoded = jax.nn.silu(preact).astype(jnp.bfloat16).reshape(block_count, BLK, D)
    block_kernels = kernels[block_kernel]
    contribution = jnp.einsum('nbp,nbd->npd', block_kernels.astype(jnp.float32), encoded.astype(jnp.float32))
    owner_device = jnp.arange(block_count, dtype=jnp.int32) // BLOCKS
    lat_band = owner_device // N_LON
    patch_ids = ((lat_band * N_LON + block_target) * PATCHES + block_patch).astype(jnp.int32)
    grid_patches = jnp.zeros((N_LAT * N_LON * PATCHES, PATCH, D), jnp.float32).at[patch_ids].add(contribution)
    spread = grid_patches.reshape(N_LAT, N_LON, TH // PH, TW // PW, PH, PW, D)
    spread = spread.transpose(0, 2, 4, 1, 3, 5, 6).reshape(NLAT, NLON, D)
    normed = normalise(spread, gain).astype(jnp.bfloat16)
    padded = widen_global(normed)
    result_sum = jnp.zeros((NLAT * NLON, D), jnp.float32)
    for row_shift in range(3):
        for col_shift in range(3):
            window = padded[row_shift:row_shift + NLAT, col_shift:col_shift + NLON].reshape(-1, D)
            result_sum = result_sum + jnp.dot(window, conv_weight[row_shift, col_shift], preferred_element_type=jnp.float32)
    conv_out = result_sum.reshape(NLAT, NLON, D).astype(jnp.bfloat16)
    loss_scale = 1.0 / math.sqrt(NLAT * NLON)
    cot_padded = widen_global(cotangent)
    cot_flat = cotangent.reshape(-1, D)
    d_normed = jnp.zeros((NLAT * NLON, D), jnp.float32)
    kernel_grads = []
    for row_shift in range(3):
        for col_shift in range(3):
            back_window = cot_padded[2 - row_shift:2 - row_shift + NLAT, 2 - col_shift:2 - col_shift + NLON].reshape(-1, D)
            d_normed = d_normed + lax.dot_general(back_window, conv_weight[row_shift, col_shift], (((1,), (1,)), ((), ())), preferred_element_type=jnp.float32)
            window = padded[row_shift:row_shift + NLAT, col_shift:col_shift + NLON].reshape(-1, D)
            kernel_grads.append(lax.dot_general(window, cot_flat, (((0,), (0,)), ((), ())), preferred_element_type=jnp.float32))
    conv_grad = jnp.stack(kernel_grads).reshape(3, 3, D, D) * loss_scale
    _, pullback = jax.vjp(normalise, spread, gain)
    d_spread, gain_part = pullback(d_normed.reshape(NLAT, NLON, D))
    gain_grad = gain_part * loss_scale
    d_spread = d_spread.astype(jnp.bfloat16)
    d_patches = d_spread.reshape(N_LAT, TH // PH, PH, N_LON, TW // PW, PW, D)
    d_patches = d_patches.transpose(0, 3, 1, 4, 2, 5, 6).reshape(-1, PATCH, D)
    block_dpatch = d_patches[patch_ids]
    d_rows = jnp.einsum('nbp,npd->nbd', block_kernels.astype(jnp.float32), block_dpatch.astype(jnp.float32)).astype(jnp.bfloat16)
    d_preact = (d_rows.reshape(-1, D).astype(jnp.float32) * silu_slope(preact)).astype(jnp.bfloat16)
    encoder_grad = lax.dot_general(spectra, d_preact, (((0,), (0,)), ((), ())), preferred_element_type=jnp.float32) * loss_scale
    return (conv_out, conv_grad, encoder_grad, gain_grad)
```

```python
import math

import jax
import jax.numpy as jnp
from jax import lax
from jax.experimental import pallas as pl
from jax.experimental.pallas import tpu as pltpu
from jax.sharding import PartitionSpec as P

PH = 8
PW = 16
MOST = 3
SIDE = 4
MESH = pl.DeviceIdType.MESH
VMEM_LIMIT = 60 * 1024 * 1024


def dot(a, b, ca, cb):
    return lax.dot_general(a, b, (((ca,), (cb,)), ((), ())), preferred_element_type=jnp.float32)


def pack_kernel(source_ref, spectra, to_a, to_b, held, blank, in_sem, out_sems):
    slots = source_ref.shape[0]
    rows = held.shape[1] // 2
    fetch = pltpu.make_async_copy(spectra, held, in_sem)
    fetch.start()
    blank[...] = jnp.zeros_like(blank)
    fetch.wait()

    def pieces(slot, source):
        tile = slot // MOST
        rank = slot - tile * MOST
        y, z = tile // SIDE, tile % SIDE
        return (
            pltpu.make_async_copy(source(0), to_a.at[z, y, rank], out_sems.at[slot, 0]),
            pltpu.make_async_copy(source(1), to_b.at[y, z, rank], out_sems.at[slot, 1]),
        )

    @pl.loop(0, slots)
    def _(slot):
        block = source_ref[slot]

        @pl.when(block >= 0)
        def _():
            for piece in pieces(slot, lambda half: held.at[block, pl.ds(half * rows, rows)]):
                piece.start()

        @pl.when(block < 0)
        def _():
            for piece in pieces(slot, lambda half: blank):
                piece.start()

    @pl.loop(0, slots)
    def _(slot):
        for piece in pieces(slot, lambda half: blank):
            piece.wait()


def pack(source_block, spectra, block_rows):
    blocks = spectra.shape[0] // block_rows
    channels = spectra.shape[1]
    half = block_rows // 2
    slots = source_block.shape[0]
    out = jax.ShapeDtypeStruct((SIDE, SIDE, MOST, half, channels), jnp.bfloat16)
    return pl.pallas_call(
        pack_kernel,
        name="pack",
        out_shape=(out, out),
        in_specs=[pl.BlockSpec(memory_space=pltpu.SMEM), pl.BlockSpec(memory_space=pl.ANY)],
        out_specs=(pl.BlockSpec(memory_space=pl.ANY),) * 2,
        scratch_shapes=[
            pltpu.VMEM((blocks, block_rows, channels), jnp.bfloat16),
            pltpu.VMEM((half, channels), jnp.bfloat16),
            pltpu.SemaphoreType.DMA,
            pltpu.SemaphoreType.DMA((slots, 2)),
        ],
        compiler_params=pltpu.CompilerParams(vmem_limit_bytes=VMEM_LIMIT),
    )(source_block, spectra.reshape(blocks, block_rows, channels))


def position():
    lat, lon = lax.axis_index("lat"), lax.axis_index("lon")
    return lat, lon, lon // SIDE, lon % SIDE


def halo_peers():
    lat, lon = lax.axis_index("lat"), lax.axis_index("lon")
    lats, lons = lax.axis_size("lat"), lax.axis_size("lon")
    up, down = (lat + lats - 1) % lats, (lat + 1) % lats
    left, right = (lon + lons - 1) % lons, (lon + 1) % lons
    return lat, lon, up, down, left, right


def halo_copies(top, bottom, first, last, from_above, from_below, from_left, from_right, sends, recvs):
    lat, lon, up, down, left, right = halo_peers()
    rows = first.shape[0]
    body = pl.ds(1, rows)
    plan = [
        (top, from_below, (up, lon)),
        (bottom, from_above, (down, lon)),
        (last, from_left.at[body], (lat, right)),
        (first, from_right.at[body], (lat, left)),
        (last.at[0], from_left.at[rows + 1], (up, right)),
        (last.at[rows - 1], from_left.at[0], (down, right)),
        (first.at[0], from_right.at[rows + 1], (up, left)),
        (first.at[rows - 1], from_right.at[0], (down, left)),
    ]
    return [
        pltpu.make_async_remote_copy(
            src_ref=src, dst_ref=dst, send_sem=sends.at[n], recv_sem=recvs.at[n], device_id=to, device_id_type=MESH
        )
        for n, (src, dst, to) in enumerate(plan)
    ]


def lay_windows(tile, from_above, from_below, from_left, from_right, wide, reverse):
    lat, lats = lax.axis_index("lat"), lax.axis_size("lat")
    rows, cols, width = tile.shape
    index = lax.broadcasted_iota(jnp.int32, (cols, width), 0)

    def lay(at, center, keep):
        value = center.astype(jnp.float32)
        before = jnp.where(index == 0, from_left[at], pltpu.roll(value, 1, 0))
        after = jnp.where(index == cols - 1, from_right[at], pltpu.roll(value, cols - 1, 0))
        if keep is not None:
            before, value, after = (jnp.where(keep, v, 0.0) for v in (before, value, after))
        order = (after, value, before) if reverse else (before, value, after)
        for n, v in enumerate(order):
            wide[at, :, n * width : (n + 1) * width] = v.astype(jnp.bfloat16)

    @pl.loop(0, rows)
    def _(row):
        lay(row + 1, tile[row], None)

    lay(0, from_above[...], lat > 0)
    lay(rows + 1, from_below[...], lat < lats - 1)


def exchange_kernel(
    send_a, send_b, meta, cot, first, last, weight,
    got_a, got_b, got_meta, wide_out, back_out, mid_a, mid_b, relay_a, relay_b,
    tile, wide, held_weight, back, above, below, lefts, rights,
    halo_send, halo_recv, meta_send, meta_recv, sends, recvs, local,
):
    lat, lon, y, z = position()
    lats = lax.axis_size("lat")
    count = lax.axis_size("lon")
    _, _, up, down, left, right = halo_peers()
    rows, cols, width = tile.shape

    barrier = pltpu.get_barrier_semaphore()
    for step in range(1, SIDE * SIDE):
        peer = (lon + step) % count
        pl.semaphore_signal(barrier, inc=1, device_id=(lat, peer), device_id_type=MESH)
    for other in (up, down):
        for peer in (left, lon, right):
            pl.semaphore_signal(barrier, inc=1, device_id=(other, peer), device_id_type=MESH)
    load_tile = pltpu.make_async_copy(cot, tile, local.at[0])
    load_weight = pltpu.make_async_copy(weight, held_weight, local.at[1])
    load_tile.start()
    load_weight.start()
    own_meta = pltpu.make_async_copy(meta.at[lon], got_meta.at[0], local.at[2])
    own_meta.start()
    pl.semaphore_wait(barrier, SIDE * SIDE - 1 + 6)

    halo = halo_copies(
        cot.at[0], cot.at[rows - 1], first, last, above, below, lefts, rights, halo_send, halo_recv
    )
    for copy in halo:
        copy.start()
    notes = []
    for dy in range(SIDE):
        for dz in range(SIDE):
            if dy or dz:
                n = dy * SIDE + dz
                to = (y + dy) % SIDE * SIDE + (z + dz) % SIDE
                notes.append(
                    pltpu.make_async_remote_copy(
                        src_ref=meta.at[to], dst_ref=got_meta.at[n], send_sem=meta_send.at[n],
                        recv_sem=meta_recv.at[n], device_id=(lat, to), device_id_type=MESH,
                    )
                )
    for copy in notes:
        copy.start()

    flows = []
    for flow, (src, mid, relay, got, u, v) in enumerate(
        ((send_a, mid_a, relay_a, got_a, z, y), (send_b, mid_b, relay_b, got_b, y, z))
    ):
        made = []

        def make(src_ref, dst_ref, du, dv, flow=flow, made=made, u=u, v=v):
            n = len(made)
            uu, vv = (u + du) % SIDE, (v + dv) % SIDE
            to = vv * SIDE + uu if flow == 0 else uu * SIDE + vv
            copy = pltpu.make_async_remote_copy(
                src_ref=src_ref, dst_ref=dst_ref, send_sem=sends.at[flow, n], recv_sem=recvs.at[flow, n],
                device_id=(lat, to), device_id_type=MESH,
            )
            made.append(copy)
            return copy

        def land(g, e, mid=mid, got=got):
            return got.at[0, e] if g == 0 else mid.at[g, e]

        def part(g, e, src=src, mid=mid, u=u, v=v):
            return src.at[u, (v + g) % SIDE] if e == 0 else mid.at[g, e]

        f = {"made": made}
        for d, sign in ((0, 1), (1, -1)):
            for j in range(2):
                g = 2 * d + j
                f["q1", d, j] = make(src.at[(u + 2) % SIDE, (v + g) % SIDE], relay.at[0, d, j], sign, 0)
                f["r1", d, j] = make(relay.at[0, d, j], land(g, 2), sign, 0)
            for g in range(SIDE):
                f["d1", d, g] = make(src.at[(u + sign) % SIDE, (v + g) % SIDE], land(g, 1 if d == 0 else 3), sign, 0)
            for e in range(SIDE):
                g = 1 if d == 0 else 3
                f["d2", d, e] = make(part(g, e), got.at[g, e], 0, sign)
            for j in range(2):
                e = ((0, 1), (3, 2))[d][j]
                f["q2", d, j] = make(part(2, e), relay.at[1, d, j], 0, sign)
                f["r2", d, j] = make(relay.at[1, d, j], got.at[2, e], 0, sign)
        flows.append(f)

    def start(*keys):
        for key in keys:
            for f in flows:
                f[key].start()

    def arrived(*keys):
        for key in keys:
            for f in flows:
                f[key].wait_recv()

    start(("q1", 0, 1), ("q1", 1, 0), ("q1", 0, 0), ("q1", 1, 1))
    for g in (2, 1, 3, 0):
        start(("d1", 0, g), ("d1", 1, g))

    load_tile.wait()
    for copy in halo:
        copy.wait()
    lay_windows(tile, above, below, lefts, rights, wide, True)
    save_wide = pltpu.make_async_copy(wide, wide_out, local.at[3])
    save_wide.start()
    load_weight.wait()
    step_rows = 4

    @pl.loop(0, rows // step_rows)
    def _(chunk):
        total = jnp.zeros((step_rows * cols, width), jnp.float32)
        for a in range(3):
            for b in range(3):
                window = wide[pl.ds(chunk * step_rows + 2 - a, step_rows), :, b * width : (b + 1) * width]
                total += dot(window.reshape(step_rows * cols, width), held_weight[a * 3 + b], 1, 1)
        back[pl.ds(chunk * step_rows, step_rows)] = total.reshape(step_rows, cols, width)

    save_back = pltpu.make_async_copy(back, back_out, local.at[4])
    save_back.start()

    for d, j in ((0, 1), (1, 0), (0, 0), (1, 1)):
        arrived(("q1", d, j))
        start(("r1", d, j))
    start(("q2", 0, 0), ("d2", 0, 0), ("d2", 1, 0))
    for g in (2, 1, 3, 0):
        arrived(("d1", 0, g), ("d1", 1, g))
        if g == 2:
            start(("q2", 0, 1), ("q2", 1, 0))
        if g == 1:
            start(("d2", 0, 1), ("d2", 0, 3))
        if g == 3:
            start(("d2", 1, 1), ("d2", 1, 3))
    arrived(("r1", 1, 0))
    start(("q2", 1, 1))
    arrived(("r1", 0, 1), ("r1", 1, 1))
    arrived(("q2", 0, 0))
    start(("r2", 0, 0))
    arrived(("q2", 0, 1), ("q2", 1, 0))
    start(("r2", 0, 1), ("r2", 1, 0))
    start(("d2", 0, 2), ("d2", 1, 2))
    arrived(("q2", 1, 1))
    start(("r2", 1, 1))
    arrived(("r1", 0, 0))
    for d in range(2):
        arrived(*(("d2", d, e) for e in range(SIDE)))
        arrived(("r2", d, 0), ("r2", d, 1))
    for f in flows:
        for copy in f["made"]:
            copy.wait_send()
    for copy in notes:
        copy.wait()
    own_meta.wait()
    save_wide.wait()
    save_back.wait()


def exchange(send_a, send_b, meta, cotangent, first, last, weight):
    rows, cols, width = cotangent.shape
    slot = send_a.shape[2:]
    lon = SIDE * SIDE
    bf, f32 = jnp.bfloat16, jnp.float32
    anywhere = pl.BlockSpec(memory_space=pl.ANY)
    whole = jax.ShapeDtypeStruct((SIDE, SIDE) + slot, bf)
    relay = jax.ShapeDtypeStruct((2, 2, 2) + slot, bf)
    out = pl.pallas_call(
        exchange_kernel,
        name="exchange",
        out_shape=(
            whole, whole, jax.ShapeDtypeStruct(meta.shape, meta.dtype),
            jax.ShapeDtypeStruct((rows + 2, cols, 3 * width), bf), jax.ShapeDtypeStruct((rows, cols, width), f32),
            whole, whole, relay, relay,
        ),
        in_specs=[anywhere] * 7,
        out_specs=(anywhere,) * 9,
        scratch_shapes=[
            pltpu.VMEM((rows, cols, width), bf),
            pltpu.VMEM((rows + 2, cols, 3 * width), bf),
            pltpu.VMEM(weight.shape, bf),
            pltpu.VMEM((rows, cols, width), f32),
            pltpu.VMEM((cols, width), bf),
            pltpu.VMEM((cols, width), bf),
            pltpu.VMEM((rows + 2, 1, width), f32),
            pltpu.VMEM((rows + 2, 1, width), f32),
            pltpu.SemaphoreType.DMA((8,)),
            pltpu.SemaphoreType.DMA((8,)),
            pltpu.SemaphoreType.DMA((lon,)),
            pltpu.SemaphoreType.DMA((lon,)),
            pltpu.SemaphoreType.DMA((2, 32)),
            pltpu.SemaphoreType.DMA((2, 32)),
            pltpu.SemaphoreType.DMA((5,)),
        ],
        compiler_params=pltpu.CompilerParams(
            collective_id=0, has_side_effects=True, vmem_limit_bytes=VMEM_LIMIT
        ),
    )(send_a, send_b, meta, cotangent, first, last, weight)
    return out[:5]


def middle_kernel(
    meta, own_a, own_b, got_a, got_b, encoder, kernels, turned, gain, wide_in, back_in,
    normed, parts,
    x, slope, encoded, spread, d_spread, wide, back, flipped, d_rows, encoder_sum, gain_sum,
    x_sems, local,
):
    lat, lon, y, z = position()
    rows, cols, width = normed.shape
    channels = encoder.shape[0]
    sources = SIDE * SIDE
    block = kernels.shape[1]
    copies = []
    for n in range(sources):
        dy, dz = n // SIDE, n % SIDE
        from_a = own_a.at[z, y] if n == 0 else got_a.at[dy, dz]
        from_b = own_b.at[y, z] if n == 0 else got_b.at[dz, dy]
        copies.append(pltpu.make_async_copy(from_a, x.at[n, :, 0], x_sems.at[n, 0]))
        copies.append(pltpu.make_async_copy(from_b, x.at[n, :, 1], x_sems.at[n, 1]))
    for copy in copies:
        copy.start()
    load_back = pltpu.make_async_copy(back_in, back, local.at[0])
    load_wide = pltpu.make_async_copy(wide_in, wide, local.at[1])
    load_back.start()
    load_wide.start()
    spread[...] = jnp.zeros_like(spread)

    @pl.loop(0, sources)
    def _(n):
        for half in range(2):
            pltpu.make_async_copy(got_a.at[0, 0], x.at[n, :, half], x_sems.at[n, half]).wait()
        pre = dot(x[n].reshape(MOST * block, channels), encoder[...], 1, 0)
        logistic = 0.5 * jnp.tanh(0.5 * pre) + 0.5
        encoded[...] = (pre * logistic).astype(jnp.bfloat16)
        slope[n] = (logistic * (1.0 + pre * (1.0 - logistic))).astype(jnp.bfloat16)
        for rank in range(MOST):
            which, patch = meta[n, rank], meta[n, MOST + rank]

            @pl.when(which >= 0)
            def _():
                spread[patch] += dot(turned[which], encoded[rank * block : (rank + 1) * block], 1, 0)

    load_back.wait()
    gain_sum[...] = jnp.zeros_like(gain_sum)
    across = cols // PW

    @pl.loop(0, spread.shape[0])
    def _(q):
        at = (pl.ds(q // across * PH, PH), pl.ds(pl.multiple_of(q % across * PW, PW), PW))
        value = spread[q]
        scale = lax.rsqrt(jnp.mean(value * value, axis=1, keepdims=True) + 1e-06)
        unit = value * scale
        weight = gain[...]
        normed[at] = (unit * weight).astype(jnp.bfloat16).reshape(PH, PW, width)
        given = back[at].reshape(PH * PW, width)
        product = given * unit
        gain_sum[...] += jnp.sum(product.reshape(PH * PW // 8, 8, width), axis=0)
        inner = jnp.mean(product * weight, axis=1, keepdims=True)
        d_spread[q] = (scale * (given * weight - unit * inner)).astype(jnp.bfloat16)

    step_rows = 4

    @pl.loop(0, rows // step_rows)
    def _(n):
        some = normed[pl.ds(n * step_rows, step_rows)].reshape(step_rows * cols, width)
        flipped[:, pl.ds(pl.multiple_of(n * step_rows * cols, 128), step_rows * cols)] = some.T

    load_wide.wait()
    for a in range(3):

        @pl.loop(0, 3 * width // 256)
        def _(j):
            window = wide[2 - a : 2 - a + rows, :, pl.ds(pl.multiple_of(j * 256, 256), 256)]
            got = dot(flipped[...], window.reshape(rows * cols, 256), 1, 0).astype(jnp.bfloat16)
            base = pl.multiple_of((a * (3 * width // 128) + 2 * j) * width, width)
            parts[pl.ds(base, width)] = got[:, :128]
            parts[pl.ds(pl.multiple_of(base + width, width), width)] = got[:, 128:]

    encoder_sum[...] = jnp.zeros_like(encoder_sum)

    @pl.loop(0, sources)
    def _(n):
        for rank in range(MOST):
            which, patch = jnp.maximum(meta[n, rank], 0), meta[n, MOST + rank]
            at = slice(rank * block, (rank + 1) * block)
            here = dot(kernels[which], d_spread[patch], 1, 0).astype(jnp.bfloat16).astype(jnp.float32)
            d_rows[at] = (here * slope[n, at].astype(jnp.float32)).astype(jnp.bfloat16)
        encoder_sum[...] += dot(x[n].reshape(MOST * block, channels), d_rows[...], 0, 0)

    base = 9 * width * width // 128
    for n in range(width // 128):
        lanes = slice(n * 128, (n + 1) * 128)
        parts[base + n * channels : base + (n + 1) * channels] = encoder_sum[:, lanes].astype(jnp.bfloat16)
    base += channels * width // 128
    for n in range(width // 128):
        parts[base + n * 8 : base + (n + 1) * 8] = gain_sum[:, n * 128 : (n + 1) * 128].astype(jnp.bfloat16)
    base += 8 * width // 128
    parts[base:] = jnp.zeros((parts.shape[0] - base, 128), jnp.bfloat16)


def middle(meta, own_a, own_b, got_a, got_b, encoder, kernels, gain, wide, back, part_rows):
    rows, cols, width = back.shape
    channels = encoder.shape[0]
    block, cells = kernels.shape[1:]
    patches = rows * cols // cells
    sources = SIDE * SIDE
    bf, f32 = jnp.bfloat16, jnp.float32
    anywhere = pl.BlockSpec(memory_space=pl.ANY)
    local = pl.BlockSpec(memory_space=pltpu.VMEM)
    return pl.pallas_call(
        middle_kernel,
        name="middle",
        out_shape=(jax.ShapeDtypeStruct((rows, cols, width), bf), jax.ShapeDtypeStruct((part_rows, 128), bf)),
        in_specs=[pl.BlockSpec(memory_space=pltpu.SMEM)] + [anywhere] * 4 + [local] * 4 + [anywhere] * 2,
        out_specs=(local, local),
        scratch_shapes=[
            pltpu.VMEM((sources, MOST, 2, block // 2, channels), bf),
            pltpu.VMEM((sources, MOST * block, width), bf),
            pltpu.VMEM((MOST * block, width), bf),
            pltpu.VMEM((patches, cells, width), f32),
            pltpu.VMEM((patches, cells, width), bf),
            pltpu.VMEM(wide.shape, bf),
            pltpu.VMEM(back.shape, f32),
            pltpu.VMEM((width, rows * cols), bf),
            pltpu.VMEM((MOST * block, width), bf),
            pltpu.VMEM((channels, width), f32),
            pltpu.VMEM((8, width), f32),
            pltpu.SemaphoreType.DMA((sources, 2)),
            pltpu.SemaphoreType.DMA((2,)),
        ],
        compiler_params=pltpu.CompilerParams(vmem_limit_bytes=VMEM_LIMIT),
    )(meta, own_a, own_b, got_a, got_b, encoder, kernels, kernels.swapaxes(1, 2), gain, wide, back)


def padded_2(shard, sides, width, wrap):
    for axis, dim in sides:
        size, length = (lax.axis_size(axis), shard.shape[dim])
        up = [(i, (i + 1) % size) for i in range(size if wrap else size - 1)]
        down = [(j, i) for i, j in up]
        last = lax.slice_in_dim(shard, length - width, length, axis=dim)
        leading = lax.slice_in_dim(shard, 0, width, axis=dim)
        before = lax.ppermute(last, axis, up)
        after = lax.ppermute(leading, axis, down)
        shard = jnp.concatenate([before, shard, after], axis=dim)
    return shard


def widen(field):
    beside_all = padded_2(field, (("lon", 1),), 1, True)
    return padded_2(beside_all, (("lat", 0),), 1, False)


def slot_tables(target, patch, kernel, tiles):
    blocks = target.shape[0]
    index = jnp.arange(blocks, dtype=jnp.int32)
    same = (target[:, None] == target[None, :]) & (index[None, :] < index[:, None])
    slot = target * MOST + jnp.sum(same, axis=1, dtype=jnp.int32)
    chosen = slot[None, :] == jnp.arange(tiles * MOST, dtype=jnp.int32)[:, None]

    def pick(values):
        return jnp.sum(jnp.where(chosen, values[None, :] + 1, 0), axis=1, dtype=jnp.int32) - 1

    source, kernels, patches = pick(index), pick(kernel), jnp.maximum(pick(patch), 0)
    meta = jnp.concatenate([kernels.reshape(tiles, MOST), patches.reshape(tiles, MOST)], axis=1)
    return source, jnp.pad(meta, ((0, 0), (0, 128 - 2 * MOST))).reshape(tiles, 1, 128)


def shards(spectra, target, patch, kernel, encoder_weight, kernels, gain, conv_weight, cotangent):
    tiles, bands = lax.axis_size("lon"), lax.axis_size("lat")
    rows, cols, width = cotangent.shape
    channels = spectra.shape[1]
    loss_scale = 1.0 / math.sqrt(rows * bands * cols * tiles)
    source, meta = slot_tables(target, patch, kernel, tiles)
    send_a, send_b = pack(source, spectra, kernels.shape[1])
    first = cotangent[:, :1].astype(jnp.float32)
    last = cotangent[:, -1:].astype(jnp.float32)
    weight = conv_weight.reshape(9, width, width)
    got_a, got_b, got_meta, wide, back = exchange(send_a, send_b, meta, cotangent, first, last, weight)
    part_rows = 192 * 112
    normed, parts = middle(
        got_meta.reshape(tiles, 128), send_a, send_b, got_a, got_b, encoder_weight, kernels,
        gain.reshape(1, width), wide, back, part_rows,
    )
    padded = widen(normed)
    total = jnp.zeros((rows * cols, width), jnp.float32)
    for a in range(3):
        for b in range(3):
            window = padded[a : a + rows, b : b + cols].reshape(-1, width)
            total = total + jnp.dot(window, conv_weight[a, b], preferred_element_type=jnp.float32)
    conv_out = total.reshape(rows, cols, width).astype(jnp.bfloat16)
    summed = lax.psum(parts.astype(jnp.float32), ("lat", "lon")) * loss_scale
    base = 9 * width * width // 128
    lanes = width // 128
    conv_grad = summed[:base].reshape(9, lanes, width, 128).swapaxes(1, 2).reshape(3, 3, width, width)
    size = channels * lanes
    encoder_grad = summed[base : base + size].reshape(lanes, channels, 128).swapaxes(0, 1).reshape(channels, width)
    gain_grad = summed[base + size : base + size + 8 * lanes].reshape(lanes, 8, 128).sum(axis=1).reshape(width)
    return conv_out, conv_grad, encoder_grad, gain_grad


def solution(mesh):
    placed = (
        P(("lat", "lon"), None),
        P(("lat", "lon")),
        P(("lat", "lon")),
        P(("lat", "lon")),
        P(),
        P(),
        P(),
        P(),
        P("lat", "lon", None),
    )
    return jax.shard_map(
        shards,
        mesh=mesh,
        in_specs=placed,
        out_specs=(P("lat", "lon", None), P(), P(), P()),
        check_vma=False,
    )
```

```python
import math

import jax
import jax.numpy as jnp
from jax import lax
from jax.experimental import pallas as pl
from jax.experimental.pallas import tpu as pltpu
from jax.sharding import PartitionSpec as P

PH = 8
PW = 16
MOST = 3
SIDE = 4
MESH = pl.DeviceIdType.MESH
VMEM_LIMIT = 60 * 1024 * 1024


def dot(a, b, ca, cb):
    return lax.dot_general(a, b, (((ca,), (cb,)), ((), ())), preferred_element_type=jnp.float32)


def pack_kernel(source_ref, spectra, to_a, to_b, held, blank, in_sem, out_sems):
    slots = source_ref.shape[0]
    rows = held.shape[1] // 2
    fetch = pltpu.make_async_copy(spectra, held, in_sem)
    fetch.start()
    blank[...] = jnp.zeros_like(blank)
    fetch.wait()

    def pieces(slot, source):
        tile = slot // MOST
        rank = slot - tile * MOST
        y, z = tile // SIDE, tile % SIDE
        return (
            pltpu.make_async_copy(source(0), to_a.at[z, y, rank], out_sems.at[slot, 0]),
            pltpu.make_async_copy(source(1), to_b.at[y, z, rank], out_sems.at[slot, 1]),
        )

    @pl.loop(0, slots)
    def _(slot):
        block = source_ref[slot]

        @pl.when(block >= 0)
        def _():
            for piece in pieces(slot, lambda half: held.at[block, pl.ds(half * rows, rows)]):
                piece.start()

        @pl.when(block < 0)
        def _():
            for piece in pieces(slot, lambda half: blank):
                piece.start()

    @pl.loop(0, slots)
    def _(slot):
        for piece in pieces(slot, lambda half: blank):
            piece.wait()


def pack(source_block, spectra, block_rows):
    blocks = spectra.shape[0] // block_rows
    channels = spectra.shape[1]
    half = block_rows // 2
    slots = source_block.shape[0]
    out = jax.ShapeDtypeStruct((SIDE, SIDE, MOST, half, channels), jnp.bfloat16)
    return pl.pallas_call(
        pack_kernel,
        name="pack",
        out_shape=(out, out),
        in_specs=[pl.BlockSpec(memory_space=pltpu.SMEM), pl.BlockSpec(memory_space=pl.ANY)],
        out_specs=(pl.BlockSpec(memory_space=pl.ANY),) * 2,
        scratch_shapes=[
            pltpu.VMEM((blocks, block_rows, channels), jnp.bfloat16),
            pltpu.VMEM((half, channels), jnp.bfloat16),
            pltpu.SemaphoreType.DMA,
            pltpu.SemaphoreType.DMA((slots, 2)),
        ],
        compiler_params=pltpu.CompilerParams(vmem_limit_bytes=VMEM_LIMIT),
    )(source_block, spectra.reshape(blocks, block_rows, channels))


def position():
    lat, lon = lax.axis_index("lat"), lax.axis_index("lon")
    return lat, lon, lon // SIDE, lon % SIDE


def halo_peers():
    lat, lon = lax.axis_index("lat"), lax.axis_index("lon")
    lats, lons = lax.axis_size("lat"), lax.axis_size("lon")
    up, down = (lat + lats - 1) % lats, (lat + 1) % lats
    left, right = (lon + lons - 1) % lons, (lon + 1) % lons
    return lat, lon, up, down, left, right


def halo_copies(top, bottom, first, last, from_above, from_below, from_left, from_right, sends, recvs):
    lat, lon, up, down, left, right = halo_peers()
    rows = first.shape[0]
    body = pl.ds(1, rows)
    plan = [
        (top, from_below, (up, lon)),
        (bottom, from_above, (down, lon)),
        (last, from_left.at[body], (lat, right)),
        (first, from_right.at[body], (lat, left)),
        (last.at[0], from_left.at[rows + 1], (up, right)),
        (last.at[rows - 1], from_left.at[0], (down, right)),
        (first.at[0], from_right.at[rows + 1], (up, left)),
        (first.at[rows - 1], from_right.at[0], (down, left)),
    ]
    return [
        pltpu.make_async_remote_copy(
            src_ref=src, dst_ref=dst, send_sem=sends.at[n], recv_sem=recvs.at[n], device_id=to, device_id_type=MESH
        )
        for n, (src, dst, to) in enumerate(plan)
    ]


def lay_windows(tile, from_above, from_below, from_left, from_right, wide, reverse):
    lat, lats = lax.axis_index("lat"), lax.axis_size("lat")
    rows, cols, width = tile.shape
    index = lax.broadcasted_iota(jnp.int32, (cols, width), 0)

    def lay(at, center, keep):
        value = center.astype(jnp.float32)
        before = jnp.where(index == 0, from_left[at], pltpu.roll(value, 1, 0))
        after = jnp.where(index == cols - 1, from_right[at], pltpu.roll(value, cols - 1, 0))
        if keep is not None:
            before, value, after = (jnp.where(keep, v, 0.0) for v in (before, value, after))
        order = (after, value, before) if reverse else (before, value, after)
        for n, v in enumerate(order):
            wide[at, :, n * width : (n + 1) * width] = v.astype(jnp.bfloat16)

    @pl.loop(0, rows)
    def _(row):
        lay(row + 1, tile[row], None)

    lay(0, from_above[...], lat > 0)
    lay(rows + 1, from_below[...], lat < lats - 1)


def exchange_kernel(
    send_a, send_b, meta, cot, first, last, weight,
    got_a, got_b, got_meta, wide_out, back_out, mid_a, mid_b, relay_a, relay_b,
    tile, wide, held_weight, back, above, below, lefts, rights,
    halo_send, halo_recv, meta_send, meta_recv, sends, recvs, local,
):
    lat, lon, y, z = position()
    lats = lax.axis_size("lat")
    count = lax.axis_size("lon")
    _, _, up, down, left, right = halo_peers()
    rows, cols, width = tile.shape

    barrier = pltpu.get_barrier_semaphore()
    for step in range(1, SIDE * SIDE):
        peer = (lon + step) % count
        pl.semaphore_signal(barrier, inc=1, device_id=(lat, peer), device_id_type=MESH)
    for other in (up, down):
        for peer in (left, lon, right):
            pl.semaphore_signal(barrier, inc=1, device_id=(other, peer), device_id_type=MESH)
    load_tile = pltpu.make_async_copy(cot, tile, local.at[0])
    load_weight = pltpu.make_async_copy(weight, held_weight, local.at[1])
    load_tile.start()
    load_weight.start()
    own_meta = pltpu.make_async_copy(meta.at[lon], got_meta.at[0], local.at[2])
    own_meta.start()
    pl.semaphore_wait(barrier, SIDE * SIDE - 1 + 6)

    halo = halo_copies(
        cot.at[0], cot.at[rows - 1], first, last, above, below, lefts, rights, halo_send, halo_recv
    )
    for copy in halo:
        copy.start()
    notes = []
    for dy in range(SIDE):
        for dz in range(SIDE):
            if dy or dz:
                n = dy * SIDE + dz
                to = (y + dy) % SIDE * SIDE + (z + dz) % SIDE
                notes.append(
                    pltpu.make_async_remote_copy(
                        src_ref=meta.at[to], dst_ref=got_meta.at[n], send_sem=meta_send.at[n],
                        recv_sem=meta_recv.at[n], device_id=(lat, to), device_id_type=MESH,
                    )
                )
    for copy in notes:
        copy.start()

    flows = []
    for flow, (src, mid, relay, got, u, v) in enumerate(
        ((send_a, mid_a, relay_a, got_a, z, y), (send_b, mid_b, relay_b, got_b, y, z))
    ):
        made = []

        def make(src_ref, dst_ref, du, dv, flow=flow, made=made, u=u, v=v):
            n = len(made)
            uu, vv = (u + du) % SIDE, (v + dv) % SIDE
            to = vv * SIDE + uu if flow == 0 else uu * SIDE + vv
            copy = pltpu.make_async_remote_copy(
                src_ref=src_ref, dst_ref=dst_ref, send_sem=sends.at[flow, n], recv_sem=recvs.at[flow, n],
                device_id=(lat, to), device_id_type=MESH,
            )
            made.append(copy)
            return copy

        def land(g, e, mid=mid, got=got):
            return got.at[0, e] if g == 0 else mid.at[g, e]

        def part(g, e, src=src, mid=mid, u=u, v=v):
            return src.at[u, (v + g) % SIDE] if e == 0 else mid.at[g, e]

        f = {"made": made}
        for d, sign in ((0, 1), (1, -1)):
            for j in range(2):
                g = 2 * d + j
                f["q1", d, j] = make(src.at[(u + 2) % SIDE, (v + g) % SIDE], relay.at[0, d, j], sign, 0)
                f["r1", d, j] = make(relay.at[0, d, j], land(g, 2), sign, 0)
            for g in range(SIDE):
                f["d1", d, g] = make(src.at[(u + sign) % SIDE, (v + g) % SIDE], land(g, 1 if d == 0 else 3), sign, 0)
            for e in range(SIDE):
                g = 1 if d == 0 else 3
                f["d2", d, e] = make(part(g, e), got.at[g, e], 0, sign)
            for j in range(2):
                e = ((0, 1), (3, 2))[d][j]
                f["q2", d, j] = make(part(2, e), relay.at[1, d, j], 0, sign)
                f["r2", d, j] = make(relay.at[1, d, j], got.at[2, e], 0, sign)
        flows.append(f)

    def start(*keys):
        for key in keys:
            for f in flows:
                f[key].start()

    def arrived(*keys):
        for key in keys:
            for f in flows:
                f[key].wait_recv()

    start(("q1", 0, 1), ("q1", 1, 0), ("q1", 0, 0), ("q1", 1, 1))
    for g in (2, 1, 3, 0):
        start(("d1", 0, g), ("d1", 1, g))

    load_tile.wait()
    for copy in halo:
        copy.wait()
    lay_windows(tile, above, below, lefts, rights, wide, True)
    save_wide = pltpu.make_async_copy(wide, wide_out, local.at[3])
    save_wide.start()
    load_weight.wait()
    step_rows = 4

    @pl.loop(0, rows // step_rows)
    def _(chunk):
        total = jnp.zeros((step_rows * cols, width), jnp.float32)
        for a in range(3):
            for b in range(3):
                window = wide[pl.ds(chunk * step_rows + 2 - a, step_rows), :, b * width : (b + 1) * width]
                total += dot(window.reshape(step_rows * cols, width), held_weight[a * 3 + b], 1, 1)
        back[pl.ds(chunk * step_rows, step_rows)] = total.reshape(step_rows, cols, width)

    save_back = pltpu.make_async_copy(back, back_out, local.at[4])
    save_back.start()

    for d, j in ((0, 1), (1, 0), (0, 0), (1, 1)):
        arrived(("q1", d, j))
        start(("r1", d, j))
    start(("q2", 0, 0), ("d2", 0, 0), ("d2", 1, 0))
    for g in (2, 1, 3, 0):
        arrived(("d1", 0, g), ("d1", 1, g))
        if g == 2:
            start(("q2", 0, 1), ("q2", 1, 0))
        if g == 1:
            start(("d2", 0, 1), ("d2", 0, 3))
        if g == 3:
            start(("d2", 1, 1), ("d2", 1, 3))
    arrived(("r1", 1, 0))
    start(("q2", 1, 1))
    arrived(("r1", 0, 1), ("r1", 1, 1))
    arrived(("q2", 0, 0))
    start(("r2", 0, 0))
    arrived(("q2", 0, 1), ("q2", 1, 0))
    start(("r2", 0, 1), ("r2", 1, 0))
    start(("d2", 0, 2), ("d2", 1, 2))
    arrived(("q2", 1, 1))
    start(("r2", 1, 1))
    arrived(("r1", 0, 0))
    for d in range(2):
        arrived(*(("d2", d, e) for e in range(SIDE)))
        arrived(("r2", d, 0), ("r2", d, 1))
    for f in flows:
        for copy in f["made"]:
            copy.wait_send()
    for copy in notes:
        copy.wait()
    own_meta.wait()
    save_wide.wait()
    save_back.wait()


def exchange(send_a, send_b, meta, cotangent, first, last, weight):
    rows, cols, width = cotangent.shape
    slot = send_a.shape[2:]
    lon = SIDE * SIDE
    bf, f32 = jnp.bfloat16, jnp.float32
    anywhere = pl.BlockSpec(memory_space=pl.ANY)
    whole = jax.ShapeDtypeStruct((SIDE, SIDE) + slot, bf)
    relay = jax.ShapeDtypeStruct((2, 2, 2) + slot, bf)
    out = pl.pallas_call(
        exchange_kernel,
        name="exchange",
        out_shape=(
            whole, whole, jax.ShapeDtypeStruct(meta.shape, meta.dtype),
            jax.ShapeDtypeStruct((rows + 2, cols, 3 * width), bf), jax.ShapeDtypeStruct((rows, cols, width), f32),
            whole, whole, relay, relay,
        ),
        in_specs=[anywhere] * 7,
        out_specs=(anywhere,) * 9,
        scratch_shapes=[
            pltpu.VMEM((rows, cols, width), bf),
            pltpu.VMEM((rows + 2, cols, 3 * width), bf),
            pltpu.VMEM(weight.shape, bf),
            pltpu.VMEM((rows, cols, width), f32),
            pltpu.VMEM((cols, width), bf),
            pltpu.VMEM((cols, width), bf),
            pltpu.VMEM((rows + 2, 1, width), f32),
            pltpu.VMEM((rows + 2, 1, width), f32),
            pltpu.SemaphoreType.DMA((8,)),
            pltpu.SemaphoreType.DMA((8,)),
            pltpu.SemaphoreType.DMA((lon,)),
            pltpu.SemaphoreType.DMA((lon,)),
            pltpu.SemaphoreType.DMA((2, 32)),
            pltpu.SemaphoreType.DMA((2, 32)),
            pltpu.SemaphoreType.DMA((5,)),
        ],
        compiler_params=pltpu.CompilerParams(
            collective_id=0, has_side_effects=True, vmem_limit_bytes=VMEM_LIMIT
        ),
    )(send_a, send_b, meta, cotangent, first, last, weight)
    return out[:5]


def middle_kernel(
    meta, own_a, own_b, got_a, got_b, encoder, kernels, turned, gain, wide_in, back_in,
    normed, parts,
    x, slope, encoded, spread, d_spread, wide, back, flipped, d_rows, encoder_sum, gain_sum,
    x_sems, local,
):
    lat, lon, y, z = position()
    rows, cols, width = normed.shape
    channels = encoder.shape[0]
    sources = SIDE * SIDE
    block = kernels.shape[1]
    copies = []
    for n in range(sources):
        dy, dz = n // SIDE, n % SIDE
        from_a = own_a.at[z, y] if n == 0 else got_a.at[dy, dz]
        from_b = own_b.at[y, z] if n == 0 else got_b.at[dz, dy]
        copies.append(pltpu.make_async_copy(from_a, x.at[n, :, 0], x_sems.at[n, 0]))
        copies.append(pltpu.make_async_copy(from_b, x.at[n, :, 1], x_sems.at[n, 1]))
    for copy in copies:
        copy.start()
    load_back = pltpu.make_async_copy(back_in, back, local.at[0])
    load_wide = pltpu.make_async_copy(wide_in, wide, local.at[1])
    load_back.start()
    load_wide.start()
    spread[...] = jnp.zeros_like(spread)

    @pl.loop(0, sources)
    def _(n):
        for half in range(2):
            pltpu.make_async_copy(got_a.at[0, 0], x.at[n, :, half], x_sems.at[n, half]).wait()
        pre = dot(x[n].reshape(MOST * block, channels), encoder[...], 1, 0)
        logistic = 0.5 * jnp.tanh(0.5 * pre) + 0.5
        encoded[...] = (pre * logistic).astype(jnp.bfloat16)
        slope[n] = (logistic * (1.0 + pre * (1.0 - logistic))).astype(jnp.bfloat16)
        for rank in range(MOST):
            which, patch = meta[n, rank], meta[n, MOST + rank]

            @pl.when(which >= 0)
            def _():
                spread[patch] += dot(turned[which], encoded[rank * block : (rank + 1) * block], 1, 0)

    load_back.wait()
    gain_sum[...] = jnp.zeros_like(gain_sum)
    across = cols // PW

    @pl.loop(0, spread.shape[0])
    def _(q):
        at = (pl.ds(q // across * PH, PH), pl.ds(pl.multiple_of(q % across * PW, PW), PW))
        value = spread[q]
        scale = lax.rsqrt(jnp.mean(value * value, axis=1, keepdims=True) + 1e-06)
        unit = value * scale
        weight = gain[...]
        normed[at] = (unit * weight).astype(jnp.bfloat16).reshape(PH, PW, width)
        given = back[at].reshape(PH * PW, width)
        product = given * unit
        gain_sum[...] += jnp.sum(product.reshape(PH * PW // 8, 8, width), axis=0)
        inner = jnp.mean(product * weight, axis=1, keepdims=True)
        d_spread[q] = (scale * (given * weight - unit * inner)).astype(jnp.bfloat16)

    step_rows = 4

    @pl.loop(0, rows // step_rows)
    def _(n):
        some = normed[pl.ds(n * step_rows, step_rows)].reshape(step_rows * cols, width)
        flipped[:, pl.ds(pl.multiple_of(n * step_rows * cols, 128), step_rows * cols)] = some.T

    load_wide.wait()
    for a in range(3):

        @pl.loop(0, 3 * width // 256)
        def _(j):
            window = wide[2 - a : 2 - a + rows, :, pl.ds(pl.multiple_of(j * 256, 256), 256)]
            got = dot(flipped[...], window.reshape(rows * cols, 256), 1, 0).astype(jnp.bfloat16)
            base = pl.multiple_of((a * (3 * width // 128) + 2 * j) * width, width)
            parts[pl.ds(base, width)] = got[:, :128]
            parts[pl.ds(pl.multiple_of(base + width, width), width)] = got[:, 128:]

    encoder_sum[...] = jnp.zeros_like(encoder_sum)

    @pl.loop(0, sources)
    def _(n):
        for rank in range(MOST):
            which, patch = jnp.maximum(meta[n, rank], 0), meta[n, MOST + rank]
            at = slice(rank * block, (rank + 1) * block)
            here = dot(kernels[which], d_spread[patch], 1, 0).astype(jnp.bfloat16).astype(jnp.float32)
            d_rows[at] = (here * slope[n, at].astype(jnp.float32)).astype(jnp.bfloat16)
        encoder_sum[...] += dot(x[n].reshape(MOST * block, channels), d_rows[...], 0, 0)

    base = 9 * width * width // 128
    for n in range(width // 128):
        lanes = slice(n * 128, (n + 1) * 128)
        parts[base + n * channels : base + (n + 1) * channels] = encoder_sum[:, lanes].astype(jnp.bfloat16)
    base += channels * width // 128
    for n in range(width // 128):
        parts[base + n * 8 : base + (n + 1) * 8] = gain_sum[:, n * 128 : (n + 1) * 128].astype(jnp.bfloat16)
    base += 8 * width // 128
    parts[base:] = jnp.zeros((parts.shape[0] - base, 128), jnp.bfloat16)


def middle(meta, own_a, own_b, got_a, got_b, encoder, kernels, gain, wide, back, part_rows):
    rows, cols, width = back.shape
    channels = encoder.shape[0]
    block, cells = kernels.shape[1:]
    patches = rows * cols // cells
    sources = SIDE * SIDE
    bf, f32 = jnp.bfloat16, jnp.float32
    anywhere = pl.BlockSpec(memory_space=pl.ANY)
    local = pl.BlockSpec(memory_space=pltpu.VMEM)
    return pl.pallas_call(
        middle_kernel,
        name="middle",
        out_shape=(jax.ShapeDtypeStruct((rows, cols, width), bf), jax.ShapeDtypeStruct((part_rows, 128), bf)),
        in_specs=[pl.BlockSpec(memory_space=pltpu.SMEM)] + [anywhere] * 4 + [local] * 4 + [anywhere] * 2,
        out_specs=(local, local),
        scratch_shapes=[
            pltpu.VMEM((sources, MOST, 2, block // 2, channels), bf),
            pltpu.VMEM((sources, MOST * block, width), bf),
            pltpu.VMEM((MOST * block, width), bf),
            pltpu.VMEM((patches, cells, width), f32),
            pltpu.VMEM((patches, cells, width), bf),
            pltpu.VMEM(wide.shape, bf),
            pltpu.VMEM(back.shape, f32),
            pltpu.VMEM((width, rows * cols), bf),
            pltpu.VMEM((MOST * block, width), bf),
            pltpu.VMEM((channels, width), f32),
            pltpu.VMEM((8, width), f32),
            pltpu.SemaphoreType.DMA((sources, 2)),
            pltpu.SemaphoreType.DMA((2,)),
        ],
        compiler_params=pltpu.CompilerParams(vmem_limit_bytes=VMEM_LIMIT),
    )(meta, own_a, own_b, got_a, got_b, encoder, kernels, kernels.swapaxes(1, 2), gain, wide, back)


PIECES = 16
PIECE_ROWS = 112
FLOWS = 6
STEP_AT = (0, 0, 8, 12, 14, 15, 16)
STEP_PIECES = 17


def pairing(place, parity):
    near, far = place + 1 - 2 * (place % 2), (place + 3 - 2 * (place % 2)) % SIDE
    turn, high, low = (place + 1) // 2 % 2, place // 2, place % 2
    return ((near, turn), (far, high)) if parity == 0 else ((far, high), (near, low))


def sum_kernel(
    parts, normed, first, last, weight,
    conv_out, summed,
    own, other, total, outgoing, incoming, result,
    tile, wide, held_weight, made, above, below, lefts, rights,
    halo_send, halo_recv, sends, recvs, local,
):
    lat, lon, y, z = position()
    x, core = lat // 2, lat % 2
    twin = (lat + 1 - 2 * core, lon)
    rows, cols, width = tile.shape
    _, _, up, down, left, right = halo_peers()

    def at_place(axis, place):
        if axis == 0:
            return (place * 2 + core, lon)
        return (lat, place * SIDE + z) if axis == 1 else (lat, y * SIDE + place)

    barrier = pltpu.get_barrier_semaphore()
    peers = [twin]
    for axis, place in enumerate((x, y, z)):
        peers += [at_place(axis, (place + 1) % SIDE), at_place(axis, (place + 3) % SIDE)]
    peers += [(lat, left), (lat, right)]
    peers += [(a, b) for a in (up, down) for b in (left, lon, right)]
    for peer in peers:
        pl.semaphore_signal(barrier, inc=1, device_id=peer, device_id_type=MESH)
    load_own = [pltpu.make_async_copy(parts.at[core, f], own.at[f], local.at[f]) for f in range(FLOWS)]
    load_tile = pltpu.make_async_copy(normed, tile, local.at[FLOWS])
    load_weight = pltpu.make_async_copy(weight, held_weight, local.at[FLOWS + 1])
    for copy in (load_tile, *load_own, load_weight):
        copy.start()
    pl.semaphore_wait(barrier, len(peers))

    halo = halo_copies(
        normed.at[0], normed.at[rows - 1], first, last, above, below, lefts, rights, halo_send, halo_recv
    )
    for copy in halo:
        copy.start()

    begun = []

    def remote(src, dst, flow, n, to):
        copy = pltpu.make_async_remote_copy(
            src_ref=src, dst_ref=dst, send_sem=sends.at[flow, n], recv_sem=recvs.at[flow, n],
            device_id=to, device_id_type=MESH,
        )
        copy.start()
        begun.append(copy)
        return copy

    plans = []
    for f in range(FLOWS):
        turn, parity = f // 2, f % 2
        places = (x, y, z)
        steps, base = [], 0
        for k in range(3):
            axis = (turn + k) % 3
            for partner, keep in pairing(places[axis], parity):
                size = PIECES >> (len(steps) + 1)
                if k < 2:
                    kept, sent = base + keep * size, base + (1 - keep) * size
                    base = kept
                else:
                    size, kept, sent = 1, base, base
                steps.append((at_place(axis, partner), size, kept, sent))
        plans.append(steps)

    crossing = [remote(parts.at[1 - core, f], other.at[f], f, 0, twin) for f in range(FLOWS)]

    load_tile.wait()
    for copy in halo:
        copy.wait()
    lay_windows(tile, above, below, lefts, rights, wide, False)
    load_weight.wait()
    step_rows = 4
    save = [pltpu.make_async_copy(made, conv_out, local.at[FLOWS + 2])]

    def convolve(chunk):
        value = jnp.zeros((step_rows * cols, width), jnp.float32)
        for a in range(3):
            window = wide[chunk * step_rows + a : chunk * step_rows + a + step_rows]
            value += dot(window.reshape(step_rows * cols, 3 * width), held_weight[a], 1, 0)
        made[chunk * step_rows : (chunk + 1) * step_rows] = value.astype(jnp.bfloat16).reshape(step_rows, cols, width)

    def send_step(f, k):
        to, size, _, _ = plans[f][k - 1]
        at = pl.ds(STEP_AT[k], size)
        return remote(outgoing.at[f, at], incoming.at[f, at], f, k, to)

    def absorb(f, k):
        _, size, kept, _ = plans[f][k - 1]
        _, _, kept_next, sent_next = plans[f][k]
        half = size // 2

        @pl.loop(0, half)
        def _(i):
            total[f, kept_next + i] += incoming[f, STEP_AT[k] + kept_next - kept + i].astype(jnp.float32)
            value = total[f, sent_next + i] + incoming[f, STEP_AT[k] + sent_next - kept + i].astype(jnp.float32)
            outgoing[f, STEP_AT[k + 1] + i] = value.astype(jnp.bfloat16)

    convolve(0)
    flying = []
    for f in range(FLOWS):
        _, size, kept, sent = plans[f][0]
        load_own[f].wait()
        crossing[f].wait_recv()

        @pl.loop(0, size)
        def _(i):
            total[f, kept + i] = own[f, kept + i].astype(jnp.float32) + other[f, kept + i].astype(jnp.float32)
            value = own[f, sent + i].astype(jnp.float32) + other[f, sent + i].astype(jnp.float32)
            outgoing[f, i] = value.astype(jnp.bfloat16)

        flying.append(send_step(f, 1))
    for k in range(1, 4):
        for chunk in ((), (1, 2, 3), (4,), (5,))[k]:
            convolve(chunk)
        if k == 3:
            save[0].start()
        for f in range(FLOWS):
            flying[f].wait_recv()
            absorb(f, k)
            flying[f] = send_step(f, k + 1)
    for f in range(FLOWS):
        flying[f].wait_recv()
        value = total[f, plans[f][3][2]] + incoming[f, STEP_AT[4]].astype(jnp.float32)
        outgoing[f, STEP_AT[5]] = value.astype(jnp.bfloat16)
        flying[f] = send_step(f, 5)
    for f in range(FLOWS):
        flying[f].wait_recv()
        value = outgoing[f, STEP_AT[5]].astype(jnp.float32) + incoming[f, STEP_AT[5]].astype(jnp.float32)
        outgoing[f, STEP_AT[6]] = value.astype(jnp.bfloat16)
        flying[f] = send_step(f, 6)

    n = 7
    passed = []

    def pass_on(f, start, size, n):
        at = result.at[core, f, pl.ds(start, size)]
        passed.append(remote(at, at, f, n, twin))

    for f in range(FLOWS):
        flying[f].wait_recv()
        value = outgoing[f, STEP_AT[6]].astype(jnp.float32) + incoming[f, STEP_AT[6]].astype(jnp.float32)
        base = plans[f][3][2]
        result[core, f, base] = value.astype(jnp.bfloat16)
        at = result.at[core, f, pl.ds(base, 1)]
        flying[f] = remote(at, at, f, n, plans[f][3][0])
        pass_on(f, base, 1, n + 1)
    for k in range(4, 0, -1):
        n += 2
        for f in range(FLOWS):
            _, size, kept, sent = plans[f][k - 1]
            flying[f].wait_recv()
            if k > 1:
                to, size_up, kept_up, _ = plans[f][k - 2]
                at = result.at[core, f, pl.ds(kept_up, size_up)]
                flying[f] = remote(at, at, f, n, to)
            pass_on(f, sent, size, n + 1)
    for copy in passed:
        copy.wait_recv()
    stored = pltpu.make_async_copy(result, summed, local.at[FLOWS + 3])
    stored.start()
    for copy in begun:
        copy.wait_send()
    save[0].wait()
    stored.wait()


def sum_all(parts, normed, first, last, weight):
    rows, cols, width = normed.shape
    bf, f32 = jnp.bfloat16, jnp.float32
    anywhere = pl.BlockSpec(memory_space=pl.ANY)
    inside = pl.BlockSpec(memory_space=pltpu.VMEM)
    piece = (PIECE_ROWS, 128)
    parts = parts.reshape((2, FLOWS, PIECES) + piece)
    return pl.pallas_call(
        sum_kernel,
        name="sum_all",
        out_shape=(jax.ShapeDtypeStruct(normed.shape, bf), jax.ShapeDtypeStruct(parts.shape, bf)),
        in_specs=[anywhere, anywhere, inside, inside, anywhere],
        out_specs=(anywhere, anywhere),
        scratch_shapes=[
            pltpu.VMEM((FLOWS, PIECES) + piece, bf),
            pltpu.VMEM((FLOWS, PIECES) + piece, bf),
            pltpu.VMEM((FLOWS, PIECES) + piece, f32),
            pltpu.VMEM((FLOWS, STEP_PIECES) + piece, bf),
            pltpu.VMEM((FLOWS, STEP_PIECES) + piece, bf),
            pltpu.VMEM((2, FLOWS, PIECES) + piece, bf),
            pltpu.VMEM((rows, cols, width), bf),
            pltpu.VMEM((rows + 2, cols, 3 * width), bf),
            pltpu.VMEM(weight.shape, bf),
            pltpu.VMEM((rows, cols, width), bf),
            pltpu.VMEM((cols, width), bf),
            pltpu.VMEM((cols, width), bf),
            pltpu.VMEM((rows + 2, 1, width), f32),
            pltpu.VMEM((rows + 2, 1, width), f32),
            pltpu.SemaphoreType.DMA((8,)),
            pltpu.SemaphoreType.DMA((8,)),
            pltpu.SemaphoreType.DMA((FLOWS, 17)),
            pltpu.SemaphoreType.DMA((FLOWS, 17)),
            pltpu.SemaphoreType.DMA((FLOWS + 4,)),
        ],
        compiler_params=pltpu.CompilerParams(
            collective_id=1, has_side_effects=True, vmem_limit_bytes=VMEM_LIMIT
        ),
    )(parts, normed, first, last, weight)


def finish_kernel(scale, some, everything, conv_grad, encoder_grad, gain_grad, rest, sem):
    width = conv_grad.shape[2]
    lanes = width // 128
    channels = encoder_grad.shape[0]
    for n in range(lanes):
        conv_grad[0, :, n * 128 : (n + 1) * 128] = some[n * width : (n + 1) * width].astype(jnp.float32) * scale

    @pl.when(pl.program_id(0) == 0)
    def _():
        copy = pltpu.make_async_copy(everything.at[pl.ds(9 * lanes * width, rest.shape[0])], rest, sem)
        copy.start()
        copy.wait()
        base = channels * lanes
        for n in range(lanes):
            at = slice(n * 128, (n + 1) * 128)
            encoder_grad[:, at] = rest[n * channels : (n + 1) * channels].astype(jnp.float32) * scale
            eight = rest[base + n * 8 : base + (n + 1) * 8].astype(jnp.float32)
            gain_grad[:, at] = jnp.sum(eight, axis=0, keepdims=True) * scale


def finish(summed, scale, channels, width):
    f32 = jnp.float32
    lanes = width // 128
    return pl.pallas_call(
        lambda *refs: finish_kernel(scale, *refs),
        name="finish",
        grid=(9,),
        out_shape=(
            jax.ShapeDtypeStruct((9, width, width), f32),
            jax.ShapeDtypeStruct((channels, width), f32),
            jax.ShapeDtypeStruct((1, width), f32),
        ),
        in_specs=[pl.BlockSpec((lanes * width, 128), lambda t: (t, 0)), pl.BlockSpec(memory_space=pl.ANY)],
        out_specs=(
            pl.BlockSpec((1, width, width), lambda t: (t, 0, 0)),
            pl.BlockSpec((channels, width), lambda t: (0, 0)),
            pl.BlockSpec((1, width), lambda t: (0, 0)),
        ),
        scratch_shapes=[pltpu.VMEM((channels * lanes + 8 * lanes, 128), jnp.bfloat16), pltpu.SemaphoreType.DMA],
        compiler_params=pltpu.CompilerParams(vmem_limit_bytes=VMEM_LIMIT),
    )(summed, summed)


def slot_tables(target, patch, kernel, tiles):
    blocks = target.shape[0]
    index = jnp.arange(blocks, dtype=jnp.int32)
    same = (target[:, None] == target[None, :]) & (index[None, :] < index[:, None])
    slot = target * MOST + jnp.sum(same, axis=1, dtype=jnp.int32)
    chosen = slot[None, :] == jnp.arange(tiles * MOST, dtype=jnp.int32)[:, None]

    def pick(values):
        return jnp.sum(jnp.where(chosen, values[None, :] + 1, 0), axis=1, dtype=jnp.int32) - 1

    source, kernels, patches = pick(index), pick(kernel), jnp.maximum(pick(patch), 0)
    meta = jnp.concatenate([kernels.reshape(tiles, MOST), patches.reshape(tiles, MOST)], axis=1)
    return source, jnp.pad(meta, ((0, 0), (0, 128 - 2 * MOST))).reshape(tiles, 1, 128)


def shards(spectra, target, patch, kernel, encoder_weight, kernels, gain, conv_weight, cotangent):
    tiles, bands = lax.axis_size("lon"), lax.axis_size("lat")
    rows, cols, width = cotangent.shape
    channels = spectra.shape[1]
    loss_scale = 1.0 / math.sqrt(rows * bands * cols * tiles)
    source, meta = slot_tables(target, patch, kernel, tiles)
    send_a, send_b = pack(source, spectra, kernels.shape[1])
    first = cotangent[:, :1].astype(jnp.float32)
    last = cotangent[:, -1:].astype(jnp.float32)
    weight = conv_weight.reshape(9, width, width)
    got_a, got_b, got_meta, wide, back = exchange(send_a, send_b, meta, cotangent, first, last, weight)
    part_rows = 192 * 112
    normed, parts = middle(
        got_meta.reshape(tiles, 128), send_a, send_b, got_a, got_b, encoder_weight, kernels,
        gain.reshape(1, width), wide, back, part_rows,
    )
    first = normed[:, :1].astype(jnp.float32)
    last = normed[:, -1:].astype(jnp.float32)
    conv_out, summed = sum_all(parts, normed, first, last, conv_weight.reshape(3, 3 * width, width))
    conv_grad, encoder_grad, gain_grad = finish(summed.reshape(part_rows, 128), loss_scale, channels, width)
    return conv_out, conv_grad.reshape(3, 3, width, width), encoder_grad, gain_grad.reshape(width)


def solution(mesh):
    placed = (
        P(("lat", "lon"), None),
        P(("lat", "lon")),
        P(("lat", "lon")),
        P(("lat", "lon")),
        P(),
        P(),
        P(),
        P(),
        P("lat", "lon", None),
    )
    return jax.shard_map(
        shards,
        mesh=mesh,
        in_specs=placed,
        out_specs=(P("lat", "lon", None), P(), P(), P()),
        check_vma=False,
    )
```

```python
import math

import jax
import jax.numpy as jnp
from jax import lax
from jax.experimental import pallas as pl
from jax.experimental.pallas import tpu as pltpu
from jax.sharding import PartitionSpec as P

PH = 8
PW = 16
MOST = 3
SIDE = 4
MESH = pl.DeviceIdType.MESH
VMEM_LIMIT = 60 * 1024 * 1024


def dot(a, b, ca, cb):
    return lax.dot_general(a, b, (((ca,), (cb,)), ((), ())), preferred_element_type=jnp.float32)


def pack_kernel(source_ref, spectra, to_a, to_b, held, blank, in_sem, out_sems):
    slots = source_ref.shape[0]
    high, block = to_a.shape[3:]
    low = to_b.shape[3]
    fetch = pltpu.make_async_copy(spectra, held, in_sem)
    fetch.start()
    blank[...] = jnp.zeros_like(blank)
    fetch.wait()

    def pieces(slot, source):
        tile = slot // MOST
        rank = slot - tile * MOST
        y, z = tile // SIDE, tile % SIDE
        return (
            pltpu.make_async_copy(source(0, high), to_a.at[z, y, rank], out_sems.at[slot, 0]),
            pltpu.make_async_copy(source(high, low), to_b.at[y, z, rank], out_sems.at[slot, 1]),
        )

    @pl.loop(0, slots)
    def _(slot):
        which = source_ref[slot]

        @pl.when(which >= 0)
        def _():
            lanes = pl.ds(pl.multiple_of(which * block, block), block)
            for piece in pieces(slot, lambda base, size: held.at[pl.ds(base, size), lanes]):
                piece.start()

        @pl.when(which < 0)
        def _():
            for piece in pieces(slot, lambda base, size: blank.at[pl.ds(0, size)]):
                piece.start()

    @pl.loop(0, slots)
    def _(slot):
        for piece in pieces(slot, lambda base, size: blank.at[pl.ds(0, size)]):
            piece.wait()


def pack(source_block, flipped_spectra, block):
    channels = flipped_spectra.shape[0]
    high = channels // 32 * 16
    low = channels - high
    slots = source_block.shape[0]
    outs = [jax.ShapeDtypeStruct((SIDE, SIDE, MOST, size, block), jnp.bfloat16) for size in (high, low)]
    return pl.pallas_call(
        pack_kernel,
        name="pack",
        out_shape=outs,
        in_specs=[pl.BlockSpec(memory_space=pltpu.SMEM), pl.BlockSpec(memory_space=pl.ANY)],
        out_specs=(pl.BlockSpec(memory_space=pl.ANY),) * 2,
        scratch_shapes=[
            pltpu.VMEM(flipped_spectra.shape, jnp.bfloat16),
            pltpu.VMEM((max(high, low), block), jnp.bfloat16),
            pltpu.SemaphoreType.DMA,
            pltpu.SemaphoreType.DMA((slots, 2)),
        ],
        compiler_params=pltpu.CompilerParams(vmem_limit_bytes=VMEM_LIMIT),
    )(source_block, flipped_spectra)


def position():
    lat, lon = lax.axis_index("lat"), lax.axis_index("lon")
    return lat, lon, lon // SIDE, lon % SIDE


def halo_peers():
    lat, lon = lax.axis_index("lat"), lax.axis_index("lon")
    lats, lons = lax.axis_size("lat"), lax.axis_size("lon")
    up, down = (lat + lats - 1) % lats, (lat + 1) % lats
    left, right = (lon + lons - 1) % lons, (lon + 1) % lons
    return lat, lon, up, down, left, right


def halo_copies(top, bottom, first, last, from_above, from_below, from_left, from_right, sends, recvs):
    lat, lon, up, down, left, right = halo_peers()
    rows = first.shape[0]
    body = pl.ds(1, rows)
    plan = [
        (top, from_below, (up, lon)),
        (bottom, from_above, (down, lon)),
        (last, from_left.at[body], (lat, right)),
        (first, from_right.at[body], (lat, left)),
        (last.at[0], from_left.at[rows + 1], (up, right)),
        (last.at[rows - 1], from_left.at[0], (down, right)),
        (first.at[0], from_right.at[rows + 1], (up, left)),
        (first.at[rows - 1], from_right.at[0], (down, left)),
    ]
    return [
        pltpu.make_async_remote_copy(
            src_ref=src, dst_ref=dst, send_sem=sends.at[n], recv_sem=recvs.at[n], device_id=to, device_id_type=MESH
        )
        for n, (src, dst, to) in enumerate(plan)
    ]


def lay_windows(tile, from_above, from_below, from_left, from_right, wide, reverse):
    lat, lats = lax.axis_index("lat"), lax.axis_size("lat")
    rows, cols, width = tile.shape
    index = lax.broadcasted_iota(jnp.int32, (cols, width), 0)

    def lay(at, center, keep):
        value = center.astype(jnp.float32)
        before = jnp.where(index == 0, from_left[at], pltpu.roll(value, 1, 0))
        after = jnp.where(index == cols - 1, from_right[at], pltpu.roll(value, cols - 1, 0))
        if keep is not None:
            before, value, after = (jnp.where(keep, v, 0.0) for v in (before, value, after))
        order = (after, value, before) if reverse else (before, value, after)
        for n, v in enumerate(order):
            wide[at, :, n * width : (n + 1) * width] = v.astype(jnp.bfloat16)

    @pl.loop(0, rows)
    def _(row):
        lay(row + 1, tile[row], None)

    lay(0, from_above[...], lat > 0)
    lay(rows + 1, from_below[...], lat < lats - 1)


def exchange_kernel(
    send_a, send_b, meta, cot, first, last, weight,
    got_a, got_b, got_meta, wide_out, back_out, mid_a, mid_b, relay_a, relay_b,
    tile, wide, held_weight, back, above, below, lefts, rights,
    halo_send, halo_recv, meta_send, meta_recv, sends, recvs, local,
):
    lat, lon, y, z = position()
    lats = lax.axis_size("lat")
    count = lax.axis_size("lon")
    _, _, up, down, left, right = halo_peers()
    rows, cols, width = tile.shape

    barrier = pltpu.get_barrier_semaphore()
    for step in range(1, SIDE * SIDE):
        peer = (lon + step) % count
        pl.semaphore_signal(barrier, inc=1, device_id=(lat, peer), device_id_type=MESH)
    for other in (up, down):
        for peer in (left, lon, right):
            pl.semaphore_signal(barrier, inc=1, device_id=(other, peer), device_id_type=MESH)
    load_tile = pltpu.make_async_copy(cot, tile, local.at[0])
    load_weight = pltpu.make_async_copy(weight, held_weight, local.at[1])
    load_tile.start()
    load_weight.start()
    own_meta = pltpu.make_async_copy(meta.at[lon], got_meta.at[0], local.at[2])
    own_meta.start()
    pl.semaphore_wait(barrier, SIDE * SIDE - 1 + 6)

    halo = halo_copies(
        cot.at[0], cot.at[rows - 1], first, last, above, below, lefts, rights, halo_send, halo_recv
    )
    for copy in halo:
        copy.start()
    notes = []
    for dy in range(SIDE):
        for dz in range(SIDE):
            if dy or dz:
                n = dy * SIDE + dz
                to = (y + dy) % SIDE * SIDE + (z + dz) % SIDE
                notes.append(
                    pltpu.make_async_remote_copy(
                        src_ref=meta.at[to], dst_ref=got_meta.at[n], send_sem=meta_send.at[n],
                        recv_sem=meta_recv.at[n], device_id=(lat, to), device_id_type=MESH,
                    )
                )
    for copy in notes:
        copy.start()

    flows = []
    for flow, (src, mid, relay, got, u, v) in enumerate(
        ((send_a, mid_a, relay_a, got_a, z, y), (send_b, mid_b, relay_b, got_b, y, z))
    ):
        made = []

        def make(src_ref, dst_ref, du, dv, flow=flow, made=made, u=u, v=v):
            n = len(made)
            uu, vv = (u + du) % SIDE, (v + dv) % SIDE
            to = vv * SIDE + uu if flow == 0 else uu * SIDE + vv
            copy = pltpu.make_async_remote_copy(
                src_ref=src_ref, dst_ref=dst_ref, send_sem=sends.at[flow, n], recv_sem=recvs.at[flow, n],
                device_id=(lat, to), device_id_type=MESH,
            )
            made.append(copy)
            return copy

        def land(g, e, mid=mid, got=got):
            return got.at[0, e] if g == 0 else mid.at[g, e]

        def part(g, e, src=src, mid=mid, u=u, v=v):
            return src.at[u, (v + g) % SIDE] if e == 0 else mid.at[g, e]

        f = {"made": made}
        for d, sign in ((0, 1), (1, -1)):
            for j in range(2):
                g = 2 * d + j
                f["q1", d, j] = make(src.at[(u + 2) % SIDE, (v + g) % SIDE], relay.at[0, d, j], sign, 0)
                f["r1", d, j] = make(relay.at[0, d, j], land(g, 2), sign, 0)
            for g in range(SIDE):
                f["d1", d, g] = make(src.at[(u + sign) % SIDE, (v + g) % SIDE], land(g, 1 if d == 0 else 3), sign, 0)
            for e in range(SIDE):
                g = 1 if d == 0 else 3
                f["d2", d, e] = make(part(g, e), got.at[g, e], 0, sign)
            for j in range(2):
                e = ((0, 1), (3, 2))[d][j]
                f["q2", d, j] = make(part(2, e), relay.at[1, d, j], 0, sign)
                f["r2", d, j] = make(relay.at[1, d, j], got.at[2, e], 0, sign)
        flows.append(f)

    def start(*keys):
        for key in keys:
            for f in flows:
                f[key].start()

    def arrived(*keys):
        for key in keys:
            for f in flows:
                f[key].wait_recv()

    start(("q1", 0, 1), ("q1", 1, 0), ("q1", 0, 0), ("q1", 1, 1))
    for g in (2, 1, 3, 0):
        start(("d1", 0, g), ("d1", 1, g))

    load_tile.wait()
    for copy in halo:
        copy.wait()
    lay_windows(tile, above, below, lefts, rights, wide, True)
    save_wide = pltpu.make_async_copy(wide, wide_out, local.at[3])
    save_wide.start()
    load_weight.wait()
    step_rows = 4

    @pl.loop(0, rows // step_rows)
    def _(chunk):
        total = jnp.zeros((step_rows * cols, width), jnp.float32)
        for a in range(3):
            for b in range(3):
                window = wide[pl.ds(chunk * step_rows + 2 - a, step_rows), :, b * width : (b + 1) * width]
                total += dot(window.reshape(step_rows * cols, width), held_weight[a * 3 + b], 1, 1)
        back[pl.ds(chunk * step_rows, step_rows)] = total.reshape(step_rows, cols, width)

    save_back = pltpu.make_async_copy(back, back_out, local.at[4])
    save_back.start()

    for d, j in ((0, 1), (1, 0), (0, 0), (1, 1)):
        arrived(("q1", d, j))
        start(("r1", d, j))
    start(("q2", 0, 0), ("d2", 0, 0), ("d2", 1, 0))
    for g in (2, 1, 3, 0):
        arrived(("d1", 0, g), ("d1", 1, g))
        if g == 2:
            start(("q2", 0, 1), ("q2", 1, 0))
        if g == 1:
            start(("d2", 0, 1), ("d2", 0, 3))
        if g == 3:
            start(("d2", 1, 1), ("d2", 1, 3))
    arrived(("r1", 1, 0))
    start(("q2", 1, 1))
    arrived(("r1", 0, 1), ("r1", 1, 1))
    arrived(("q2", 0, 0))
    start(("r2", 0, 0))
    arrived(("q2", 0, 1), ("q2", 1, 0))
    start(("r2", 0, 1), ("r2", 1, 0))
    start(("d2", 0, 2), ("d2", 1, 2))
    arrived(("q2", 1, 1))
    start(("r2", 1, 1))
    arrived(("r1", 0, 0))
    for d in range(2):
        arrived(*(("d2", d, e) for e in range(SIDE)))
        arrived(("r2", d, 0), ("r2", d, 1))
    for f in flows:
        for copy in f["made"]:
            copy.wait_send()
    for copy in notes:
        copy.wait()
    own_meta.wait()
    save_wide.wait()
    save_back.wait()


def exchange(send_a, send_b, meta, cotangent, first, last, weight):
    rows, cols, width = cotangent.shape
    lon = SIDE * SIDE
    bf, f32 = jnp.bfloat16, jnp.float32
    anywhere = pl.BlockSpec(memory_space=pl.ANY)
    whole = [jax.ShapeDtypeStruct(a.shape, bf) for a in (send_a, send_b)]
    relay = [jax.ShapeDtypeStruct((2, 2, 2) + a.shape[2:], bf) for a in (send_a, send_b)]
    out = pl.pallas_call(
        exchange_kernel,
        name="exchange",
        out_shape=(
            *whole, jax.ShapeDtypeStruct(meta.shape, meta.dtype),
            jax.ShapeDtypeStruct((rows + 2, cols, 3 * width), bf), jax.ShapeDtypeStruct((rows, cols, width), f32),
            *whole, *relay,
        ),
        in_specs=[anywhere] * 7,
        out_specs=(anywhere,) * 9,
        scratch_shapes=[
            pltpu.VMEM((rows, cols, width), bf),
            pltpu.VMEM((rows + 2, cols, 3 * width), bf),
            pltpu.VMEM(weight.shape, bf),
            pltpu.VMEM((rows, cols, width), f32),
            pltpu.VMEM((cols, width), bf),
            pltpu.VMEM((cols, width), bf),
            pltpu.VMEM((rows + 2, 1, width), f32),
            pltpu.VMEM((rows + 2, 1, width), f32),
            pltpu.SemaphoreType.DMA((8,)),
            pltpu.SemaphoreType.DMA((8,)),
            pltpu.SemaphoreType.DMA((lon,)),
            pltpu.SemaphoreType.DMA((lon,)),
            pltpu.SemaphoreType.DMA((2, 32)),
            pltpu.SemaphoreType.DMA((2, 32)),
            pltpu.SemaphoreType.DMA((5,)),
        ],
        compiler_params=pltpu.CompilerParams(
            collective_id=0, has_side_effects=True, vmem_limit_bytes=VMEM_LIMIT
        ),
    )(send_a, send_b, meta, cotangent, first, last, weight)
    return out[:5]


def middle_kernel(
    meta, own_a, own_b, got_a, got_b, encoder, kernels, turned, gain, wide_in, back_in,
    normed, first, last, parts,
    x, slope, encoded, spread, d_spread, wide, back, flipped, d_rows, encoder_sum, gain_sum,
    x_sems, local,
):
    lat, lon, y, z = position()
    rows, cols, width = normed.shape
    channels = encoder.shape[1]
    high = own_a.shape[3]
    sources = SIDE * SIDE
    block = kernels.shape[1]

    def fetch(n, rank, from_a, from_b):
        lanes = pl.ds(rank * block, block)
        return (
            pltpu.make_async_copy(from_a.at[rank], x.at[n, pl.ds(0, high), lanes], x_sems.at[n, rank, 0]),
            pltpu.make_async_copy(from_b.at[rank], x.at[n, pl.ds(high, channels - high), lanes], x_sems.at[n, rank, 1]),
        )

    for n in range(sources):
        dy, dz = n // SIDE, n % SIDE
        from_a = own_a.at[z, y] if n == 0 else got_a.at[dy, dz]
        from_b = own_b.at[y, z] if n == 0 else got_b.at[dz, dy]
        for rank in range(MOST):
            for copy in fetch(n, rank, from_a, from_b):
                copy.start()
    load_back = pltpu.make_async_copy(back_in, back, local.at[0])
    load_wide = pltpu.make_async_copy(wide_in, wide, local.at[1])
    load_back.start()
    load_wide.start()
    spread[...] = jnp.zeros_like(spread)

    @pl.loop(0, sources)
    def _(n):
        for rank in range(MOST):
            for copy in fetch(n, rank, got_a.at[0, 0], got_b.at[0, 0]):
                copy.wait()
        pre = dot(encoder[...], x[n], 1, 0)
        logistic = 0.5 * jnp.tanh(0.5 * pre) + 0.5
        encoded[...] = (pre * logistic).astype(jnp.bfloat16)
        slope[n] = logistic * (1.0 + pre * (1.0 - logistic))
        for rank in range(MOST):
            which, patch = meta[n, rank], meta[n, MOST + rank]

            @pl.when(which >= 0)
            def _():
                spread[patch] += dot(turned[which], encoded[:, rank * block : (rank + 1) * block], 1, 1)

    load_back.wait()
    gain_sum[...] = jnp.zeros_like(gain_sum)
    across = cols // PW

    @pl.loop(0, spread.shape[0])
    def _(q):
        at = (pl.ds(q // across * PH, PH), pl.ds(pl.multiple_of(q % across * PW, PW), PW))
        value = spread[q]
        scale = lax.rsqrt(jnp.mean(value * value, axis=1, keepdims=True) + 1e-06)
        unit = value * scale
        weight = gain[...]
        normed[at] = (unit * weight).astype(jnp.bfloat16).reshape(PH, PW, width)
        given = back[at].reshape(PH * PW, width)
        product = given * unit
        gain_sum[...] += jnp.sum(product.reshape(PH * PW // 8, 8, width), axis=0)
        inner = jnp.mean(product * weight, axis=1, keepdims=True)
        d_spread[q] = (scale * (given * weight - unit * inner)).astype(jnp.bfloat16).T

    step_rows = 4

    @pl.loop(0, rows // step_rows)
    def _(n):
        some = normed[pl.ds(n * step_rows, step_rows)].reshape(step_rows * cols, width)
        flipped[:, pl.ds(pl.multiple_of(n * step_rows * cols, 128), step_rows * cols)] = some.T

    @pl.loop(0, rows)
    def _(row):
        some = normed[row].astype(jnp.float32)
        first[row] = some[:1]
        last[row] = some[cols - 1 :]

    load_wide.wait()
    for a in range(3):

        @pl.loop(0, 3 * width // 256)
        def _(j):
            window = wide[2 - a : 2 - a + rows, :, pl.ds(pl.multiple_of(j * 256, 256), 256)]
            got = dot(flipped[...], window.reshape(rows * cols, 256), 1, 0).astype(jnp.bfloat16)
            base = pl.multiple_of((a * (3 * width // 128) + 2 * j) * width, width)
            parts[pl.ds(base, width)] = got[:, :128]
            parts[pl.ds(pl.multiple_of(base + width, width), width)] = got[:, 128:]

    encoder_sum[...] = jnp.zeros_like(encoder_sum)

    @pl.loop(0, sources)
    def _(n):
        for rank in range(MOST):
            which, patch = jnp.maximum(meta[n, rank], 0), meta[n, MOST + rank]
            lanes = slice(rank * block, (rank + 1) * block)
            here = dot(d_spread[patch], turned[which], 1, 0).astype(jnp.bfloat16).astype(jnp.float32)
            d_rows[:, lanes] = (here * slope[n, :, lanes]).astype(jnp.bfloat16)
        encoder_sum[...] += dot(x[n], d_rows[...], 1, 1)

    base = 9 * width * width // 128
    for n in range(width // 128):
        lanes = slice(n * 128, (n + 1) * 128)
        parts[base + n * channels : base + (n + 1) * channels] = encoder_sum[:, lanes].astype(jnp.bfloat16)
    base += channels * width // 128
    for n in range(width // 128):
        parts[base + n * 8 : base + (n + 1) * 8] = gain_sum[:, n * 128 : (n + 1) * 128].astype(jnp.bfloat16)
    base += 8 * width // 128
    parts[base:] = jnp.zeros((parts.shape[0] - base, 128), jnp.bfloat16)


def middle(meta, own_a, own_b, got_a, got_b, encoder, kernels, gain, wide, back, part_rows):
    rows, cols, width = back.shape
    channels = encoder.shape[0]
    block, cells = kernels.shape[1:]
    patches = rows * cols // cells
    sources = SIDE * SIDE
    bf, f32 = jnp.bfloat16, jnp.float32
    anywhere = pl.BlockSpec(memory_space=pl.ANY)
    local = pl.BlockSpec(memory_space=pltpu.VMEM)
    column = jax.ShapeDtypeStruct((rows, 1, width), f32)
    return pl.pallas_call(
        middle_kernel,
        name="middle",
        out_shape=(
            jax.ShapeDtypeStruct((rows, cols, width), bf), column, column, jax.ShapeDtypeStruct((part_rows, 128), bf)
        ),
        in_specs=[pl.BlockSpec(memory_space=pltpu.SMEM)] + [anywhere] * 4 + [local] * 4 + [anywhere] * 2,
        out_specs=(local,) * 4,
        scratch_shapes=[
            pltpu.VMEM((sources, channels, MOST * block), bf),
            pltpu.VMEM((sources, width, MOST * block), f32),
            pltpu.VMEM((width, MOST * block), bf),
            pltpu.VMEM((patches, cells, width), f32),
            pltpu.VMEM((patches, width, cells), bf),
            pltpu.VMEM(wide.shape, bf),
            pltpu.VMEM(back.shape, f32),
            pltpu.VMEM((width, rows * cols), bf),
            pltpu.VMEM((width, MOST * block), bf),
            pltpu.VMEM((channels, width), f32),
            pltpu.VMEM((8, width), f32),
            pltpu.SemaphoreType.DMA((sources, MOST, 2)),
            pltpu.SemaphoreType.DMA((2,)),
        ],
        compiler_params=pltpu.CompilerParams(vmem_limit_bytes=VMEM_LIMIT),
    )(meta, own_a, own_b, got_a, got_b, encoder.T, kernels, kernels.swapaxes(1, 2), gain, wide, back)


PIECES = 16
PIECE_ROWS = 112
FLOWS = 6
STEP_AT = (0, 0, 8, 0, 2, 3, 4)
EARLY_PIECES, LATE_PIECES = 12, 5


def pairing(place, parity):
    near, far = place + 1 - 2 * (place % 2), (place + 3 - 2 * (place % 2)) % SIDE
    turn, high, low = (place + 1) // 2 % 2, place // 2, place % 2
    return ((near, turn), (far, high)) if parity == 0 else ((far, high), (near, low))


def sum_kernel(
    parts, normed, first, last, weight,
    conv_out, summed,
    own, other, total, early_out, early_in, late_out, late_in, result,
    tile, wide, held_weight, made, above, below, lefts, rights,
    halo_send, halo_recv, sends, recvs, local,
):
    lat, lon, y, z = position()
    x, core = lat // 2, lat % 2
    twin = (lat + 1 - 2 * core, lon)
    rows, cols, width = tile.shape
    _, _, up, down, left, right = halo_peers()

    def at_place(axis, place):
        if axis == 0:
            return (place * 2 + core, lon)
        return (lat, place * SIDE + z) if axis == 1 else (lat, y * SIDE + place)

    barrier = pltpu.get_barrier_semaphore()
    peers = [twin]
    for axis, place in enumerate((x, y, z)):
        peers += [at_place(axis, (place + 1) % SIDE), at_place(axis, (place + 3) % SIDE)]
    peers += [(lat, left), (lat, right)]
    peers += [(a, b) for a in (up, down) for b in (left, lon, right)]
    for peer in peers:
        pl.semaphore_signal(barrier, inc=1, device_id=peer, device_id_type=MESH)
    load_own = [pltpu.make_async_copy(parts.at[core, f], own.at[f], local.at[f]) for f in range(FLOWS)]
    load_tile = pltpu.make_async_copy(normed, tile, local.at[FLOWS])
    load_weight = pltpu.make_async_copy(weight, held_weight, local.at[FLOWS + 1])
    for copy in (load_tile, *load_own, load_weight):
        copy.start()
    pl.semaphore_wait(barrier, len(peers))

    halo = halo_copies(
        normed.at[0], normed.at[rows - 1], first, last, above, below, lefts, rights, halo_send, halo_recv
    )
    for copy in halo:
        copy.start()

    begun = []

    def remote(src, dst, flow, n, to):
        copy = pltpu.make_async_remote_copy(
            src_ref=src, dst_ref=dst, send_sem=sends.at[flow, n], recv_sem=recvs.at[flow, n],
            device_id=to, device_id_type=MESH,
        )
        copy.start()
        begun.append(copy)
        return copy

    plans = []
    for f in range(FLOWS):
        turn, parity = f // 2, f % 2
        places = (x, y, z)
        steps, base = [], 0
        for k in range(3):
            axis = (turn + k) % 3
            for partner, keep in pairing(places[axis], parity):
                size = PIECES >> (len(steps) + 1)
                if k < 2:
                    kept, sent = base + keep * size, base + (1 - keep) * size
                    base = kept
                else:
                    size, kept, sent = 1, base, base
                steps.append((at_place(axis, partner), size, kept, sent))
        plans.append(steps)

    crossing = [remote(parts.at[1 - core, f], other.at[f], f, 0, twin) for f in range(FLOWS)]

    load_tile.wait()
    for copy in halo:
        copy.wait()
    lay_windows(tile, above, below, lefts, rights, wide, False)
    load_weight.wait()
    step_rows = 4
    save = [pltpu.make_async_copy(made, conv_out, local.at[FLOWS + 2])]

    def convolve(chunk):
        value = jnp.zeros((step_rows * cols, width), jnp.float32)
        for a in range(3):
            window = wide[chunk * step_rows + a : chunk * step_rows + a + step_rows]
            value += dot(window.reshape(step_rows * cols, 3 * width), held_weight[a], 1, 0)
        made[chunk * step_rows : (chunk + 1) * step_rows] = value.astype(jnp.bfloat16).reshape(step_rows, cols, width)

    def leaving(k):
        return early_out if k < 3 else late_out

    def arriving(k):
        return early_in if k < 3 else late_in

    def send_step(f, k):
        to, size, _, _ = plans[f][k - 1]
        at = pl.ds(STEP_AT[k], size)
        return remote(leaving(k).at[f, at], arriving(k).at[f, at], f, k, to)

    def absorb(f, k):
        _, size, kept, _ = plans[f][k - 1]
        _, _, kept_next, sent_next = plans[f][k]
        half = size // 2
        incoming, outgoing = arriving(k), leaving(k + 1)

        @pl.loop(0, half)
        def _(i):
            total[f, kept_next + i] += incoming[f, STEP_AT[k] + kept_next - kept + i].astype(jnp.float32)
            value = total[f, sent_next + i] + incoming[f, STEP_AT[k] + sent_next - kept + i].astype(jnp.float32)
            outgoing[f, STEP_AT[k + 1] + i] = value.astype(outgoing.dtype)

    convolve(0)
    flying = []
    for f in range(FLOWS):
        _, size, kept, sent = plans[f][0]
        load_own[f].wait()
        crossing[f].wait_recv()

        @pl.loop(0, size)
        def _(i):
            total[f, kept + i] = own[f, kept + i].astype(jnp.float32) + other[f, kept + i].astype(jnp.float32)
            value = own[f, sent + i].astype(jnp.float32) + other[f, sent + i].astype(jnp.float32)
            early_out[f, i] = value.astype(jnp.bfloat16)

        flying.append(send_step(f, 1))
    for k in range(1, 4):
        for chunk in ((), (1, 2, 3), (4,), (5,))[k]:
            convolve(chunk)
        if k == 3:
            save[0].start()
        for f in range(FLOWS):
            flying[f].wait_recv()
            absorb(f, k)
            flying[f] = send_step(f, k + 1)
    for f in range(FLOWS):
        flying[f].wait_recv()
        late_out[f, STEP_AT[5]] = total[f, plans[f][3][2]] + late_in[f, STEP_AT[4]]
        flying[f] = send_step(f, 5)
    for f in range(FLOWS):
        flying[f].wait_recv()
        late_out[f, STEP_AT[6]] = late_out[f, STEP_AT[5]] + late_in[f, STEP_AT[5]]
        flying[f] = send_step(f, 6)

    n = 7
    passed = []

    def pass_on(f, start, size, n):
        at = result.at[core, f, pl.ds(start, size)]
        passed.append(remote(at, at, f, n, twin))

    for f in range(FLOWS):
        flying[f].wait_recv()
        value = late_out[f, STEP_AT[6]] + late_in[f, STEP_AT[6]]
        base = plans[f][3][2]
        result[core, f, base] = value.astype(jnp.bfloat16)
        at = result.at[core, f, pl.ds(base, 1)]
        flying[f] = remote(at, at, f, n, plans[f][3][0])
        pass_on(f, base, 1, n + 1)
    for k in range(4, 0, -1):
        n += 2
        for f in range(FLOWS):
            _, size, kept, sent = plans[f][k - 1]
            flying[f].wait_recv()
            if k > 1:
                to, size_up, kept_up, _ = plans[f][k - 2]
                at = result.at[core, f, pl.ds(kept_up, size_up)]
                flying[f] = remote(at, at, f, n, to)
            pass_on(f, sent, size, n + 1)
    for copy in passed:
        copy.wait_recv()
    stored = pltpu.make_async_copy(result, summed, local.at[FLOWS + 3])
    stored.start()
    for copy in begun:
        copy.wait_send()
    save[0].wait()
    stored.wait()


def sum_all(parts, normed, first, last, weight):
    rows, cols, width = normed.shape
    bf, f32 = jnp.bfloat16, jnp.float32
    anywhere = pl.BlockSpec(memory_space=pl.ANY)
    inside = pl.BlockSpec(memory_space=pltpu.VMEM)
    piece = (PIECE_ROWS, 128)
    parts = parts.reshape((2, FLOWS, PIECES) + piece)
    return pl.pallas_call(
        sum_kernel,
        name="sum_all",
        out_shape=(jax.ShapeDtypeStruct(normed.shape, bf), jax.ShapeDtypeStruct(parts.shape, bf)),
        in_specs=[anywhere, anywhere, inside, inside, anywhere],
        out_specs=(anywhere, anywhere),
        scratch_shapes=[
            pltpu.VMEM((FLOWS, PIECES) + piece, bf),
            pltpu.VMEM((FLOWS, PIECES) + piece, bf),
            pltpu.VMEM((FLOWS, PIECES) + piece, f32),
            pltpu.VMEM((FLOWS, EARLY_PIECES) + piece, bf),
            pltpu.VMEM((FLOWS, EARLY_PIECES) + piece, bf),
            pltpu.VMEM((FLOWS, LATE_PIECES) + piece, f32),
            pltpu.VMEM((FLOWS, LATE_PIECES) + piece, f32),
            pltpu.VMEM((2, FLOWS, PIECES) + piece, bf),
            pltpu.VMEM((rows, cols, width), bf),
            pltpu.VMEM((rows + 2, cols, 3 * width), bf),
            pltpu.VMEM(weight.shape, bf),
            pltpu.VMEM((rows, cols, width), bf),
            pltpu.VMEM((cols, width), bf),
            pltpu.VMEM((cols, width), bf),
            pltpu.VMEM((rows + 2, 1, width), f32),
            pltpu.VMEM((rows + 2, 1, width), f32),
            pltpu.SemaphoreType.DMA((8,)),
            pltpu.SemaphoreType.DMA((8,)),
            pltpu.SemaphoreType.DMA((FLOWS, 17)),
            pltpu.SemaphoreType.DMA((FLOWS, 17)),
            pltpu.SemaphoreType.DMA((FLOWS + 4,)),
        ],
        compiler_params=pltpu.CompilerParams(
            collective_id=1, has_side_effects=True, vmem_limit_bytes=VMEM_LIMIT
        ),
    )(parts, normed, first, last, weight)


def finish_kernel(scale, some, everything, conv_grad, encoder_grad, gain_grad, rest, sem):
    width = conv_grad.shape[2]
    lanes = width // 128
    channels = encoder_grad.shape[0]
    for n in range(lanes):
        conv_grad[0, :, n * 128 : (n + 1) * 128] = some[n * width : (n + 1) * width].astype(jnp.float32) * scale

    @pl.when(pl.program_id(0) == 0)
    def _():
        copy = pltpu.make_async_copy(everything.at[pl.ds(9 * lanes * width, rest.shape[0])], rest, sem)
        copy.start()
        copy.wait()
        base = channels * lanes
        for n in range(lanes):
            at = slice(n * 128, (n + 1) * 128)
            encoder_grad[:, at] = rest[n * channels : (n + 1) * channels].astype(jnp.float32) * scale
            eight = rest[base + n * 8 : base + (n + 1) * 8].astype(jnp.float32)
            gain_grad[:, at] = jnp.sum(eight, axis=0, keepdims=True) * scale


def finish(summed, scale, channels, width):
    f32 = jnp.float32
    lanes = width // 128
    return pl.pallas_call(
        lambda *refs: finish_kernel(scale, *refs),
        name="finish",
        grid=(9,),
        out_shape=(
            jax.ShapeDtypeStruct((9, width, width), f32),
            jax.ShapeDtypeStruct((channels, width), f32),
            jax.ShapeDtypeStruct((1, width), f32),
        ),
        in_specs=[pl.BlockSpec((lanes * width, 128), lambda t: (t, 0)), pl.BlockSpec(memory_space=pl.ANY)],
        out_specs=(
            pl.BlockSpec((1, width, width), lambda t: (t, 0, 0)),
            pl.BlockSpec((channels, width), lambda t: (0, 0)),
            pl.BlockSpec((1, width), lambda t: (0, 0)),
        ),
        scratch_shapes=[pltpu.VMEM((channels * lanes + 8 * lanes, 128), jnp.bfloat16), pltpu.SemaphoreType.DMA],
        compiler_params=pltpu.CompilerParams(vmem_limit_bytes=VMEM_LIMIT),
    )(summed, summed)


def slot_tables(target, patch, kernel, tiles):
    blocks = target.shape[0]
    index = jnp.arange(blocks, dtype=jnp.int32)
    same = (target[:, None] == target[None, :]) & (index[None, :] < index[:, None])
    slot = target * MOST + jnp.sum(same, axis=1, dtype=jnp.int32)
    chosen = slot[None, :] == jnp.arange(tiles * MOST, dtype=jnp.int32)[:, None]

    def pick(values):
        return jnp.sum(jnp.where(chosen, values[None, :] + 1, 0), axis=1, dtype=jnp.int32) - 1

    source, kernels, patches = pick(index), pick(kernel), jnp.maximum(pick(patch), 0)
    meta = jnp.concatenate([kernels.reshape(tiles, MOST), patches.reshape(tiles, MOST)], axis=1)
    return source, jnp.pad(meta, ((0, 0), (0, 128 - 2 * MOST))).reshape(tiles, 1, 128)


def shards(spectra, target, patch, kernel, encoder_weight, kernels, gain, conv_weight, cotangent):
    tiles, bands = lax.axis_size("lon"), lax.axis_size("lat")
    rows, cols, width = cotangent.shape
    channels = spectra.shape[1]
    loss_scale = 1.0 / math.sqrt(rows * bands * cols * tiles)
    source, meta = slot_tables(target, patch, kernel, tiles)
    send_a, send_b = pack(source, spectra.T, kernels.shape[1])
    first = cotangent[:, :1].astype(jnp.float32)
    last = cotangent[:, -1:].astype(jnp.float32)
    weight = conv_weight.reshape(9, width, width)
    got_a, got_b, got_meta, wide, back = exchange(send_a, send_b, meta, cotangent, first, last, weight)
    part_rows = 192 * 112
    normed, first, last, parts = middle(
        got_meta.reshape(tiles, 128), send_a, send_b, got_a, got_b, encoder_weight, kernels,
        gain.reshape(1, width), wide, back, part_rows,
    )
    conv_out, summed = sum_all(parts, normed, first, last, conv_weight.reshape(3, 3 * width, width))
    conv_grad, encoder_grad, gain_grad = finish(summed.reshape(part_rows, 128), loss_scale, channels, width)
    return conv_out, conv_grad.reshape(3, 3, width, width), encoder_grad, gain_grad.reshape(width)


def solution(mesh):
    placed = (
        P(("lat", "lon"), None),
        P(("lat", "lon")),
        P(("lat", "lon")),
        P(("lat", "lon")),
        P(),
        P(),
        P(),
        P(),
        P("lat", "lon", None),
    )
    return jax.shard_map(
        shards,
        mesh=mesh,
        in_specs=placed,
        out_specs=(P("lat", "lon", None), P(), P(), P()),
        check_vma=False,
    )
```

```python
import math

import jax
import jax.numpy as jnp
from jax import lax
from jax.experimental import pallas as pl
from jax.experimental.pallas import tpu as pltpu
from jax.sharding import PartitionSpec as P

PH = 8
PW = 16
MOST = 3
SIDE = 4
MESH = pl.DeviceIdType.MESH
VMEM_LIMIT = 60 * 1024 * 1024


def dot(a, b, ca, cb):
    return lax.dot_general(a, b, (((ca,), (cb,)), ((), ())), preferred_element_type=jnp.float32)


def pack_kernel(
    target, patch, kernel, spectra, cot, to_a, to_b, meta, first, last,
    held, blank, near, far, block_in, counts, in_sems, out_sems,
):
    slots = block_in.shape[0]
    high, block = to_a.shape[3:]
    low = to_b.shape[3]
    rows, cols, _ = cot.shape
    fetch = pltpu.make_async_copy(spectra, held, in_sems.at[0])
    fetch.start()
    edges = [
        pltpu.make_async_copy(cot.at[:, pl.ds(0, 8)], near, in_sems.at[1]),
        pltpu.make_async_copy(cot.at[:, pl.ds(cols - 8, 8)], far, in_sems.at[2]),
    ]
    for edge in edges:
        edge.start()
    blank[...] = jnp.zeros_like(blank)

    @pl.loop(0, slots // MOST)
    def _(tile):
        counts[tile] = 0
        for rank in range(MOST):
            block_in[tile * MOST + rank] = -1
            meta[tile, rank] = -1
            meta[tile, MOST + rank] = 0

    @pl.loop(0, target.shape[0])
    def _(which):
        tile = target[which]
        rank = counts[tile]
        counts[tile] = rank + 1
        block_in[tile * MOST + rank] = which
        meta[tile, rank] = kernel[which]
        meta[tile, MOST + rank] = patch[which]

    fetch.wait()

    def pieces(slot, source):
        tile = slot // MOST
        rank = slot - tile * MOST
        y, z = tile // SIDE, tile % SIDE
        return (
            pltpu.make_async_copy(source(0, high), to_a.at[z, y, rank], out_sems.at[slot, 0]),
            pltpu.make_async_copy(source(high, low), to_b.at[y, z, rank], out_sems.at[slot, 1]),
        )

    @pl.loop(0, slots)
    def _(slot):
        which = block_in[slot]

        @pl.when(which >= 0)
        def _():
            lanes = pl.ds(pl.multiple_of(which * block, block), block)
            for piece in pieces(slot, lambda base, size: held.at[pl.ds(base, size), lanes]):
                piece.start()

        @pl.when(which < 0)
        def _():
            for piece in pieces(slot, lambda base, size: blank.at[pl.ds(0, size)]):
                piece.start()

    for edge in edges:
        edge.wait()

    @pl.loop(0, rows)
    def _(row):
        first[row] = near[row].astype(jnp.float32)[:1]
        last[row] = far[row].astype(jnp.float32)[7:]

    @pl.loop(0, slots)
    def _(slot):
        for piece in pieces(slot, lambda base, size: blank.at[pl.ds(0, size)]):
            piece.wait()


def pack(target, patch, kernel, flipped_spectra, cotangent, block, tiles):
    channels = flipped_spectra.shape[0]
    rows, _, width = cotangent.shape
    high = channels // 32 * 16
    low = channels - high
    slots = tiles * MOST
    bf, f32 = jnp.bfloat16, jnp.float32
    outs = [jax.ShapeDtypeStruct((SIDE, SIDE, MOST, size, block), bf) for size in (high, low)]
    outs.append(jax.ShapeDtypeStruct((tiles, 128), jnp.int32))
    outs += [jax.ShapeDtypeStruct((rows, 1, width), f32)] * 2
    anywhere = pl.BlockSpec(memory_space=pl.ANY)
    scalars = pl.BlockSpec(memory_space=pltpu.SMEM)
    inside = pl.BlockSpec(memory_space=pltpu.VMEM)
    return pl.pallas_call(
        pack_kernel,
        name="pack",
        out_shape=outs,
        in_specs=[scalars] * 3 + [anywhere] * 2,
        out_specs=(anywhere, anywhere, scalars, inside, inside),
        scratch_shapes=[
            pltpu.VMEM(flipped_spectra.shape, bf),
            pltpu.VMEM((max(high, low), block), bf),
            pltpu.VMEM((rows, 8, width), bf),
            pltpu.VMEM((rows, 8, width), bf),
            pltpu.SMEM((slots,), jnp.int32),
            pltpu.SMEM((tiles,), jnp.int32),
            pltpu.SemaphoreType.DMA((3,)),
            pltpu.SemaphoreType.DMA((slots, 2)),
        ],
        compiler_params=pltpu.CompilerParams(vmem_limit_bytes=VMEM_LIMIT),
    )(target, patch, kernel, flipped_spectra, cotangent)


def position():
    lat, lon = lax.axis_index("lat"), lax.axis_index("lon")
    return lat, lon, lon // SIDE, lon % SIDE


def halo_peers():
    lat, lon = lax.axis_index("lat"), lax.axis_index("lon")
    lats, lons = lax.axis_size("lat"), lax.axis_size("lon")
    up, down = (lat + lats - 1) % lats, (lat + 1) % lats
    left, right = (lon + lons - 1) % lons, (lon + 1) % lons
    return lat, lon, up, down, left, right


def halo_copies(top, bottom, first, last, from_above, from_below, from_left, from_right, sends, recvs):
    lat, lon, up, down, left, right = halo_peers()
    rows = first.shape[0]
    body = pl.ds(1, rows)
    plan = [
        (top, from_below, (up, lon)),
        (bottom, from_above, (down, lon)),
        (last, from_left.at[body], (lat, right)),
        (first, from_right.at[body], (lat, left)),
        (last.at[0], from_left.at[rows + 1], (up, right)),
        (last.at[rows - 1], from_left.at[0], (down, right)),
        (first.at[0], from_right.at[rows + 1], (up, left)),
        (first.at[rows - 1], from_right.at[0], (down, left)),
    ]
    return [
        pltpu.make_async_remote_copy(
            src_ref=src, dst_ref=dst, send_sem=sends.at[n], recv_sem=recvs.at[n], device_id=to, device_id_type=MESH
        )
        for n, (src, dst, to) in enumerate(plan)
    ]


def lay_windows(tile, from_above, from_below, from_left, from_right, wide, reverse):
    lat, lats = lax.axis_index("lat"), lax.axis_size("lat")
    rows, cols, width = tile.shape
    index = lax.broadcasted_iota(jnp.int32, (cols, width), 0)

    def lay(at, center, keep):
        value = center.astype(jnp.float32)
        before = jnp.where(index == 0, from_left[at], pltpu.roll(value, 1, 0))
        after = jnp.where(index == cols - 1, from_right[at], pltpu.roll(value, cols - 1, 0))
        if keep is not None:
            before, value, after = (jnp.where(keep, v, 0.0) for v in (before, value, after))
        order = (after, value, before) if reverse else (before, value, after)
        for n, v in enumerate(order):
            wide[at, :, n * width : (n + 1) * width] = v.astype(jnp.bfloat16)

    @pl.loop(0, rows)
    def _(row):
        lay(row + 1, tile[row], None)

    lay(0, from_above[...], lat > 0)
    lay(rows + 1, from_below[...], lat < lats - 1)


def exchange_kernel(
    send_a, send_b, meta, cot, first, last, weight,
    got_a, got_b, got_meta, wide_out, back_out, mid_a, mid_b, relay_a, relay_b,
    tile, wide, held_weight, back, above, below, lefts, rights,
    halo_send, halo_recv, meta_send, meta_recv, sends, recvs, local,
):
    lat, lon, y, z = position()
    lats = lax.axis_size("lat")
    count = lax.axis_size("lon")
    _, _, up, down, left, right = halo_peers()
    rows, cols, width = tile.shape

    barrier = pltpu.get_barrier_semaphore()
    for step in range(1, SIDE * SIDE):
        peer = (lon + step) % count
        pl.semaphore_signal(barrier, inc=1, device_id=(lat, peer), device_id_type=MESH)
    for other in (up, down):
        for peer in (left, lon, right):
            pl.semaphore_signal(barrier, inc=1, device_id=(other, peer), device_id_type=MESH)
    load_tile = pltpu.make_async_copy(cot, tile, local.at[0])
    load_weight = pltpu.make_async_copy(weight, held_weight, local.at[1])
    load_tile.start()
    load_weight.start()
    own_meta = pltpu.make_async_copy(meta.at[lon], got_meta.at[0], local.at[2])
    own_meta.start()
    pl.semaphore_wait(barrier, SIDE * SIDE - 1 + 6)

    halo = halo_copies(
        cot.at[0], cot.at[rows - 1], first, last, above, below, lefts, rights, halo_send, halo_recv
    )
    for copy in halo:
        copy.start()
    notes = []
    for dy in range(SIDE):
        for dz in range(SIDE):
            if dy or dz:
                n = dy * SIDE + dz
                to = (y + dy) % SIDE * SIDE + (z + dz) % SIDE
                notes.append(
                    pltpu.make_async_remote_copy(
                        src_ref=meta.at[to], dst_ref=got_meta.at[n], send_sem=meta_send.at[n],
                        recv_sem=meta_recv.at[n], device_id=(lat, to), device_id_type=MESH,
                    )
                )
    for copy in notes:
        copy.start()

    flows = []
    for flow, (src, mid, relay, got, u, v) in enumerate(
        ((send_a, mid_a, relay_a, got_a, z, y), (send_b, mid_b, relay_b, got_b, y, z))
    ):
        made = []

        def make(src_ref, dst_ref, du, dv, flow=flow, made=made, u=u, v=v):
            n = len(made)
            uu, vv = (u + du) % SIDE, (v + dv) % SIDE
            to = vv * SIDE + uu if flow == 0 else uu * SIDE + vv
            copy = pltpu.make_async_remote_copy(
                src_ref=src_ref, dst_ref=dst_ref, send_sem=sends.at[flow, n], recv_sem=recvs.at[flow, n],
                device_id=(lat, to), device_id_type=MESH,
            )
            made.append(copy)
            return copy

        def land(g, e, mid=mid, got=got):
            return got.at[0, e] if g == 0 else mid.at[g, e]

        def part(g, e, src=src, mid=mid, u=u, v=v):
            return src.at[u, (v + g) % SIDE] if e == 0 else mid.at[g, e]

        f = {"made": made}
        for d, sign in ((0, 1), (1, -1)):
            for j in range(2):
                g = 2 * d + j
                f["q1", d, j] = make(src.at[(u + 2) % SIDE, (v + g) % SIDE], relay.at[0, d, j], sign, 0)
                f["r1", d, j] = make(relay.at[0, d, j], land(g, 2), sign, 0)
            for g in range(SIDE):
                f["d1", d, g] = make(src.at[(u + sign) % SIDE, (v + g) % SIDE], land(g, 1 if d == 0 else 3), sign, 0)
            for e in range(SIDE):
                g = 1 if d == 0 else 3
                f["d2", d, e] = make(part(g, e), got.at[g, e], 0, sign)
            for j in range(2):
                e = ((0, 1), (3, 2))[d][j]
                f["q2", d, j] = make(part(2, e), relay.at[1, d, j], 0, sign)
                f["r2", d, j] = make(relay.at[1, d, j], got.at[2, e], 0, sign)
        flows.append(f)

    def start(*keys):
        for key in keys:
            for f in flows:
                f[key].start()

    def arrived(*keys):
        for key in keys:
            for f in flows:
                f[key].wait_recv()

    start(("q1", 0, 1), ("q1", 1, 0), ("q1", 0, 0), ("q1", 1, 1))
    for g in (2, 1, 3, 0):
        start(("d1", 0, g), ("d1", 1, g))

    load_tile.wait()
    for copy in halo:
        copy.wait()
    lay_windows(tile, above, below, lefts, rights, wide, True)
    save_wide = pltpu.make_async_copy(wide, wide_out, local.at[3])
    save_wide.start()
    load_weight.wait()
    step_rows = 4

    @pl.loop(0, rows // step_rows)
    def _(chunk):
        total = jnp.zeros((step_rows * cols, width), jnp.float32)
        for a in range(3):
            for b in range(3):
                window = wide[pl.ds(chunk * step_rows + 2 - a, step_rows), :, b * width : (b + 1) * width]
                total += dot(window.reshape(step_rows * cols, width), held_weight[a * 3 + b], 1, 1)
        back[pl.ds(chunk * step_rows, step_rows)] = total.reshape(step_rows, cols, width)

    save_back = pltpu.make_async_copy(back, back_out, local.at[4])
    save_back.start()

    for d, j in ((0, 1), (1, 0), (0, 0), (1, 1)):
        arrived(("q1", d, j))
        start(("r1", d, j))
    start(("q2", 0, 0), ("d2", 0, 0), ("d2", 1, 0))
    for g in (2, 1, 3, 0):
        arrived(("d1", 0, g), ("d1", 1, g))
        if g == 2:
            start(("q2", 0, 1), ("q2", 1, 0))
        if g == 1:
            start(("d2", 0, 1), ("d2", 0, 3))
        if g == 3:
            start(("d2", 1, 1), ("d2", 1, 3))
    arrived(("r1", 1, 0))
    start(("q2", 1, 1))
    arrived(("r1", 0, 1), ("r1", 1, 1))
    arrived(("q2", 0, 0))
    start(("r2", 0, 0))
    arrived(("q2", 0, 1), ("q2", 1, 0))
    start(("r2", 0, 1), ("r2", 1, 0))
    start(("d2", 0, 2), ("d2", 1, 2))
    arrived(("q2", 1, 1))
    start(("r2", 1, 1))
    arrived(("r1", 0, 0))
    for d in range(2):
        arrived(*(("d2", d, e) for e in range(SIDE)))
        arrived(("r2", d, 0), ("r2", d, 1))
    for f in flows:
        for copy in f["made"]:
            copy.wait_send()
    for copy in notes:
        copy.wait()
    own_meta.wait()
    save_wide.wait()
    save_back.wait()


def exchange(send_a, send_b, meta, cotangent, first, last, weight):
    rows, cols, width = cotangent.shape
    lon = SIDE * SIDE
    bf, f32 = jnp.bfloat16, jnp.float32
    anywhere = pl.BlockSpec(memory_space=pl.ANY)
    whole = [jax.ShapeDtypeStruct(a.shape, bf) for a in (send_a, send_b)]
    relay = [jax.ShapeDtypeStruct((2, 2, 2) + a.shape[2:], bf) for a in (send_a, send_b)]
    out = pl.pallas_call(
        exchange_kernel,
        name="exchange",
        out_shape=(
            *whole, jax.ShapeDtypeStruct(meta.shape, meta.dtype),
            jax.ShapeDtypeStruct((rows + 2, cols, 3 * width), bf), jax.ShapeDtypeStruct((rows, cols, width), f32),
            *whole, *relay,
        ),
        in_specs=[anywhere] * 7,
        out_specs=(anywhere,) * 9,
        scratch_shapes=[
            pltpu.VMEM((rows, cols, width), bf),
            pltpu.VMEM((rows + 2, cols, 3 * width), bf),
            pltpu.VMEM(weight.shape, bf),
            pltpu.VMEM((rows, cols, width), f32),
            pltpu.VMEM((cols, width), bf),
            pltpu.VMEM((cols, width), bf),
            pltpu.VMEM((rows + 2, 1, width), f32),
            pltpu.VMEM((rows + 2, 1, width), f32),
            pltpu.SemaphoreType.DMA((8,)),
            pltpu.SemaphoreType.DMA((8,)),
            pltpu.SemaphoreType.DMA((lon,)),
            pltpu.SemaphoreType.DMA((lon,)),
            pltpu.SemaphoreType.DMA((2, 32)),
            pltpu.SemaphoreType.DMA((2, 32)),
            pltpu.SemaphoreType.DMA((5,)),
        ],
        compiler_params=pltpu.CompilerParams(
            collective_id=0, has_side_effects=True, vmem_limit_bytes=VMEM_LIMIT
        ),
    )(send_a, send_b, meta, cotangent, first, last, weight)
    return out[:5]


def middle_kernel(
    meta, own_a, own_b, got_a, got_b, encoder, kernels, turned, gain, wide_in, back_in,
    normed, first, last, parts,
    x, slope, encoded, spread, d_spread, wide, back, flipped, d_rows, encoder_sum, gain_sum,
    x_sems, local,
):
    lat, lon, y, z = position()
    rows, cols, width = normed.shape
    channels = encoder.shape[1]
    high = own_a.shape[3]
    sources = SIDE * SIDE
    block = kernels.shape[1]

    def fetch(n, rank, from_a, from_b):
        lanes = pl.ds(rank * block, block)
        return (
            pltpu.make_async_copy(from_a.at[rank], x.at[n, pl.ds(0, high), lanes], x_sems.at[n, rank, 0]),
            pltpu.make_async_copy(from_b.at[rank], x.at[n, pl.ds(high, channels - high), lanes], x_sems.at[n, rank, 1]),
        )

    for n in range(sources):
        dy, dz = n // SIDE, n % SIDE
        from_a = own_a.at[z, y] if n == 0 else got_a.at[dy, dz]
        from_b = own_b.at[y, z] if n == 0 else got_b.at[dz, dy]
        for rank in range(MOST):
            for copy in fetch(n, rank, from_a, from_b):
                copy.start()
    load_back = pltpu.make_async_copy(back_in, back, local.at[0])
    load_wide = pltpu.make_async_copy(wide_in, wide, local.at[1])
    load_back.start()
    load_wide.start()
    spread[...] = jnp.zeros_like(spread)

    @pl.loop(0, sources)
    def _(n):
        for rank in range(MOST):
            for copy in fetch(n, rank, got_a.at[0, 0], got_b.at[0, 0]):
                copy.wait()
        pre = dot(encoder[...], x[n], 1, 0)
        logistic = 0.5 * jnp.tanh(0.5 * pre) + 0.5
        encoded[...] = (pre * logistic).astype(jnp.bfloat16)
        slope[n] = logistic * (1.0 + pre * (1.0 - logistic))
        for rank in range(MOST):
            which, patch = meta[n, rank], meta[n, MOST + rank]

            @pl.when(which >= 0)
            def _():
                spread[patch] += dot(turned[which], encoded[:, rank * block : (rank + 1) * block], 1, 1)

    load_back.wait()
    gain_sum[...] = jnp.zeros_like(gain_sum)
    across = cols // PW

    @pl.loop(0, spread.shape[0])
    def _(q):
        at = (pl.ds(q // across * PH, PH), pl.ds(pl.multiple_of(q % across * PW, PW), PW))
        value = spread[q]
        scale = lax.rsqrt(jnp.mean(value * value, axis=1, keepdims=True) + 1e-06)
        unit = value * scale
        weight = gain[...]
        normed[at] = (unit * weight).astype(jnp.bfloat16).reshape(PH, PW, width)
        given = back[at].reshape(PH * PW, width)
        product = given * unit
        gain_sum[...] += jnp.sum(product.reshape(PH * PW // 8, 8, width), axis=0)
        inner = jnp.mean(product * weight, axis=1, keepdims=True)
        d_spread[q] = (scale * (given * weight - unit * inner)).astype(jnp.bfloat16).T

    step_rows = 4

    @pl.loop(0, rows // step_rows)
    def _(n):
        some = normed[pl.ds(n * step_rows, step_rows)].reshape(step_rows * cols, width)
        flipped[:, pl.ds(pl.multiple_of(n * step_rows * cols, 128), step_rows * cols)] = some.T

    @pl.loop(0, rows)
    def _(row):
        some = normed[row].astype(jnp.float32)
        first[row] = some[:1]
        last[row] = some[cols - 1 :]

    load_wide.wait()
    for a in range(3):

        @pl.loop(0, 3 * width // 256)
        def _(j):
            window = wide[2 - a : 2 - a + rows, :, pl.ds(pl.multiple_of(j * 256, 256), 256)]
            got = dot(flipped[...], window.reshape(rows * cols, 256), 1, 0).astype(jnp.bfloat16)
            base = pl.multiple_of((a * (3 * width // 128) + 2 * j) * width, width)
            parts[pl.ds(base, width)] = got[:, :128]
            parts[pl.ds(pl.multiple_of(base + width, width), width)] = got[:, 128:]

    encoder_sum[...] = jnp.zeros_like(encoder_sum)

    @pl.loop(0, sources)
    def _(n):
        for rank in range(MOST):
            which, patch = jnp.maximum(meta[n, rank], 0), meta[n, MOST + rank]
            lanes = slice(rank * block, (rank + 1) * block)
            here = dot(d_spread[patch], turned[which], 1, 0).astype(jnp.bfloat16).astype(jnp.float32)
            d_rows[:, lanes] = (here * slope[n, :, lanes]).astype(jnp.bfloat16)
        encoder_sum[...] += dot(x[n], d_rows[...], 1, 1)

    base = 9 * width * width // 128
    for n in range(width // 128):
        lanes = slice(n * 128, (n + 1) * 128)
        parts[base + n * channels : base + (n + 1) * channels] = encoder_sum[:, lanes].astype(jnp.bfloat16)
    base += channels * width // 128
    for n in range(width // 128):
        parts[base + n * 8 : base + (n + 1) * 8] = gain_sum[:, n * 128 : (n + 1) * 128].astype(jnp.bfloat16)
    base += 8 * width // 128
    parts[base:] = jnp.zeros((parts.shape[0] - base, 128), jnp.bfloat16)


def middle(meta, own_a, own_b, got_a, got_b, encoder, kernels, gain, wide, back, part_rows):
    rows, cols, width = back.shape
    channels = encoder.shape[0]
    block, cells = kernels.shape[1:]
    patches = rows * cols // cells
    sources = SIDE * SIDE
    bf, f32 = jnp.bfloat16, jnp.float32
    anywhere = pl.BlockSpec(memory_space=pl.ANY)
    local = pl.BlockSpec(memory_space=pltpu.VMEM)
    column = jax.ShapeDtypeStruct((rows, 1, width), f32)
    return pl.pallas_call(
        middle_kernel,
        name="middle",
        out_shape=(
            jax.ShapeDtypeStruct((rows, cols, width), bf), column, column, jax.ShapeDtypeStruct((part_rows, 128), bf)
        ),
        in_specs=[pl.BlockSpec(memory_space=pltpu.SMEM)] + [anywhere] * 4 + [local] * 4 + [anywhere] * 2,
        out_specs=(local,) * 4,
        scratch_shapes=[
            pltpu.VMEM((sources, channels, MOST * block), bf),
            pltpu.VMEM((sources, width, MOST * block), f32),
            pltpu.VMEM((width, MOST * block), bf),
            pltpu.VMEM((patches, cells, width), f32),
            pltpu.VMEM((patches, width, cells), bf),
            pltpu.VMEM(wide.shape, bf),
            pltpu.VMEM(back.shape, f32),
            pltpu.VMEM((width, rows * cols), bf),
            pltpu.VMEM((width, MOST * block), bf),
            pltpu.VMEM((channels, width), f32),
            pltpu.VMEM((8, width), f32),
            pltpu.SemaphoreType.DMA((sources, MOST, 2)),
            pltpu.SemaphoreType.DMA((2,)),
        ],
        compiler_params=pltpu.CompilerParams(vmem_limit_bytes=VMEM_LIMIT),
    )(meta, own_a, own_b, got_a, got_b, encoder.T, kernels, kernels.swapaxes(1, 2), gain, wide, back)


PIECES = 16
PIECE_ROWS = 112
FLOWS = 6
HALVED = 12


def pairing(place, parity):
    near, far = place + 1 - 2 * (place % 2), (place + 3 - 2 * (place % 2)) % SIDE
    turn, high, low = (place + 1) // 2 % 2, place // 2, place % 2
    return ((near, turn), (far, high)) if parity == 0 else ((far, high), (near, low))


def sum_kernel(
    parts, normed, first, last, weight,
    conv_out, summed,
    own, other, total, outgoing, incoming, quarter_out, quarter_in, shared, result,
    tile, wide, held_weight, made, above, below, lefts, rights,
    halo_send, halo_recv, sends, recvs, local,
):
    lat, lon, y, z = position()
    x, core = lat // 2, lat % 2
    twin = (lat + 1 - 2 * core, lon)
    rows, cols, width = tile.shape
    _, _, up, down, left, right = halo_peers()

    def at_place(axis, place):
        if axis == 0:
            return (place * 2 + core, lon)
        return (lat, place * SIDE + z) if axis == 1 else (lat, y * SIDE + place)

    barrier = pltpu.get_barrier_semaphore()
    peers = [twin]
    for axis, place in enumerate((x, y, z)):
        peers += [at_place(axis, (place + step) % SIDE) for step in range(1, SIDE)]
    peers += [(lat, left), (lat, right)]
    peers += [(a, b) for a in (up, down) for b in (left, lon, right)]
    for peer in peers:
        pl.semaphore_signal(barrier, inc=1, device_id=peer, device_id_type=MESH)
    load_own = [pltpu.make_async_copy(parts.at[core, f], own.at[f], local.at[f]) for f in range(FLOWS)]
    load_tile = pltpu.make_async_copy(normed, tile, local.at[FLOWS])
    load_weight = pltpu.make_async_copy(weight, held_weight, local.at[FLOWS + 1])
    for copy in (load_tile, *load_own, load_weight):
        copy.start()
    pl.semaphore_wait(barrier, len(peers))

    halo = halo_copies(
        normed.at[0], normed.at[rows - 1], first, last, above, below, lefts, rights, halo_send, halo_recv
    )
    for copy in halo:
        copy.start()

    begun = []

    def remote(src, dst, flow, n, to):
        copy = pltpu.make_async_remote_copy(
            src_ref=src, dst_ref=dst, send_sem=sends.at[flow, n], recv_sem=recvs.at[flow, n],
            device_id=to, device_id_type=MESH,
        )
        copy.start()
        begun.append(copy)
        return copy

    places = (x, y, z)
    plans = []
    for f in range(FLOWS):
        turn, parity = f // 2, f % 2
        steps, base = [], 0
        for k, (partner, keep) in enumerate(pairing(places[turn], parity)):
            size = PIECES >> (k + 1)
            kept, sent = base + keep * size, base + (1 - keep) * size
            base = kept
            steps.append((at_place(turn, partner), size, kept, sent))
        plans.append((steps, (turn + 1) % 3, (turn + 2) % 3))

    crossing = [remote(parts.at[1 - core, f], other.at[f], f, 0, twin) for f in range(FLOWS)]

    load_tile.wait()
    for copy in halo:
        copy.wait()
    lay_windows(tile, above, below, lefts, rights, wide, False)
    load_weight.wait()
    step_rows = 4
    save = [pltpu.make_async_copy(made, conv_out, local.at[FLOWS + 2])]

    def convolve(chunk):
        value = jnp.zeros((step_rows * cols, width), jnp.float32)
        for a in range(3):
            window = wide[chunk * step_rows + a : chunk * step_rows + a + step_rows]
            value += dot(window.reshape(step_rows * cols, 3 * width), held_weight[a], 1, 0)
        made[chunk * step_rows : (chunk + 1) * step_rows] = value.astype(jnp.bfloat16).reshape(step_rows, cols, width)

    def halve(f, k):
        to, size, _, _ = plans[f][0][k]
        at = pl.ds((0, PIECES // 2)[k], size)
        return remote(outgoing.at[f, at], incoming.at[f, at], f, 1 + k, to)

    convolve(0)
    flying = []
    for f in range(FLOWS):
        _, size, kept, sent = plans[f][0][0]
        load_own[f].wait()
        crossing[f].wait_recv()

        @pl.loop(0, size)
        def _(i):
            total[f, kept + i] = own[f, kept + i].astype(jnp.float32) + other[f, kept + i].astype(jnp.float32)
            value = own[f, sent + i].astype(jnp.float32) + other[f, sent + i].astype(jnp.float32)
            outgoing[f, i] = value.astype(jnp.bfloat16)

        flying.append(halve(f, 0))
    for chunk in (1, 2, 3):
        convolve(chunk)
    for f in range(FLOWS):
        _, _, kept, _ = plans[f][0][0]
        _, size, keep_next, send_next = plans[f][0][1]
        flying[f].wait_recv()

        @pl.loop(0, size)
        def _(i):
            total[f, keep_next + i] += incoming[f, keep_next - kept + i].astype(jnp.float32)
            value = total[f, send_next + i] + incoming[f, send_next - kept + i].astype(jnp.float32)
            outgoing[f, PIECES // 2 + i] = value.astype(jnp.bfloat16)

        flying[f] = halve(f, 1)
    convolve(4)
    for f in range(FLOWS):
        steps, axis, _ = plans[f]
        base = steps[1][2]
        flying[f].wait_recv()
        flying[f] = []
        for step in range(1, SIDE):
            place = (places[axis] + step) % SIDE
            value = total[f, base + place] + incoming[f, PIECES // 2 + place].astype(jnp.float32)
            quarter_out[f, step - 1] = value.astype(jnp.bfloat16)
            flying[f].append(
                remote(quarter_out.at[f, step - 1], quarter_in.at[f, step - 1], f, 2 + step, at_place(axis, place))
            )
    convolve(5)
    save[0].start()
    for f in range(FLOWS):
        steps, axis, other_axis = plans[f]
        here, there = places[axis], places[other_axis]
        value = total[f, steps[1][2] + here] + incoming[f, PIECES // 2 + here].astype(jnp.float32)
        for step in range(1, SIDE):
            flying[f][step - 1].wait_recv()
            value += quarter_in[f, step - 1].astype(jnp.float32)
        shared[f, there] = value.astype(jnp.bfloat16)
        flying[f] = [
            remote(shared.at[f, there], shared.at[f, there], f, 5 + step, at_place(other_axis, (there + step) % SIDE))
            for step in range(1, SIDE)
        ]

    passed = []

    def pass_on(f, start, size, n):
        at = result.at[core, f, pl.ds(start, size)]
        passed.append(remote(at, at, f, n, twin))

    for f in range(FLOWS):
        steps, axis, _ = plans[f]
        mine = steps[1][2] + places[axis]
        for copy in flying[f]:
            copy.wait_recv()
        value = shared[f, 0].astype(jnp.float32)
        for place in range(1, SIDE):
            value += shared[f, place].astype(jnp.float32)
        result[core, f, mine] = value.astype(jnp.bfloat16)
        at = result.at[core, f, mine]
        flying[f] = [
            remote(at, at, f, 8 + step, at_place(axis, (places[axis] + step) % SIDE)) for step in range(1, SIDE)
        ]
    for k in (1, 0):
        for f in range(FLOWS):
            to, size, kept, _ = plans[f][0][k]
            for copy in flying[f]:
                copy.wait_recv()
            at = result.at[core, f, pl.ds(kept, size)]
            flying[f] = [remote(at, at, f, 13 - k, to)]
            if k == 1:
                pass_on(f, kept, size, 14)
            else:
                pass_on(f, plans[f][0][1][3], plans[f][0][1][1], 15)
    for f in range(FLOWS):
        _, size, _, sent = plans[f][0][0]
        flying[f][0].wait_recv()
        pass_on(f, sent, size, 16)
    for copy in passed:
        copy.wait_recv()
    stored = pltpu.make_async_copy(result, summed, local.at[FLOWS + 3])
    stored.start()
    for copy in begun:
        copy.wait_send()
    save[0].wait()
    stored.wait()


def sum_all(parts, normed, first, last, weight):
    rows, cols, width = normed.shape
    bf, f32 = jnp.bfloat16, jnp.float32
    anywhere = pl.BlockSpec(memory_space=pl.ANY)
    inside = pl.BlockSpec(memory_space=pltpu.VMEM)
    piece = (PIECE_ROWS, 128)
    parts = parts.reshape((2, FLOWS, PIECES) + piece)
    return pl.pallas_call(
        sum_kernel,
        name="sum_all",
        out_shape=(jax.ShapeDtypeStruct(normed.shape, bf), jax.ShapeDtypeStruct(parts.shape, bf)),
        in_specs=[anywhere, anywhere, inside, inside, anywhere],
        out_specs=(anywhere, anywhere),
        scratch_shapes=[
            pltpu.VMEM((FLOWS, PIECES) + piece, bf),
            pltpu.VMEM((FLOWS, PIECES) + piece, bf),
            pltpu.VMEM((FLOWS, PIECES) + piece, f32),
            pltpu.VMEM((FLOWS, HALVED) + piece, bf),
            pltpu.VMEM((FLOWS, HALVED) + piece, bf),
            pltpu.VMEM((FLOWS, SIDE - 1) + piece, bf),
            pltpu.VMEM((FLOWS, SIDE - 1) + piece, bf),
            pltpu.VMEM((FLOWS, SIDE) + piece, bf),
            pltpu.VMEM((2, FLOWS, PIECES) + piece, bf),
            pltpu.VMEM((rows, cols, width), bf),
            pltpu.VMEM((rows + 2, cols, 3 * width), bf),
            pltpu.VMEM(weight.shape, bf),
            pltpu.VMEM((rows, cols, width), bf),
            pltpu.VMEM((cols, width), bf),
            pltpu.VMEM((cols, width), bf),
            pltpu.VMEM((rows + 2, 1, width), f32),
            pltpu.VMEM((rows + 2, 1, width), f32),
            pltpu.SemaphoreType.DMA((8,)),
            pltpu.SemaphoreType.DMA((8,)),
            pltpu.SemaphoreType.DMA((FLOWS, 17)),
            pltpu.SemaphoreType.DMA((FLOWS, 17)),
            pltpu.SemaphoreType.DMA((FLOWS + 4,)),
        ],
        compiler_params=pltpu.CompilerParams(
            collective_id=1, has_side_effects=True, vmem_limit_bytes=VMEM_LIMIT
        ),
    )(parts, normed, first, last, weight)


def finish_kernel(scale, summed, conv_grad, encoder_grad, gain_grad, held, taps, encoder, sems):
    count, width = taps.shape[0], taps.shape[2]
    lanes = width // 128
    channels = encoder.shape[0]
    size = lanes * width
    base = count * size
    rest = channels * lanes + 8 * lanes

    def load(tap):
        at = pl.ds(pl.multiple_of(tap * size, size), size)
        return pltpu.make_async_copy(summed.at[at], held.at[at], sems.at[0, tap])

    def save(tap):
        return pltpu.make_async_copy(taps.at[tap], conv_grad.at[tap], sems.at[1, tap])

    last = pl.ds(base, rest)
    load_rest = pltpu.make_async_copy(summed.at[last], held.at[last], sems.at[0, count])
    for tap in range(count):
        load(tap).start()
    load_rest.start()

    @pl.loop(0, count)
    def _(tap):
        load(tap).wait()
        for n in range(lanes):
            at = pl.ds(pl.multiple_of(tap * size + n * width, width), width)
            taps[tap, :, n * 128 : (n + 1) * 128] = held[at].astype(jnp.float32) * scale
        save(tap).start()

    load_rest.wait()
    for n in range(lanes):
        at = slice(n * 128, (n + 1) * 128)
        encoder[:, at] = held[base + n * channels : base + (n + 1) * channels].astype(jnp.float32) * scale
        start = base + channels * lanes + n * 8
        gain_grad[:, at] = jnp.sum(held[start : start + 8].astype(jnp.float32), axis=0, keepdims=True) * scale
    save_encoder = pltpu.make_async_copy(encoder, encoder_grad, sems.at[1, count])
    save_encoder.start()

    @pl.loop(0, count)
    def _(tap):
        save(tap).wait()

    save_encoder.wait()


def finish(summed, scale, channels, width):
    f32 = jnp.float32
    anywhere = pl.BlockSpec(memory_space=pl.ANY)
    return pl.pallas_call(
        lambda *refs: finish_kernel(scale, *refs),
        name="finish",
        out_shape=(
            jax.ShapeDtypeStruct((9, width, width), f32),
            jax.ShapeDtypeStruct((channels, width), f32),
            jax.ShapeDtypeStruct((1, width), f32),
        ),
        in_specs=[anywhere],
        out_specs=(anywhere, anywhere, pl.BlockSpec(memory_space=pltpu.VMEM)),
        scratch_shapes=[
            pltpu.VMEM(summed.shape, jnp.bfloat16),
            pltpu.VMEM((9, width, width), f32),
            pltpu.VMEM((channels, width), f32),
            pltpu.SemaphoreType.DMA((2, 10)),
        ],
        compiler_params=pltpu.CompilerParams(vmem_limit_bytes=VMEM_LIMIT),
    )(summed)


def shards(spectra, target, patch, kernel, encoder_weight, kernels, gain, conv_weight, cotangent):
    tiles, bands = lax.axis_size("lon"), lax.axis_size("lat")
    rows, cols, width = cotangent.shape
    channels = spectra.shape[1]
    loss_scale = 1.0 / math.sqrt(rows * bands * cols * tiles)
    send_a, send_b, meta, first, last = pack(target, patch, kernel, spectra.T, cotangent, kernels.shape[1], tiles)
    meta = meta.reshape(tiles, 1, 128)
    weight = conv_weight.reshape(9, width, width)
    got_a, got_b, got_meta, wide, back = exchange(send_a, send_b, meta, cotangent, first, last, weight)
    part_rows = 192 * 112
    normed, first, last, parts = middle(
        got_meta.reshape(tiles, 128), send_a, send_b, got_a, got_b, encoder_weight, kernels,
        gain.reshape(1, width), wide, back, part_rows,
    )
    conv_out, summed = sum_all(parts, normed, first, last, conv_weight.reshape(3, 3 * width, width))
    conv_grad, encoder_grad, gain_grad = finish(summed.reshape(part_rows, 128), loss_scale, channels, width)
    return conv_out, conv_grad.reshape(3, 3, width, width), encoder_grad, gain_grad.reshape(width)


def solution(mesh):
    placed = (
        P(("lat", "lon"), None),
        P(("lat", "lon")),
        P(("lat", "lon")),
        P(("lat", "lon")),
        P(),
        P(),
        P(),
        P(),
        P("lat", "lon", None),
    )
    return jax.shard_map(
        shards,
        mesh=mesh,
        in_specs=placed,
        out_specs=(P("lat", "lon", None), P(), P(), P()),
        check_vma=False,
    )
```

```python
import math

import jax
import jax.numpy as jnp
from jax import lax
from jax.experimental import pallas as pl
from jax.experimental.pallas import tpu as pltpu
from jax.sharding import PartitionSpec as P

PH = 8
PW = 16
MOST = 3
SIDE = 4
MESH = pl.DeviceIdType.MESH
VMEM_LIMIT = 60 * 1024 * 1024
SOURCES = sorted(((dy, dz) for dy in range(SIDE) for dz in range(SIDE)), key=lambda o: (o.count(2), o))
GROUPS = (0, 9, 15, 16)


def dot(a, b, ca, cb):
    return lax.dot_general(a, b, (((ca,), (cb,)), ((), ())), preferred_element_type=jnp.float32)


def pack_kernel(
    target, patch, kernel, spectra, cot, to_a, to_b, meta, first, last,
    held, blank, near, far, block_in, counts, in_sems, out_sems,
):
    slots = block_in.shape[0]
    high, block = to_a.shape[3:]
    low = to_b.shape[3]
    rows, cols, _ = cot.shape
    fetch = pltpu.make_async_copy(spectra, held, in_sems.at[0])
    fetch.start()
    edges = [
        pltpu.make_async_copy(cot.at[:, pl.ds(0, 8)], near, in_sems.at[1]),
        pltpu.make_async_copy(cot.at[:, pl.ds(cols - 8, 8)], far, in_sems.at[2]),
    ]
    for edge in edges:
        edge.start()
    blank[...] = jnp.zeros_like(blank)

    @pl.loop(0, slots // MOST)
    def _(tile):
        counts[tile] = 0
        for rank in range(MOST):
            block_in[tile * MOST + rank] = -1
            meta[tile, rank] = -1
            meta[tile, MOST + rank] = 0

    @pl.loop(0, target.shape[0])
    def _(which):
        tile = target[which]
        rank = counts[tile]
        counts[tile] = rank + 1
        block_in[tile * MOST + rank] = which
        meta[tile, rank] = kernel[which]
        meta[tile, MOST + rank] = patch[which]

    fetch.wait()

    def pieces(slot, source):
        tile = slot // MOST
        rank = slot - tile * MOST
        y, z = tile // SIDE, tile % SIDE
        return (
            pltpu.make_async_copy(source(0, high), to_a.at[z, y, rank], out_sems.at[slot, 0]),
            pltpu.make_async_copy(source(high, low), to_b.at[y, z, rank], out_sems.at[slot, 1]),
        )

    @pl.loop(0, slots)
    def _(slot):
        which = block_in[slot]

        @pl.when(which >= 0)
        def _():
            lanes = pl.ds(pl.multiple_of(which * block, block), block)
            for piece in pieces(slot, lambda base, size: held.at[pl.ds(base, size), lanes]):
                piece.start()

        @pl.when(which < 0)
        def _():
            for piece in pieces(slot, lambda base, size: blank.at[pl.ds(0, size)]):
                piece.start()

    for edge in edges:
        edge.wait()

    @pl.loop(0, rows)
    def _(row):
        first[row] = near[row].astype(jnp.float32)[:1]
        last[row] = far[row].astype(jnp.float32)[7:]

    @pl.loop(0, slots)
    def _(slot):
        for piece in pieces(slot, lambda base, size: blank.at[pl.ds(0, size)]):
            piece.wait()


def pack(target, patch, kernel, flipped_spectra, cotangent, block, tiles):
    channels = flipped_spectra.shape[0]
    rows, _, width = cotangent.shape
    high = channels // 32 * 16
    low = channels - high
    slots = tiles * MOST
    bf, f32 = jnp.bfloat16, jnp.float32
    outs = [jax.ShapeDtypeStruct((SIDE, SIDE, MOST, size, block), bf) for size in (high, low)]
    outs.append(jax.ShapeDtypeStruct((tiles, 128), jnp.int32))
    outs += [jax.ShapeDtypeStruct((rows, 1, width), f32)] * 2
    anywhere = pl.BlockSpec(memory_space=pl.ANY)
    scalars = pl.BlockSpec(memory_space=pltpu.SMEM)
    inside = pl.BlockSpec(memory_space=pltpu.VMEM)
    return pl.pallas_call(
        pack_kernel,
        name="pack",
        out_shape=outs,
        in_specs=[scalars] * 3 + [anywhere] * 2,
        out_specs=(anywhere, anywhere, scalars, inside, inside),
        scratch_shapes=[
            pltpu.VMEM(flipped_spectra.shape, bf),
            pltpu.VMEM((max(high, low), block), bf),
            pltpu.VMEM((rows, 8, width), bf),
            pltpu.VMEM((rows, 8, width), bf),
            pltpu.SMEM((slots,), jnp.int32),
            pltpu.SMEM((tiles,), jnp.int32),
            pltpu.SemaphoreType.DMA((3,)),
            pltpu.SemaphoreType.DMA((slots, 2)),
        ],
        compiler_params=pltpu.CompilerParams(vmem_limit_bytes=VMEM_LIMIT),
    )(target, patch, kernel, flipped_spectra, cotangent)


def position():
    lat, lon = lax.axis_index("lat"), lax.axis_index("lon")
    return lat, lon, lon // SIDE, lon % SIDE


def halo_peers():
    lat, lon = lax.axis_index("lat"), lax.axis_index("lon")
    lats, lons = lax.axis_size("lat"), lax.axis_size("lon")
    up, down = (lat + lats - 1) % lats, (lat + 1) % lats
    left, right = (lon + lons - 1) % lons, (lon + 1) % lons
    return lat, lon, up, down, left, right


def halo_copies(top, bottom, first, last, from_above, from_below, from_left, from_right, sends, recvs):
    lat, lon, up, down, left, right = halo_peers()
    rows = first.shape[0]
    body = pl.ds(1, rows)
    plan = [
        (top, from_below, (up, lon)),
        (bottom, from_above, (down, lon)),
        (last, from_left.at[body], (lat, right)),
        (first, from_right.at[body], (lat, left)),
        (last.at[0], from_left.at[rows + 1], (up, right)),
        (last.at[rows - 1], from_left.at[0], (down, right)),
        (first.at[0], from_right.at[rows + 1], (up, left)),
        (first.at[rows - 1], from_right.at[0], (down, left)),
    ]
    return [
        pltpu.make_async_remote_copy(
            src_ref=src, dst_ref=dst, send_sem=sends.at[n], recv_sem=recvs.at[n], device_id=to, device_id_type=MESH
        )
        for n, (src, dst, to) in enumerate(plan)
    ]


def lay_windows(tile, from_above, from_below, from_left, from_right, wide, reverse):
    lat, lats = lax.axis_index("lat"), lax.axis_size("lat")
    rows, cols, width = tile.shape
    index = lax.broadcasted_iota(jnp.int32, (cols, width), 0)

    def lay(at, center, keep):
        value = center.astype(jnp.float32)
        before = jnp.where(index == 0, from_left[at], pltpu.roll(value, 1, 0))
        after = jnp.where(index == cols - 1, from_right[at], pltpu.roll(value, cols - 1, 0))
        if keep is not None:
            before, value, after = (jnp.where(keep, v, 0.0) for v in (before, value, after))
        order = (after, value, before) if reverse else (before, value, after)
        for n, v in enumerate(order):
            wide[at, :, n * width : (n + 1) * width] = v.astype(jnp.bfloat16)

    @pl.loop(0, rows)
    def _(row):
        lay(row + 1, tile[row], None)

    lay(0, from_above[...], lat > 0)
    lay(rows + 1, from_below[...], lat < lats - 1)


def exchange_kernel(
    send_a, send_b, meta, cot, first, last, weight, encoder_in, kernels_in,
    got_a, got_b, got_meta, wide_out, back_out, encoded_out, slope_out, turned_out, mid_a, mid_b, relay_a, relay_b,
    tile, wide, held_weight, back, above, below, lefts, rights, encoder, flat, table, turned, x, encoded, slope,
    halo_send, halo_recv, meta_send, meta_recv, sends, recvs, local, x_sems, out_sems,
):
    lat, lon, y, z = position()
    lats = lax.axis_size("lat")
    count = lax.axis_size("lon")
    _, _, up, down, left, right = halo_peers()
    rows, cols, width = tile.shape
    high, block = send_a.shape[3:]
    channels = x.shape[1]

    barrier = pltpu.get_barrier_semaphore()
    for step in range(1, SIDE * SIDE):
        peer = (lon + step) % count
        pl.semaphore_signal(barrier, inc=1, device_id=(lat, peer), device_id_type=MESH)
    for other in (up, down):
        for peer in (left, lon, right):
            pl.semaphore_signal(barrier, inc=1, device_id=(other, peer), device_id_type=MESH)
    load_tile = pltpu.make_async_copy(cot, tile, local.at[0])
    load_weight = pltpu.make_async_copy(weight, held_weight, local.at[1])
    load_tile.start()
    load_weight.start()
    own_meta = pltpu.make_async_copy(meta.at[lon], got_meta.at[0], local.at[2])
    own_meta.start()
    load_encoder = pltpu.make_async_copy(encoder_in, flat, local.at[5])
    load_kernels = pltpu.make_async_copy(kernels_in, table, local.at[6])
    load_encoder.start()
    load_kernels.start()

    def fetch(at, rank, from_a, from_b):
        lanes = pl.ds(rank * block, block)
        return (
            pltpu.make_async_copy(from_a.at[rank], x.at[at, pl.ds(0, high), lanes], x_sems.at[at, rank, 0]),
            pltpu.make_async_copy(from_b.at[rank], x.at[at, pl.ds(high, channels - high), lanes], x_sems.at[at, rank, 1]),
        )

    def bring(at, from_a, from_b):
        for rank in range(MOST):
            for copy in fetch(at, rank, from_a, from_b):
                copy.start()

    bring(0, send_a.at[z, y], send_b.at[y, z])
    pl.semaphore_wait(barrier, SIDE * SIDE - 1 + 6)

    halo = halo_copies(
        cot.at[0], cot.at[rows - 1], first, last, above, below, lefts, rights, halo_send, halo_recv
    )
    for copy in halo:
        copy.start()
    notes = []
    for dy in range(SIDE):
        for dz in range(SIDE):
            if dy or dz:
                n = SOURCES.index((dy, dz))
                to = (y + dy) % SIDE * SIDE + (z + dz) % SIDE
                notes.append(
                    pltpu.make_async_remote_copy(
                        src_ref=meta.at[to], dst_ref=got_meta.at[n], send_sem=meta_send.at[n],
                        recv_sem=meta_recv.at[n], device_id=(lat, to), device_id_type=MESH,
                    )
                )
    for copy in notes:
        copy.start()

    flows = []
    for flow, (src, mid, relay, got, u, v) in enumerate(
        ((send_a, mid_a, relay_a, got_a, z, y), (send_b, mid_b, relay_b, got_b, y, z))
    ):
        made = []

        def make(src_ref, dst_ref, du, dv, flow=flow, made=made, u=u, v=v):
            n = len(made)
            uu, vv = (u + du) % SIDE, (v + dv) % SIDE
            to = vv * SIDE + uu if flow == 0 else uu * SIDE + vv
            copy = pltpu.make_async_remote_copy(
                src_ref=src_ref, dst_ref=dst_ref, send_sem=sends.at[flow, n], recv_sem=recvs.at[flow, n],
                device_id=(lat, to), device_id_type=MESH,
            )
            made.append(copy)
            return copy

        def land(g, e, mid=mid, got=got):
            return got.at[0, e] if g == 0 else mid.at[g, e]

        def part(g, e, src=src, mid=mid, u=u, v=v):
            return src.at[u, (v + g) % SIDE] if e == 0 else mid.at[g, e]

        f = {"made": made}
        for d, sign in ((0, 1), (1, -1)):
            for j in range(2):
                g = 2 * d + j
                f["q1", d, j] = make(src.at[(u + 2) % SIDE, (v + g) % SIDE], relay.at[0, d, j], sign, 0)
                f["r1", d, j] = make(relay.at[0, d, j], land(g, 2), sign, 0)
            for g in range(SIDE):
                f["d1", d, g] = make(src.at[(u + sign) % SIDE, (v + g) % SIDE], land(g, 1 if d == 0 else 3), sign, 0)
            for e in range(SIDE):
                g = 1 if d == 0 else 3
                f["d2", d, e] = make(part(g, e), got.at[g, e], 0, sign)
            for j in range(2):
                e = ((0, 1), (3, 2))[d][j]
                f["q2", d, j] = make(part(2, e), relay.at[1, d, j], 0, sign)
                f["r2", d, j] = make(relay.at[1, d, j], got.at[2, e], 0, sign)
        flows.append(f)

    def start(*keys):
        for key in keys:
            for f in flows:
                f[key].start()

    def arrived(*keys):
        for key in keys:
            for f in flows:
                f[key].wait_recv()

    start(("q1", 0, 1), ("q1", 1, 0), ("q1", 0, 0), ("q1", 1, 1))
    for g in (2, 1, 3, 0):
        start(("d1", 0, g), ("d1", 1, g))

    load_tile.wait()
    for copy in halo:
        copy.wait()
    lay_windows(tile, above, below, lefts, rights, wide, True)
    save_wide = pltpu.make_async_copy(wide, wide_out, local.at[3])
    save_wide.start()
    load_weight.wait()
    step_rows = 4

    @pl.loop(0, rows // step_rows)
    def _(chunk):
        total = jnp.zeros((step_rows * cols, width), jnp.float32)
        for a in range(3):
            for b in range(3):
                window = wide[pl.ds(chunk * step_rows + 2 - a, step_rows), :, b * width : (b + 1) * width]
                total += dot(window.reshape(step_rows * cols, width), held_weight[a * 3 + b], 1, 1)
        back[pl.ds(chunk * step_rows, step_rows)] = total.reshape(step_rows, cols, width)

    save_back = pltpu.make_async_copy(back, back_out, local.at[4])
    save_back.start()
    load_encoder.wait()
    encoder[...] = flat[...].T
    load_kernels.wait()
    for n in range(table.shape[0]):
        turned[n] = table[n].T
    save_turned = pltpu.make_async_copy(turned, turned_out, local.at[7])
    save_turned.start()

    def landed(f, stage, e):
        if stage == 0:
            return f[{1: ("d1", 0, 0), 3: ("d1", 1, 0), 2: ("r1", 0, 0)}[e]]
        if stage == 2:
            return f[{0: ("r2", 0, 0), 1: ("r2", 0, 1), 3: ("r2", 1, 0), 2: ("r2", 1, 1)}[e]]
        return f["d2", stage // 2, e]

    def save(at):
        return (
            pltpu.make_async_copy(encoded.at[at], encoded_out.at[at], out_sems.at[at, 0]),
            pltpu.make_async_copy(slope.at[at], slope_out.at[at], out_sems.at[at, 1]),
        )

    def encode(group):
        for at in range(GROUPS[group], GROUPS[group + 1]):
            dy, dz = SOURCES[at]
            if at:
                landed(flows[0], dy, dz).wait_recv()
                landed(flows[1], dz, dy).wait_recv()
                bring(at, got_a.at[dy, dz], got_b.at[dz, dy])

        @pl.loop(GROUPS[group], GROUPS[group + 1])
        def _(at):
            for rank in range(MOST):
                for copy in fetch(at, rank, got_a.at[0, 0], got_b.at[0, 0]):
                    copy.wait()
            pre = dot(encoder[...], x[at], 1, 0)
            logistic = 0.5 * jnp.tanh(0.5 * pre) + 0.5
            encoded[at] = (pre * logistic).astype(jnp.bfloat16)
            slope[at] = logistic * (1.0 + pre * (1.0 - logistic))
            for copy in save(at):
                copy.start()

    for d, j in ((0, 1), (1, 0), (0, 0), (1, 1)):
        arrived(("q1", d, j))
        start(("r1", d, j))
    start(("q2", 0, 0), ("d2", 0, 0), ("d2", 1, 0))
    for g in (2, 1, 3):
        arrived(("d1", 0, g), ("d1", 1, g))
        if g == 2:
            start(("q2", 0, 1), ("q2", 1, 0))
        if g == 1:
            start(("d2", 0, 1), ("d2", 0, 3))
        if g == 3:
            start(("d2", 1, 1), ("d2", 1, 3))
    arrived(("r1", 1, 0))
    start(("q2", 1, 1))
    arrived(("r1", 0, 1), ("r1", 1, 1))
    arrived(("q2", 0, 0))
    start(("r2", 0, 0))
    arrived(("q2", 0, 1), ("q2", 1, 0))
    start(("r2", 0, 1), ("r2", 1, 0))
    start(("d2", 0, 2), ("d2", 1, 2))
    encode(0)
    arrived(("q2", 1, 1))
    start(("r2", 1, 1))
    encode(1)
    encode(2)
    for f in flows:
        for copy in f["made"]:
            copy.wait_send()
    for copy in notes:
        copy.wait()
    own_meta.wait()
    save_wide.wait()
    save_back.wait()
    save_turned.wait()

    @pl.loop(0, len(SOURCES))
    def _(at):
        for copy in save(at):
            copy.wait()


def exchange(send_a, send_b, meta, cotangent, first, last, weight, encoder, kernels):
    rows, cols, width = cotangent.shape
    lon = SIDE * SIDE
    channels = encoder.shape[0]
    observed = MOST * send_a.shape[4]
    bf, f32 = jnp.bfloat16, jnp.float32
    anywhere = pl.BlockSpec(memory_space=pl.ANY)
    whole = [jax.ShapeDtypeStruct(a.shape, bf) for a in (send_a, send_b)]
    relay = [jax.ShapeDtypeStruct((2, 2, 2) + a.shape[2:], bf) for a in (send_a, send_b)]
    out = pl.pallas_call(
        exchange_kernel,
        name="exchange",
        out_shape=(
            *whole, jax.ShapeDtypeStruct(meta.shape, meta.dtype),
            jax.ShapeDtypeStruct((rows + 2, cols, 3 * width), bf), jax.ShapeDtypeStruct((rows, cols, width), f32),
            jax.ShapeDtypeStruct((lon, width, observed), bf), jax.ShapeDtypeStruct((lon, width, observed), f32),
            jax.ShapeDtypeStruct(kernels.shape, bf),
            *whole, *relay,
        ),
        in_specs=[anywhere] * 9,
        out_specs=(anywhere,) * 12,
        scratch_shapes=[
            pltpu.VMEM((rows, cols, width), bf),
            pltpu.VMEM((rows + 2, cols, 3 * width), bf),
            pltpu.VMEM(weight.shape, bf),
            pltpu.VMEM((rows, cols, width), f32),
            pltpu.VMEM((cols, width), bf),
            pltpu.VMEM((cols, width), bf),
            pltpu.VMEM((rows + 2, 1, width), f32),
            pltpu.VMEM((rows + 2, 1, width), f32),
            pltpu.VMEM((width, channels), bf),
            pltpu.VMEM((channels, width), bf),
            pltpu.VMEM(kernels.shape, bf),
            pltpu.VMEM(kernels.shape, bf),
            pltpu.VMEM((lon, channels, observed), bf),
            pltpu.VMEM((lon, width, observed), bf),
            pltpu.VMEM((lon, width, observed), f32),
            pltpu.SemaphoreType.DMA((8,)),
            pltpu.SemaphoreType.DMA((8,)),
            pltpu.SemaphoreType.DMA((lon,)),
            pltpu.SemaphoreType.DMA((lon,)),
            pltpu.SemaphoreType.DMA((2, 32)),
            pltpu.SemaphoreType.DMA((2, 32)),
            pltpu.SemaphoreType.DMA((8,)),
            pltpu.SemaphoreType.DMA((lon, MOST, 2)),
            pltpu.SemaphoreType.DMA((lon, 2)),
        ],
        compiler_params=pltpu.CompilerParams(
            collective_id=0, has_side_effects=True, vmem_limit_bytes=VMEM_LIMIT
        ),
    )(send_a, send_b, meta, cotangent, first, last, weight, encoder, kernels)
    return out[:8]


def middle_kernel(
    meta, own_a, own_b, got_a, got_b, turned, gain, wide_in, back_in, encoded_in, slope_in,
    normed, first, last, parts,
    x, slope, encoded, spread, d_spread, wide, back, flipped, d_rows, encoder_sum, gain_sum,
    x_sems, pair_sems, local,
):
    lat, lon, y, z = position()
    rows, cols, width = normed.shape
    channels = x.shape[1]
    high, block = own_a.shape[3:]
    sources = SIDE * SIDE

    def fetch(n, rank, from_a, from_b):
        lanes = pl.ds(rank * block, block)
        return (
            pltpu.make_async_copy(from_a.at[rank], x.at[n, pl.ds(0, high), lanes], x_sems.at[n, rank, 0]),
            pltpu.make_async_copy(from_b.at[rank], x.at[n, pl.ds(high, channels - high), lanes], x_sems.at[n, rank, 1]),
        )

    def load_encoded(n):
        return pltpu.make_async_copy(encoded_in.at[n], encoded.at[n], pair_sems.at[n, 0])

    def load_slope(n):
        return pltpu.make_async_copy(slope_in.at[n], slope.at[n], pair_sems.at[n, 1])

    load_back = pltpu.make_async_copy(back_in, back, local.at[0])
    load_wide = pltpu.make_async_copy(wide_in, wide, local.at[1])
    for n in range(sources):
        load_encoded(n).start()
    load_back.start()
    load_wide.start()
    for n, (dy, dz) in enumerate(SOURCES):
        from_a = own_a.at[z, y] if n == 0 else got_a.at[dy, dz]
        from_b = own_b.at[y, z] if n == 0 else got_b.at[dz, dy]
        for rank in range(MOST):
            for copy in fetch(n, rank, from_a, from_b):
                copy.start()
        load_slope(n).start()
    spread[...] = jnp.zeros_like(spread)

    @pl.loop(0, sources)
    def _(n):
        load_encoded(n).wait()
        for rank in range(MOST):
            which, patch = meta[n, rank], meta[n, MOST + rank]

            @pl.when(which >= 0)
            def _():
                spread[patch] += dot(turned[which], encoded[n, :, rank * block : (rank + 1) * block], 1, 1)

    load_back.wait()
    gain_sum[...] = jnp.zeros_like(gain_sum)
    across = cols // PW

    @pl.loop(0, spread.shape[0])
    def _(q):
        at = (pl.ds(q // across * PH, PH), pl.ds(pl.multiple_of(q % across * PW, PW), PW))
        value = spread[q]
        scale = lax.rsqrt(jnp.mean(value * value, axis=1, keepdims=True) + 1e-06)
        unit = value * scale
        weight = gain[...]
        normed[at] = (unit * weight).astype(jnp.bfloat16).reshape(PH, PW, width)
        given = back[at].reshape(PH * PW, width)
        product = given * unit
        gain_sum[...] += jnp.sum(product.reshape(PH * PW // 8, 8, width), axis=0)
        inner = jnp.mean(product * weight, axis=1, keepdims=True)
        d_spread[q] = (scale * (given * weight - unit * inner)).astype(jnp.bfloat16).T

    step_rows = 4

    @pl.loop(0, rows // step_rows)
    def _(n):
        some = normed[pl.ds(n * step_rows, step_rows)].reshape(step_rows * cols, width)
        flipped[:, pl.ds(pl.multiple_of(n * step_rows * cols, 128), step_rows * cols)] = some.T

    @pl.loop(0, rows)
    def _(row):
        some = normed[row].astype(jnp.float32)
        first[row] = some[:1]
        last[row] = some[cols - 1 :]

    load_wide.wait()
    for a in range(3):

        @pl.loop(0, 3 * width // 256)
        def _(j):
            window = wide[2 - a : 2 - a + rows, :, pl.ds(pl.multiple_of(j * 256, 256), 256)]
            got = dot(flipped[...], window.reshape(rows * cols, 256), 1, 0).astype(jnp.bfloat16)
            base = pl.multiple_of((a * (3 * width // 128) + 2 * j) * width, width)
            parts[pl.ds(base, width)] = got[:, :128]
            parts[pl.ds(pl.multiple_of(base + width, width), width)] = got[:, 128:]

    encoder_sum[...] = jnp.zeros_like(encoder_sum)

    @pl.loop(0, sources)
    def _(n):
        for rank in range(MOST):
            for copy in fetch(n, rank, got_a.at[0, 0], got_b.at[0, 0]):
                copy.wait()
        load_slope(n).wait()
        for rank in range(MOST):
            which, patch = jnp.maximum(meta[n, rank], 0), meta[n, MOST + rank]
            lanes = slice(rank * block, (rank + 1) * block)
            here = dot(d_spread[patch], turned[which], 1, 0).astype(jnp.bfloat16).astype(jnp.float32)
            d_rows[:, lanes] = (here * slope[n, :, lanes]).astype(jnp.bfloat16)
        encoder_sum[...] += dot(x[n], d_rows[...], 1, 1)

    base = 9 * width * width // 128
    for n in range(width // 128):
        lanes = slice(n * 128, (n + 1) * 128)
        parts[base + n * channels : base + (n + 1) * channels] = encoder_sum[:, lanes].astype(jnp.bfloat16)
    base += channels * width // 128
    for n in range(width // 128):
        parts[base + n * 8 : base + (n + 1) * 8] = gain_sum[:, n * 128 : (n + 1) * 128].astype(jnp.bfloat16)
    base += 8 * width // 128
    parts[base:] = jnp.zeros((parts.shape[0] - base, 128), jnp.bfloat16)


def middle(meta, own_a, own_b, got_a, got_b, turned, gain, wide, back, encoded, slope, channels, part_rows):
    rows, cols, width = back.shape
    cells, block = turned.shape[1:]
    patches = rows * cols // cells
    sources = SIDE * SIDE
    bf, f32 = jnp.bfloat16, jnp.float32
    anywhere = pl.BlockSpec(memory_space=pl.ANY)
    local = pl.BlockSpec(memory_space=pltpu.VMEM)
    column = jax.ShapeDtypeStruct((rows, 1, width), f32)
    return pl.pallas_call(
        middle_kernel,
        name="middle",
        out_shape=(
            jax.ShapeDtypeStruct((rows, cols, width), bf), column, column, jax.ShapeDtypeStruct((part_rows, 128), bf)
        ),
        in_specs=[pl.BlockSpec(memory_space=pltpu.SMEM)] + [anywhere] * 4 + [local] * 2 + [anywhere] * 4,
        out_specs=(local,) * 4,
        scratch_shapes=[
            pltpu.VMEM((sources, channels, MOST * block), bf),
            pltpu.VMEM((sources, width, MOST * block), f32),
            pltpu.VMEM((sources, width, MOST * block), bf),
            pltpu.VMEM((patches, cells, width), f32),
            pltpu.VMEM((patches, width, cells), bf),
            pltpu.VMEM(wide.shape, bf),
            pltpu.VMEM(back.shape, f32),
            pltpu.VMEM((width, rows * cols), bf),
            pltpu.VMEM((width, MOST * block), bf),
            pltpu.VMEM((channels, width), f32),
            pltpu.VMEM((8, width), f32),
            pltpu.SemaphoreType.DMA((sources, MOST, 2)),
            pltpu.SemaphoreType.DMA((sources, 2)),
            pltpu.SemaphoreType.DMA((2,)),
        ],
        compiler_params=pltpu.CompilerParams(vmem_limit_bytes=VMEM_LIMIT),
    )(meta, own_a, own_b, got_a, got_b, turned, gain, wide, back, encoded, slope)


PIECES = 16
PIECE_ROWS = 112
FLOWS = 6
HALVED = 12


def pairing(place, parity):
    near, far = place + 1 - 2 * (place % 2), (place + 3 - 2 * (place % 2)) % SIDE
    turn, high, low = (place + 1) // 2 % 2, place // 2, place % 2
    return ((near, turn), (far, high)) if parity == 0 else ((far, high), (near, low))


def sum_kernel(
    parts, normed, first, last, weight,
    conv_out, summed,
    own, other, total, outgoing, incoming, quarter_out, quarter_in, shared, result,
    tile, wide, held_weight, made, above, below, lefts, rights,
    halo_send, halo_recv, sends, recvs, local,
):
    lat, lon, y, z = position()
    x, core = lat // 2, lat % 2
    twin = (lat + 1 - 2 * core, lon)
    rows, cols, width = tile.shape
    _, _, up, down, left, right = halo_peers()

    def at_place(axis, place):
        if axis == 0:
            return (place * 2 + core, lon)
        return (lat, place * SIDE + z) if axis == 1 else (lat, y * SIDE + place)

    barrier = pltpu.get_barrier_semaphore()
    peers = [twin]
    for axis, place in enumerate((x, y, z)):
        peers += [at_place(axis, (place + step) % SIDE) for step in range(1, SIDE)]
    peers += [(lat, left), (lat, right)]
    peers += [(a, b) for a in (up, down) for b in (left, lon, right)]
    for peer in peers:
        pl.semaphore_signal(barrier, inc=1, device_id=peer, device_id_type=MESH)
    load_own = [pltpu.make_async_copy(parts.at[core, f], own.at[f], local.at[f]) for f in range(FLOWS)]
    load_tile = pltpu.make_async_copy(normed, tile, local.at[FLOWS])
    load_weight = pltpu.make_async_copy(weight, held_weight, local.at[FLOWS + 1])
    for copy in (load_tile, *load_own, load_weight):
        copy.start()
    pl.semaphore_wait(barrier, len(peers))

    halo = halo_copies(
        normed.at[0], normed.at[rows - 1], first, last, above, below, lefts, rights, halo_send, halo_recv
    )
    for copy in halo:
        copy.start()

    begun = []

    def remote(src, dst, flow, n, to):
        copy = pltpu.make_async_remote_copy(
            src_ref=src, dst_ref=dst, send_sem=sends.at[flow, n], recv_sem=recvs.at[flow, n],
            device_id=to, device_id_type=MESH,
        )
        copy.start()
        begun.append(copy)
        return copy

    places = (x, y, z)
    plans = []
    for f in range(FLOWS):
        turn, parity = f // 2, f % 2
        steps, base = [], 0
        for k, (partner, keep) in enumerate(pairing(places[turn], parity)):
            size = PIECES >> (k + 1)
            kept, sent = base + keep * size, base + (1 - keep) * size
            base = kept
            steps.append((at_place(turn, partner), size, kept, sent))
        plans.append((steps, (turn + 1) % 3, (turn + 2) % 3))

    crossing = [remote(parts.at[1 - core, f], other.at[f], f, 0, twin) for f in range(FLOWS)]

    load_tile.wait()
    for copy in halo:
        copy.wait()
    lay_windows(tile, above, below, lefts, rights, wide, False)
    load_weight.wait()
    step_rows = 4
    save = [pltpu.make_async_copy(made, conv_out, local.at[FLOWS + 2])]

    def convolve(chunk):
        value = jnp.zeros((step_rows * cols, width), jnp.float32)
        for a in range(3):
            window = wide[chunk * step_rows + a : chunk * step_rows + a + step_rows]
            value += dot(window.reshape(step_rows * cols, 3 * width), held_weight[a], 1, 0)
        made[chunk * step_rows : (chunk + 1) * step_rows] = value.astype(jnp.bfloat16).reshape(step_rows, cols, width)

    def halve(f, k):
        to, size, _, _ = plans[f][0][k]
        at = pl.ds((0, PIECES // 2)[k], size)
        return remote(outgoing.at[f, at], incoming.at[f, at], f, 1 + k, to)

    convolve(0)
    flying = []
    for f in range(FLOWS):
        _, size, kept, sent = plans[f][0][0]
        load_own[f].wait()
        crossing[f].wait_recv()

        @pl.loop(0, size)
        def _(i):
            total[f, kept + i] = own[f, kept + i].astype(jnp.float32) + other[f, kept + i].astype(jnp.float32)
            value = own[f, sent + i].astype(jnp.float32) + other[f, sent + i].astype(jnp.float32)
            outgoing[f, i] = value.astype(jnp.bfloat16)

        flying.append(halve(f, 0))
    for chunk in (1, 2, 3):
        convolve(chunk)
    for f in range(FLOWS):
        _, _, kept, _ = plans[f][0][0]
        _, size, keep_next, send_next = plans[f][0][1]
        flying[f].wait_recv()

        @pl.loop(0, size)
        def _(i):
            total[f, keep_next + i] += incoming[f, keep_next - kept + i].astype(jnp.float32)
            value = total[f, send_next + i] + incoming[f, send_next - kept + i].astype(jnp.float32)
            outgoing[f, PIECES // 2 + i] = value.astype(jnp.bfloat16)

        flying[f] = halve(f, 1)
    convolve(4)
    for f in range(FLOWS):
        steps, axis, _ = plans[f]
        base = steps[1][2]
        flying[f].wait_recv()
        flying[f] = []
        for step in range(1, SIDE):
            place = (places[axis] + step) % SIDE
            value = total[f, base + place] + incoming[f, PIECES // 2 + place].astype(jnp.float32)
            quarter_out[f, step - 1] = value.astype(jnp.bfloat16)
            flying[f].append(
                remote(quarter_out.at[f, step - 1], quarter_in.at[f, step - 1], f, 2 + step, at_place(axis, place))
            )
    convolve(5)
    save[0].start()
    for f in range(FLOWS):
        steps, axis, other_axis = plans[f]
        here, there = places[axis], places[other_axis]
        value = total[f, steps[1][2] + here] + incoming[f, PIECES // 2 + here].astype(jnp.float32)
        for step in range(1, SIDE):
            flying[f][step - 1].wait_recv()
            value += quarter_in[f, step - 1].astype(jnp.float32)
        shared[f, there] = value.astype(jnp.bfloat16)
        flying[f] = [
            remote(shared.at[f, there], shared.at[f, there], f, 5 + step, at_place(other_axis, (there + step) % SIDE))
            for step in range(1, SIDE)
        ]

    passed = []

    def pass_on(f, start, size, n):
        at = result.at[core, f, pl.ds(start, size)]
        passed.append(remote(at, at, f, n, twin))

    for f in range(FLOWS):
        steps, axis, _ = plans[f]
        mine = steps[1][2] + places[axis]
        for copy in flying[f]:
            copy.wait_recv()
        value = shared[f, 0].astype(jnp.float32)
        for place in range(1, SIDE):
            value += shared[f, place].astype(jnp.float32)
        result[core, f, mine] = value.astype(jnp.bfloat16)
        at = result.at[core, f, mine]
        flying[f] = [
            remote(at, at, f, 8 + step, at_place(axis, (places[axis] + step) % SIDE)) for step in range(1, SIDE)
        ]
    for k in (1, 0):
        for f in range(FLOWS):
            to, size, kept, _ = plans[f][0][k]
            for copy in flying[f]:
                copy.wait_recv()
            at = result.at[core, f, pl.ds(kept, size)]
            flying[f] = [remote(at, at, f, 13 - k, to)]
            if k == 1:
                pass_on(f, kept, size, 14)
            else:
                pass_on(f, plans[f][0][1][3], plans[f][0][1][1], 15)
    for f in range(FLOWS):
        _, size, _, sent = plans[f][0][0]
        flying[f][0].wait_recv()
        pass_on(f, sent, size, 16)
    for copy in passed:
        copy.wait_recv()
    stored = pltpu.make_async_copy(result, summed, local.at[FLOWS + 3])
    stored.start()
    for copy in begun:
        copy.wait_send()
    save[0].wait()
    stored.wait()


def sum_all(parts, normed, first, last, weight):
    rows, cols, width = normed.shape
    bf, f32 = jnp.bfloat16, jnp.float32
    anywhere = pl.BlockSpec(memory_space=pl.ANY)
    inside = pl.BlockSpec(memory_space=pltpu.VMEM)
    piece = (PIECE_ROWS, 128)
    parts = parts.reshape((2, FLOWS, PIECES) + piece)
    return pl.pallas_call(
        sum_kernel,
        name="sum_all",
        out_shape=(jax.ShapeDtypeStruct(normed.shape, bf), jax.ShapeDtypeStruct(parts.shape, bf)),
        in_specs=[anywhere, anywhere, inside, inside, anywhere],
        out_specs=(anywhere, anywhere),
        scratch_shapes=[
            pltpu.VMEM((FLOWS, PIECES) + piece, bf),
            pltpu.VMEM((FLOWS, PIECES) + piece, bf),
            pltpu.VMEM((FLOWS, PIECES) + piece, f32),
            pltpu.VMEM((FLOWS, HALVED) + piece, bf),
            pltpu.VMEM((FLOWS, HALVED) + piece, bf),
            pltpu.VMEM((FLOWS, SIDE - 1) + piece, bf),
            pltpu.VMEM((FLOWS, SIDE - 1) + piece, bf),
            pltpu.VMEM((FLOWS, SIDE) + piece, bf),
            pltpu.VMEM((2, FLOWS, PIECES) + piece, bf),
            pltpu.VMEM((rows, cols, width), bf),
            pltpu.VMEM((rows + 2, cols, 3 * width), bf),
            pltpu.VMEM(weight.shape, bf),
            pltpu.VMEM((rows, cols, width), bf),
            pltpu.VMEM((cols, width), bf),
            pltpu.VMEM((cols, width), bf),
            pltpu.VMEM((rows + 2, 1, width), f32),
            pltpu.VMEM((rows + 2, 1, width), f32),
            pltpu.SemaphoreType.DMA((8,)),
            pltpu.SemaphoreType.DMA((8,)),
            pltpu.SemaphoreType.DMA((FLOWS, 17)),
            pltpu.SemaphoreType.DMA((FLOWS, 17)),
            pltpu.SemaphoreType.DMA((FLOWS + 4,)),
        ],
        compiler_params=pltpu.CompilerParams(
            collective_id=1, has_side_effects=True, vmem_limit_bytes=VMEM_LIMIT
        ),
    )(parts, normed, first, last, weight)


def finish_kernel(scale, summed, conv_grad, encoder_grad, gain_grad, held, taps, encoder, sems):
    count, width = taps.shape[0], taps.shape[2]
    lanes = width // 128
    channels = encoder.shape[0]
    size = lanes * width
    base = count * size
    rest = channels * lanes + 8 * lanes

    def load(tap):
        at = pl.ds(pl.multiple_of(tap * size, size), size)
        return pltpu.make_async_copy(summed.at[at], held.at[at], sems.at[0, tap])

    def save(tap):
        return pltpu.make_async_copy(taps.at[tap], conv_grad.at[tap], sems.at[1, tap])

    last = pl.ds(base, rest)
    load_rest = pltpu.make_async_copy(summed.at[last], held.at[last], sems.at[0, count])
    for tap in range(count):
        load(tap).start()
    load_rest.start()

    @pl.loop(0, count)
    def _(tap):
        load(tap).wait()
        for n in range(lanes):
            at = pl.ds(pl.multiple_of(tap * size + n * width, width), width)
            taps[tap, :, n * 128 : (n + 1) * 128] = held[at].astype(jnp.float32) * scale
        save(tap).start()

    load_rest.wait()
    for n in range(lanes):
        at = slice(n * 128, (n + 1) * 128)
        encoder[:, at] = held[base + n * channels : base + (n + 1) * channels].astype(jnp.float32) * scale
        start = base + channels * lanes + n * 8
        gain_grad[:, at] = jnp.sum(held[start : start + 8].astype(jnp.float32), axis=0, keepdims=True) * scale
    save_encoder = pltpu.make_async_copy(encoder, encoder_grad, sems.at[1, count])
    save_encoder.start()

    @pl.loop(0, count)
    def _(tap):
        save(tap).wait()

    save_encoder.wait()


def finish(summed, scale, channels, width):
    f32 = jnp.float32
    anywhere = pl.BlockSpec(memory_space=pl.ANY)
    return pl.pallas_call(
        lambda *refs: finish_kernel(scale, *refs),
        name="finish",
        out_shape=(
            jax.ShapeDtypeStruct((9, width, width), f32),
            jax.ShapeDtypeStruct((channels, width), f32),
            jax.ShapeDtypeStruct((1, width), f32),
        ),
        in_specs=[anywhere],
        out_specs=(anywhere, anywhere, pl.BlockSpec(memory_space=pltpu.VMEM)),
        scratch_shapes=[
            pltpu.VMEM(summed.shape, jnp.bfloat16),
            pltpu.VMEM((9, width, width), f32),
            pltpu.VMEM((channels, width), f32),
            pltpu.SemaphoreType.DMA((2, 10)),
        ],
        compiler_params=pltpu.CompilerParams(vmem_limit_bytes=VMEM_LIMIT),
    )(summed)


def shards(spectra, target, patch, kernel, encoder_weight, kernels, gain, conv_weight, cotangent):
    tiles, bands = lax.axis_size("lon"), lax.axis_size("lat")
    rows, cols, width = cotangent.shape
    channels = spectra.shape[1]
    loss_scale = 1.0 / math.sqrt(rows * bands * cols * tiles)
    send_a, send_b, meta, first, last = pack(target, patch, kernel, spectra.T, cotangent, kernels.shape[1], tiles)
    meta = meta.reshape(tiles, 1, 128)
    weight = conv_weight.reshape(9, width, width)
    got_a, got_b, got_meta, wide, back, encoded, slope, turned = exchange(
        send_a, send_b, meta, cotangent, first, last, weight, encoder_weight, kernels
    )
    part_rows = 192 * 112
    normed, first, last, parts = middle(
        got_meta.reshape(tiles, 128), send_a, send_b, got_a, got_b, turned, gain.reshape(1, width), wide, back,
        encoded, slope, channels, part_rows,
    )
    conv_out, summed = sum_all(parts, normed, first, last, conv_weight.reshape(3, 3 * width, width))
    conv_grad, encoder_grad, gain_grad = finish(summed.reshape(part_rows, 128), loss_scale, channels, width)
    return conv_out, conv_grad.reshape(3, 3, width, width), encoder_grad, gain_grad.reshape(width)


def solution(mesh):
    placed = (
        P(("lat", "lon"), None),
        P(("lat", "lon")),
        P(("lat", "lon")),
        P(("lat", "lon")),
        P(),
        P(),
        P(),
        P(),
        P("lat", "lon", None),
    )
    return jax.shard_map(
        shards,
        mesh=mesh,
        in_specs=placed,
        out_specs=(P("lat", "lon", None), P(), P(), P()),
        check_vma=False,
    )
```

```python
import math

import jax
import jax.numpy as jnp
from jax import lax
from jax.experimental import pallas as pl
from jax.experimental.pallas import tpu as pltpu
from jax.sharding import PartitionSpec as P

PH = 8
PW = 16
MOST = 3
SIDE = 4
MESH = pl.DeviceIdType.MESH
VMEM_LIMIT = 60 * 1024 * 1024
SOURCES = sorted(((dy, dz) for dy in range(SIDE) for dz in range(SIDE)), key=lambda o: (o.count(2), sum(o) if 2 in o else 0, o))
GROUPS = (0, 9, 11, 13, 15, 16)


def dot(a, b, ca, cb):
    return lax.dot_general(a, b, (((ca,), (cb,)), ((), ())), preferred_element_type=jnp.float32)


def pack_kernel(
    target, patch, kernel, spectra, cot, to_a, to_b, meta, first, last,
    held, blank, near, far, block_in, counts, in_sems, out_sems,
):
    slots = block_in.shape[0]
    high, block = to_a.shape[3:]
    low = to_b.shape[3]
    rows, cols, _ = cot.shape
    fetch = pltpu.make_async_copy(spectra, held, in_sems.at[0])
    fetch.start()
    edges = [
        pltpu.make_async_copy(cot.at[:, pl.ds(0, 8)], near, in_sems.at[1]),
        pltpu.make_async_copy(cot.at[:, pl.ds(cols - 8, 8)], far, in_sems.at[2]),
    ]
    for edge in edges:
        edge.start()
    blank[...] = jnp.zeros_like(blank)

    @pl.loop(0, slots // MOST)
    def _(tile):
        counts[tile] = 0
        for rank in range(MOST):
            block_in[tile * MOST + rank] = -1
            meta[tile, rank] = -1
            meta[tile, MOST + rank] = 0

    @pl.loop(0, target.shape[0])
    def _(which):
        tile = target[which]
        rank = counts[tile]
        counts[tile] = rank + 1
        block_in[tile * MOST + rank] = which
        meta[tile, rank] = kernel[which]
        meta[tile, MOST + rank] = patch[which]

    fetch.wait()

    def pieces(slot, source):
        tile = slot // MOST
        rank = slot - tile * MOST
        y, z = tile // SIDE, tile % SIDE
        return (
            pltpu.make_async_copy(source(0, high), to_a.at[z, y, rank], out_sems.at[slot, 0]),
            pltpu.make_async_copy(source(high, low), to_b.at[y, z, rank], out_sems.at[slot, 1]),
        )

    @pl.loop(0, slots)
    def _(slot):
        which = block_in[slot]

        @pl.when(which >= 0)
        def _():
            lanes = pl.ds(pl.multiple_of(which * block, block), block)
            for piece in pieces(slot, lambda base, size: held.at[pl.ds(base, size), lanes]):
                piece.start()

        @pl.when(which < 0)
        def _():
            for piece in pieces(slot, lambda base, size: blank.at[pl.ds(0, size)]):
                piece.start()

    for edge in edges:
        edge.wait()

    @pl.loop(0, rows)
    def _(row):
        first[row] = near[row].astype(jnp.float32)[:1]
        last[row] = far[row].astype(jnp.float32)[7:]

    @pl.loop(0, slots)
    def _(slot):
        for piece in pieces(slot, lambda base, size: blank.at[pl.ds(0, size)]):
            piece.wait()


def pack(target, patch, kernel, flipped_spectra, cotangent, block, tiles):
    channels = flipped_spectra.shape[0]
    rows, _, width = cotangent.shape
    high = channels // 32 * 16
    low = channels - high
    slots = tiles * MOST
    bf, f32 = jnp.bfloat16, jnp.float32
    outs = [jax.ShapeDtypeStruct((SIDE, SIDE, MOST, size, block), bf) for size in (high, low)]
    outs.append(jax.ShapeDtypeStruct((tiles, 128), jnp.int32))
    outs += [jax.ShapeDtypeStruct((rows, 1, width), f32)] * 2
    anywhere = pl.BlockSpec(memory_space=pl.ANY)
    scalars = pl.BlockSpec(memory_space=pltpu.SMEM)
    inside = pl.BlockSpec(memory_space=pltpu.VMEM)
    return pl.pallas_call(
        pack_kernel,
        name="pack",
        out_shape=outs,
        in_specs=[scalars] * 3 + [anywhere] * 2,
        out_specs=(anywhere, anywhere, scalars, inside, inside),
        scratch_shapes=[
            pltpu.VMEM(flipped_spectra.shape, bf),
            pltpu.VMEM((max(high, low), block), bf),
            pltpu.VMEM((rows, 8, width), bf),
            pltpu.VMEM((rows, 8, width), bf),
            pltpu.SMEM((slots,), jnp.int32),
            pltpu.SMEM((tiles,), jnp.int32),
            pltpu.SemaphoreType.DMA((3,)),
            pltpu.SemaphoreType.DMA((slots, 2)),
        ],
        compiler_params=pltpu.CompilerParams(vmem_limit_bytes=VMEM_LIMIT),
    )(target, patch, kernel, flipped_spectra, cotangent)


def position():
    lat, lon = lax.axis_index("lat"), lax.axis_index("lon")
    return lat, lon, lon // SIDE, lon % SIDE


def halo_peers():
    lat, lon = lax.axis_index("lat"), lax.axis_index("lon")
    lats, lons = lax.axis_size("lat"), lax.axis_size("lon")
    up, down = (lat + lats - 1) % lats, (lat + 1) % lats
    left, right = (lon + lons - 1) % lons, (lon + 1) % lons
    return lat, lon, up, down, left, right


def halo_copies(top, bottom, first, last, from_above, from_below, from_left, from_right, sends, recvs):
    lat, lon, up, down, left, right = halo_peers()
    rows = first.shape[0]
    body = pl.ds(1, rows)
    plan = [
        (top, from_below, (up, lon)),
        (bottom, from_above, (down, lon)),
        (last, from_left.at[body], (lat, right)),
        (first, from_right.at[body], (lat, left)),
        (last.at[0], from_left.at[rows + 1], (up, right)),
        (last.at[rows - 1], from_left.at[0], (down, right)),
        (first.at[0], from_right.at[rows + 1], (up, left)),
        (first.at[rows - 1], from_right.at[0], (down, left)),
    ]
    return [
        pltpu.make_async_remote_copy(
            src_ref=src, dst_ref=dst, send_sem=sends.at[n], recv_sem=recvs.at[n], device_id=to, device_id_type=MESH
        )
        for n, (src, dst, to) in enumerate(plan)
    ]


def lay_windows(tile, from_above, from_below, from_left, from_right, wide, reverse):
    lat, lats = lax.axis_index("lat"), lax.axis_size("lat")
    rows, cols, width = tile.shape
    index = lax.broadcasted_iota(jnp.int32, (cols, width), 0)

    def lay(at, center, keep):
        value = center.astype(jnp.float32)
        before = jnp.where(index == 0, from_left[at], pltpu.roll(value, 1, 0))
        after = jnp.where(index == cols - 1, from_right[at], pltpu.roll(value, cols - 1, 0))
        if keep is not None:
            before, value, after = (jnp.where(keep, v, 0.0) for v in (before, value, after))
        order = (after, value, before) if reverse else (before, value, after)
        for n, v in enumerate(order):
            wide[at, :, n * width : (n + 1) * width] = v.astype(jnp.bfloat16)

    @pl.loop(0, rows)
    def _(row):
        lay(row + 1, tile[row], None)

    lay(0, from_above[...], lat > 0)
    lay(rows + 1, from_below[...], lat < lats - 1)


def exchange_kernel(
    send_a, send_b, meta, cot, first, last, weight, encoder_in, kernels_in,
    got_a, got_b, got_meta, wide_out, back_out, encoded_out, slope_out, turned_out, mid_a, mid_b, relay_a, relay_b,
    tile, wide, held_weight, back, above, below, lefts, rights, encoder, flat, table, turned, x, encoded, slope,
    halo_send, halo_recv, meta_send, meta_recv, sends, recvs, local, x_sems, out_sems,
):
    lat, lon, y, z = position()
    lats = lax.axis_size("lat")
    count = lax.axis_size("lon")
    _, _, up, down, left, right = halo_peers()
    rows, cols, width = tile.shape
    high, block = send_a.shape[3:]
    channels = x.shape[1]

    barrier = pltpu.get_barrier_semaphore()
    for step in range(1, SIDE * SIDE):
        peer = (lon + step) % count
        pl.semaphore_signal(barrier, inc=1, device_id=(lat, peer), device_id_type=MESH)
    for other in (up, down):
        for peer in (left, lon, right):
            pl.semaphore_signal(barrier, inc=1, device_id=(other, peer), device_id_type=MESH)
    load_tile = pltpu.make_async_copy(cot, tile, local.at[0])
    load_weight = pltpu.make_async_copy(weight, held_weight, local.at[1])
    load_tile.start()
    load_weight.start()
    own_meta = pltpu.make_async_copy(meta.at[lon], got_meta.at[0], local.at[2])
    own_meta.start()
    load_encoder = pltpu.make_async_copy(encoder_in, flat, local.at[5])
    load_kernels = pltpu.make_async_copy(kernels_in, table, local.at[6])
    load_encoder.start()
    load_kernels.start()

    def fetch(at, rank, from_a, from_b):
        lanes = pl.ds(rank * block, block)
        return (
            pltpu.make_async_copy(from_a.at[rank], x.at[at, pl.ds(0, high), lanes], x_sems.at[at, rank, 0]),
            pltpu.make_async_copy(from_b.at[rank], x.at[at, pl.ds(high, channels - high), lanes], x_sems.at[at, rank, 1]),
        )

    def bring(at, from_a, from_b):
        for rank in range(MOST):
            for copy in fetch(at, rank, from_a, from_b):
                copy.start()

    bring(0, send_a.at[z, y], send_b.at[y, z])
    pl.semaphore_wait(barrier, SIDE * SIDE - 1 + 6)

    halo = halo_copies(
        cot.at[0], cot.at[rows - 1], first, last, above, below, lefts, rights, halo_send, halo_recv
    )
    for copy in halo:
        copy.start()
    notes = []
    for dy in range(SIDE):
        for dz in range(SIDE):
            if dy or dz:
                n = SOURCES.index((dy, dz))
                to = (y + dy) % SIDE * SIDE + (z + dz) % SIDE
                notes.append(
                    pltpu.make_async_remote_copy(
                        src_ref=meta.at[to], dst_ref=got_meta.at[n], send_sem=meta_send.at[n],
                        recv_sem=meta_recv.at[n], device_id=(lat, to), device_id_type=MESH,
                    )
                )
    for copy in notes:
        copy.start()

    flows = []
    for flow, (src, mid, relay, got, u, v) in enumerate(
        ((send_a, mid_a, relay_a, got_a, z, y), (send_b, mid_b, relay_b, got_b, y, z))
    ):
        made = []

        def make(src_ref, dst_ref, du, dv, flow=flow, made=made, u=u, v=v):
            n = len(made)
            uu, vv = (u + du) % SIDE, (v + dv) % SIDE
            to = vv * SIDE + uu if flow == 0 else uu * SIDE + vv
            copy = pltpu.make_async_remote_copy(
                src_ref=src_ref, dst_ref=dst_ref, send_sem=sends.at[flow, n], recv_sem=recvs.at[flow, n],
                device_id=(lat, to), device_id_type=MESH,
            )
            made.append(copy)
            return copy

        def land(g, e, mid=mid, got=got):
            return got.at[0, e] if g == 0 else mid.at[g, e]

        def part(g, e, src=src, mid=mid, u=u, v=v):
            return src.at[u, (v + g) % SIDE] if e == 0 else mid.at[g, e]

        f = {"made": made}
        for d, sign in ((0, 1), (1, -1)):
            for j in range(2):
                g = 2 * d + j
                f["q1", d, j] = make(src.at[(u + 2) % SIDE, (v + g) % SIDE], relay.at[0, d, j], sign, 0)
                f["r1", d, j] = make(relay.at[0, d, j], land(g, 2), sign, 0)
            for g in range(SIDE):
                f["d1", d, g] = make(src.at[(u + sign) % SIDE, (v + g) % SIDE], land(g, 1 if d == 0 else 3), sign, 0)
            for e in range(SIDE):
                g = 1 if d == 0 else 3
                f["d2", d, e] = make(part(g, e), got.at[g, e], 0, sign)
            for j in range(2):
                e = ((0, 1), (3, 2))[d][j]
                f["q2", d, j] = make(part(2, e), relay.at[1, d, j], 0, sign)
                f["r2", d, j] = make(relay.at[1, d, j], got.at[2, e], 0, sign)
        flows.append(f)

    def start(*keys):
        for key in keys:
            for f in flows:
                f[key].start()

    def arrived(*keys):
        for key in keys:
            for f in flows:
                f[key].wait_recv()

    start(("q1", 0, 1), ("q1", 1, 0), ("q1", 0, 0), ("q1", 1, 1))
    for g in (2, 1, 3, 0):
        start(("d1", 0, g), ("d1", 1, g))

    load_tile.wait()
    for copy in halo:
        copy.wait()
    lay_windows(tile, above, below, lefts, rights, wide, True)
    save_wide = pltpu.make_async_copy(wide, wide_out, local.at[3])
    save_wide.start()
    load_weight.wait()
    step_rows = 4

    @pl.loop(0, rows // step_rows)
    def _(chunk):
        total = jnp.zeros((step_rows * cols, width), jnp.float32)
        for a in range(3):
            for b in range(3):
                window = wide[pl.ds(chunk * step_rows + 2 - a, step_rows), :, b * width : (b + 1) * width]
                total += dot(window.reshape(step_rows * cols, width), held_weight[a * 3 + b], 1, 1)
        back[pl.ds(chunk * step_rows, step_rows)] = total.reshape(step_rows, cols, width)

    save_back = pltpu.make_async_copy(back, back_out, local.at[4])
    save_back.start()
    load_encoder.wait()
    encoder[...] = flat[...].T
    load_kernels.wait()
    for n in range(table.shape[0]):
        turned[n] = table[n].T
    save_turned = pltpu.make_async_copy(turned, turned_out, local.at[7])
    save_turned.start()

    def landed(f, stage, e):
        if stage == 0:
            return f[{1: ("d1", 0, 0), 3: ("d1", 1, 0), 2: ("r1", 0, 0)}[e]]
        if stage == 2:
            return f[{0: ("r2", 0, 0), 1: ("r2", 0, 1), 3: ("r2", 1, 0), 2: ("r2", 1, 1)}[e]]
        return f["d2", stage // 2, e]

    def save(at):
        return (
            pltpu.make_async_copy(encoded.at[at], encoded_out.at[at], out_sems.at[at, 0]),
            pltpu.make_async_copy(slope.at[at], slope_out.at[at], out_sems.at[at, 1]),
        )

    def encode(group):
        for at in range(GROUPS[group], GROUPS[group + 1]):
            dy, dz = SOURCES[at]
            if at:
                landed(flows[0], dy, dz).wait_recv()
                landed(flows[1], dz, dy).wait_recv()
                bring(at, got_a.at[dy, dz], got_b.at[dz, dy])

        @pl.loop(GROUPS[group], GROUPS[group + 1])
        def _(at):
            for rank in range(MOST):
                for copy in fetch(at, rank, got_a.at[0, 0], got_b.at[0, 0]):
                    copy.wait()
            pre = dot(encoder[...], x[at], 1, 0)
            logistic = 0.5 * jnp.tanh(0.5 * pre) + 0.5
            encoded[at] = (pre * logistic).astype(jnp.bfloat16)
            slope[at] = logistic * (1.0 + pre * (1.0 - logistic))
            for copy in save(at):
                copy.start()

    for d, j in ((0, 1), (1, 0), (0, 0), (1, 1)):
        arrived(("q1", d, j))
        start(("r1", d, j))
    start(("q2", 0, 0), ("d2", 0, 0), ("d2", 1, 0))
    for g in (2, 1, 3):
        arrived(("d1", 0, g), ("d1", 1, g))
        if g == 2:
            start(("q2", 0, 1), ("q2", 1, 0))
        if g == 1:
            start(("d2", 0, 1), ("d2", 0, 3))
        if g == 3:
            start(("d2", 1, 1), ("d2", 1, 3))
    arrived(("r1", 1, 0))
    start(("q2", 1, 1))
    arrived(("r1", 0, 1), ("r1", 1, 1))
    arrived(("q2", 0, 0))
    start(("r2", 0, 0))
    arrived(("q2", 0, 1), ("q2", 1, 0))
    start(("r2", 0, 1), ("r2", 1, 0))
    start(("d2", 0, 2), ("d2", 1, 2))
    arrived(("q2", 1, 1))
    start(("r2", 1, 1))
    for group in range(len(GROUPS) - 1):
        encode(group)
    for f in flows:
        for copy in f["made"]:
            copy.wait_send()
    for copy in notes:
        copy.wait()
    own_meta.wait()
    save_wide.wait()
    save_back.wait()
    save_turned.wait()

    @pl.loop(0, len(SOURCES))
    def _(at):
        for copy in save(at):
            copy.wait()


def exchange(send_a, send_b, meta, cotangent, first, last, weight, encoder, kernels):
    rows, cols, width = cotangent.shape
    lon = SIDE * SIDE
    channels = encoder.shape[0]
    observed = MOST * send_a.shape[4]
    bf, f32 = jnp.bfloat16, jnp.float32
    anywhere = pl.BlockSpec(memory_space=pl.ANY)
    whole = [jax.ShapeDtypeStruct(a.shape, bf) for a in (send_a, send_b)]
    relay = [jax.ShapeDtypeStruct((2, 2, 2) + a.shape[2:], bf) for a in (send_a, send_b)]
    out = pl.pallas_call(
        exchange_kernel,
        name="exchange",
        out_shape=(
            *whole, jax.ShapeDtypeStruct(meta.shape, meta.dtype),
            jax.ShapeDtypeStruct((rows + 2, cols, 3 * width), bf), jax.ShapeDtypeStruct((rows, cols, width), f32),
            jax.ShapeDtypeStruct((lon, width, observed), bf), jax.ShapeDtypeStruct((lon, width, observed), f32),
            jax.ShapeDtypeStruct(kernels.shape, bf),
            *whole, *relay,
        ),
        in_specs=[anywhere] * 9,
        out_specs=(anywhere,) * 12,
        scratch_shapes=[
            pltpu.VMEM((rows, cols, width), bf),
            pltpu.VMEM((rows + 2, cols, 3 * width), bf),
            pltpu.VMEM(weight.shape, bf),
            pltpu.VMEM((rows, cols, width), f32),
            pltpu.VMEM((cols, width), bf),
            pltpu.VMEM((cols, width), bf),
            pltpu.VMEM((rows + 2, 1, width), f32),
            pltpu.VMEM((rows + 2, 1, width), f32),
            pltpu.VMEM((width, channels), bf),
            pltpu.VMEM((channels, width), bf),
            pltpu.VMEM(kernels.shape, bf),
            pltpu.VMEM(kernels.shape, bf),
            pltpu.VMEM((lon, channels, observed), bf),
            pltpu.VMEM((lon, width, observed), bf),
            pltpu.VMEM((lon, width, observed), f32),
            pltpu.SemaphoreType.DMA((8,)),
            pltpu.SemaphoreType.DMA((8,)),
            pltpu.SemaphoreType.DMA((lon,)),
            pltpu.SemaphoreType.DMA((lon,)),
            pltpu.SemaphoreType.DMA((2, 32)),
            pltpu.SemaphoreType.DMA((2, 32)),
            pltpu.SemaphoreType.DMA((8,)),
            pltpu.SemaphoreType.DMA((lon, MOST, 2)),
            pltpu.SemaphoreType.DMA((lon, 2)),
        ],
        compiler_params=pltpu.CompilerParams(
            collective_id=0, has_side_effects=True, vmem_limit_bytes=VMEM_LIMIT
        ),
    )(send_a, send_b, meta, cotangent, first, last, weight, encoder, kernels)
    return out[:8]


def middle_kernel(
    meta, own_a, own_b, got_a, got_b, turned, gain, wide_in, back_in, encoded_in, slope_in,
    normed, first, last, parts,
    x, slope, encoded, spread, d_spread, wide, back, flipped, d_rows, encoder_sum, gain_sum,
    x_sems, pair_sems, local,
):
    lat, lon, y, z = position()
    rows, cols, width = normed.shape
    channels = x.shape[1]
    high, block = own_a.shape[3:]
    sources = SIDE * SIDE

    def fetch(n, rank, from_a, from_b):
        lanes = pl.ds(rank * block, block)
        return (
            pltpu.make_async_copy(from_a.at[rank], x.at[n, pl.ds(0, high), lanes], x_sems.at[n, rank, 0]),
            pltpu.make_async_copy(from_b.at[rank], x.at[n, pl.ds(high, channels - high), lanes], x_sems.at[n, rank, 1]),
        )

    def load_encoded(n):
        return pltpu.make_async_copy(encoded_in.at[n], encoded.at[n], pair_sems.at[n, 0])

    def load_slope(n):
        return pltpu.make_async_copy(slope_in.at[n], slope.at[n], pair_sems.at[n, 1])

    load_back = pltpu.make_async_copy(back_in, back, local.at[0])
    load_wide = pltpu.make_async_copy(wide_in, wide, local.at[1])
    for n in range(sources):
        load_encoded(n).start()
    load_back.start()
    load_wide.start()
    for n, (dy, dz) in enumerate(SOURCES):
        from_a = own_a.at[z, y] if n == 0 else got_a.at[dy, dz]
        from_b = own_b.at[y, z] if n == 0 else got_b.at[dz, dy]
        for rank in range(MOST):
            for copy in fetch(n, rank, from_a, from_b):
                copy.start()
        load_slope(n).start()
    spread[...] = jnp.zeros_like(spread)

    @pl.loop(0, sources)
    def _(n):
        load_encoded(n).wait()
        for rank in range(MOST):
            which, patch = meta[n, rank], meta[n, MOST + rank]

            @pl.when(which >= 0)
            def _():
                spread[patch] += dot(turned[which], encoded[n, :, rank * block : (rank + 1) * block], 1, 1)

    load_back.wait()
    gain_sum[...] = jnp.zeros_like(gain_sum)
    across = cols // PW

    @pl.loop(0, spread.shape[0])
    def _(q):
        at = (pl.ds(q // across * PH, PH), pl.ds(pl.multiple_of(q % across * PW, PW), PW))
        value = spread[q]
        scale = lax.rsqrt(jnp.mean(value * value, axis=1, keepdims=True) + 1e-06)
        unit = value * scale
        weight = gain[...]
        normed[at] = (unit * weight).astype(jnp.bfloat16).reshape(PH, PW, width)
        given = back[at].reshape(PH * PW, width)
        product = given * unit
        gain_sum[...] += jnp.sum(product.reshape(PH * PW // 8, 8, width), axis=0)
        inner = jnp.mean(product * weight, axis=1, keepdims=True)
        d_spread[q] = (scale * (given * weight - unit * inner)).astype(jnp.bfloat16).T

    step_rows = 4

    @pl.loop(0, rows // step_rows)
    def _(n):
        some = normed[pl.ds(n * step_rows, step_rows)].reshape(step_rows * cols, width)
        flipped[:, pl.ds(pl.multiple_of(n * step_rows * cols, 128), step_rows * cols)] = some.T

    @pl.loop(0, rows)
    def _(row):
        some = normed[row].astype(jnp.float32)
        first[row] = some[:1]
        last[row] = some[cols - 1 :]

    load_wide.wait()
    for a in range(3):

        @pl.loop(0, 3 * width // 256)
        def _(j):
            window = wide[2 - a : 2 - a + rows, :, pl.ds(pl.multiple_of(j * 256, 256), 256)]
            got = dot(flipped[...], window.reshape(rows * cols, 256), 1, 0).astype(jnp.bfloat16)
            base = pl.multiple_of((a * (3 * width // 128) + 2 * j) * width, width)
            parts[pl.ds(base, width)] = got[:, :128]
            parts[pl.ds(pl.multiple_of(base + width, width), width)] = got[:, 128:]

    encoder_sum[...] = jnp.zeros_like(encoder_sum)

    @pl.loop(0, sources)
    def _(n):
        for rank in range(MOST):
            for copy in fetch(n, rank, got_a.at[0, 0], got_b.at[0, 0]):
                copy.wait()
        load_slope(n).wait()
        for rank in range(MOST):
            which, patch = jnp.maximum(meta[n, rank], 0), meta[n, MOST + rank]
            lanes = slice(rank * block, (rank + 1) * block)
            here = dot(d_spread[patch], turned[which], 1, 0).astype(jnp.bfloat16).astype(jnp.float32)
            d_rows[:, lanes] = (here * slope[n, :, lanes]).astype(jnp.bfloat16)
        encoder_sum[...] += dot(x[n], d_rows[...], 1, 1)

    base = 9 * width * width // 128
    for n in range(width // 128):
        lanes = slice(n * 128, (n + 1) * 128)
        parts[base + n * channels : base + (n + 1) * channels] = encoder_sum[:, lanes].astype(jnp.bfloat16)
    base += channels * width // 128
    for n in range(width // 128):
        parts[base + n * 8 : base + (n + 1) * 8] = gain_sum[:, n * 128 : (n + 1) * 128].astype(jnp.bfloat16)
    base += 8 * width // 128
    parts[base:] = jnp.zeros((parts.shape[0] - base, 128), jnp.bfloat16)


def middle(meta, own_a, own_b, got_a, got_b, turned, gain, wide, back, encoded, slope, channels, part_rows):
    rows, cols, width = back.shape
    cells, block = turned.shape[1:]
    patches = rows * cols // cells
    sources = SIDE * SIDE
    bf, f32 = jnp.bfloat16, jnp.float32
    anywhere = pl.BlockSpec(memory_space=pl.ANY)
    local = pl.BlockSpec(memory_space=pltpu.VMEM)
    column = jax.ShapeDtypeStruct((rows, 1, width), f32)
    return pl.pallas_call(
        middle_kernel,
        name="middle",
        out_shape=(
            jax.ShapeDtypeStruct((rows, cols, width), bf), column, column, jax.ShapeDtypeStruct((part_rows, 128), bf)
        ),
        in_specs=[pl.BlockSpec(memory_space=pltpu.SMEM)] + [anywhere] * 4 + [local] * 2 + [anywhere] * 4,
        out_specs=(local,) * 4,
        scratch_shapes=[
            pltpu.VMEM((sources, channels, MOST * block), bf),
            pltpu.VMEM((sources, width, MOST * block), f32),
            pltpu.VMEM((sources, width, MOST * block), bf),
            pltpu.VMEM((patches, cells, width), f32),
            pltpu.VMEM((patches, width, cells), bf),
            pltpu.VMEM(wide.shape, bf),
            pltpu.VMEM(back.shape, f32),
            pltpu.VMEM((width, rows * cols), bf),
            pltpu.VMEM((width, MOST * block), bf),
            pltpu.VMEM((channels, width), f32),
            pltpu.VMEM((8, width), f32),
            pltpu.SemaphoreType.DMA((sources, MOST, 2)),
            pltpu.SemaphoreType.DMA((sources, 2)),
            pltpu.SemaphoreType.DMA((2,)),
        ],
        compiler_params=pltpu.CompilerParams(vmem_limit_bytes=VMEM_LIMIT),
    )(meta, own_a, own_b, got_a, got_b, turned, gain, wide, back, encoded, slope)


PIECES = 16
PIECE_ROWS = 112
FLOWS = 6
HALVED = 12


def pairing(place, parity):
    near, far = place + 1 - 2 * (place % 2), (place + 3 - 2 * (place % 2)) % SIDE
    turn, high, low = (place + 1) // 2 % 2, place // 2, place % 2
    return ((near, turn), (far, high)) if parity == 0 else ((far, high), (near, low))


def sum_kernel(
    parts, normed, first, last, weight,
    conv_out, summed,
    own, other, total, outgoing, incoming, quarter_out, quarter_in, shared, result,
    tile, wide, held_weight, made, above, below, lefts, rights,
    halo_send, halo_recv, sends, recvs, local,
):
    lat, lon, y, z = position()
    x, core = lat // 2, lat % 2
    twin = (lat + 1 - 2 * core, lon)
    rows, cols, width = tile.shape
    _, _, up, down, left, right = halo_peers()

    def at_place(axis, place):
        if axis == 0:
            return (place * 2 + core, lon)
        return (lat, place * SIDE + z) if axis == 1 else (lat, y * SIDE + place)

    barrier = pltpu.get_barrier_semaphore()
    peers = [twin]
    for axis, place in enumerate((x, y, z)):
        peers += [at_place(axis, (place + step) % SIDE) for step in range(1, SIDE)]
    peers += [(lat, left), (lat, right)]
    peers += [(a, b) for a in (up, down) for b in (left, lon, right)]
    for peer in peers:
        pl.semaphore_signal(barrier, inc=1, device_id=peer, device_id_type=MESH)
    load_own = [pltpu.make_async_copy(parts.at[core, f], own.at[f], local.at[f]) for f in range(FLOWS)]
    load_tile = pltpu.make_async_copy(normed, tile, local.at[FLOWS])
    load_weight = pltpu.make_async_copy(weight, held_weight, local.at[FLOWS + 1])
    for copy in (load_tile, *load_own, load_weight):
        copy.start()
    pl.semaphore_wait(barrier, len(peers))

    halo = halo_copies(
        normed.at[0], normed.at[rows - 1], first, last, above, below, lefts, rights, halo_send, halo_recv
    )
    for copy in halo:
        copy.start()

    begun = []

    def remote(src, dst, flow, n, to):
        copy = pltpu.make_async_remote_copy(
            src_ref=src, dst_ref=dst, send_sem=sends.at[flow, n], recv_sem=recvs.at[flow, n],
            device_id=to, device_id_type=MESH,
        )
        copy.start()
        begun.append(copy)
        return copy

    places = (x, y, z)
    plans = []
    for f in range(FLOWS):
        turn, parity = f // 2, f % 2
        steps, base = [], 0
        for k, (partner, keep) in enumerate(pairing(places[turn], parity)):
            size = PIECES >> (k + 1)
            kept, sent = base + keep * size, base + (1 - keep) * size
            base = kept
            steps.append((at_place(turn, partner), size, kept, sent))
        plans.append((steps, (turn + 1) % 3, (turn + 2) % 3))

    crossing = [remote(parts.at[1 - core, f], other.at[f], f, 0, twin) for f in range(FLOWS)]

    load_tile.wait()
    for copy in halo:
        copy.wait()
    lay_windows(tile, above, below, lefts, rights, wide, False)
    load_weight.wait()
    step_rows = 4
    save = [pltpu.make_async_copy(made, conv_out, local.at[FLOWS + 2])]

    def convolve(chunk):
        value = jnp.zeros((step_rows * cols, width), jnp.float32)
        for a in range(3):
            window = wide[chunk * step_rows + a : chunk * step_rows + a + step_rows]
            value += dot(window.reshape(step_rows * cols, 3 * width), held_weight[a], 1, 0)
        made[chunk * step_rows : (chunk + 1) * step_rows] = value.astype(jnp.bfloat16).reshape(step_rows, cols, width)

    def halve(f, k):
        to, size, _, _ = plans[f][0][k]
        at = pl.ds((0, PIECES // 2)[k], size)
        return remote(outgoing.at[f, at], incoming.at[f, at], f, 1 + k, to)

    convolve(0)
    flying = []
    for f in range(FLOWS):
        _, size, kept, sent = plans[f][0][0]
        load_own[f].wait()
        crossing[f].wait_recv()

        @pl.loop(0, size)
        def _(i):
            total[f, kept + i] = own[f, kept + i].astype(jnp.float32) + other[f, kept + i].astype(jnp.float32)
            value = own[f, sent + i].astype(jnp.float32) + other[f, sent + i].astype(jnp.float32)
            outgoing[f, i] = value.astype(jnp.bfloat16)

        flying.append(halve(f, 0))
    for chunk in (1, 2, 3):
        convolve(chunk)
    for f in range(FLOWS):
        _, _, kept, _ = plans[f][0][0]
        _, size, keep_next, send_next = plans[f][0][1]
        flying[f].wait_recv()

        @pl.loop(0, size)
        def _(i):
            total[f, keep_next + i] += incoming[f, keep_next - kept + i].astype(jnp.float32)
            value = total[f, send_next + i] + incoming[f, send_next - kept + i].astype(jnp.float32)
            outgoing[f, PIECES // 2 + i] = value.astype(jnp.bfloat16)

        flying[f] = halve(f, 1)
    convolve(4)
    for f in range(FLOWS):
        steps, axis, _ = plans[f]
        base = steps[1][2]
        flying[f].wait_recv()
        flying[f] = []
        for step in range(1, SIDE):
            place = (places[axis] + step) % SIDE
            value = total[f, base + place] + incoming[f, PIECES // 2 + place].astype(jnp.float32)
            quarter_out[f, step - 1] = value.astype(jnp.bfloat16)
            flying[f].append(
                remote(quarter_out.at[f, step - 1], quarter_in.at[f, step - 1], f, 2 + step, at_place(axis, place))
            )
    convolve(5)
    save[0].start()
    for f in range(FLOWS):
        steps, axis, other_axis = plans[f]
        here, there = places[axis], places[other_axis]
        value = total[f, steps[1][2] + here] + incoming[f, PIECES // 2 + here].astype(jnp.float32)
        for step in range(1, SIDE):
            flying[f][step - 1].wait_recv()
            value += quarter_in[f, step - 1].astype(jnp.float32)
        shared[f, there] = value.astype(jnp.bfloat16)
        flying[f] = [
            remote(shared.at[f, there], shared.at[f, there], f, 5 + step, at_place(other_axis, (there + step) % SIDE))
            for step in range(1, SIDE)
        ]

    passed = []

    def pass_on(f, start, size, n):
        at = result.at[core, f, pl.ds(start, size)]
        passed.append(remote(at, at, f, n, twin))

    for f in range(FLOWS):
        steps, axis, _ = plans[f]
        mine = steps[1][2] + places[axis]
        for copy in flying[f]:
            copy.wait_recv()
        value = shared[f, 0].astype(jnp.float32)
        for place in range(1, SIDE):
            value += shared[f, place].astype(jnp.float32)
        result[core, f, mine] = value.astype(jnp.bfloat16)
        at = result.at[core, f, mine]
        flying[f] = [
            remote(at, at, f, 8 + step, at_place(axis, (places[axis] + step) % SIDE)) for step in range(1, SIDE)
        ]
    for k in (1, 0):
        for f in range(FLOWS):
            to, size, kept, _ = plans[f][0][k]
            for copy in flying[f]:
                copy.wait_recv()
            at = result.at[core, f, pl.ds(kept, size)]
            flying[f] = [remote(at, at, f, 13 - k, to)]
            if k == 1:
                pass_on(f, kept, size, 14)
            else:
                pass_on(f, plans[f][0][1][3], plans[f][0][1][1], 15)
    for f in range(FLOWS):
        _, size, _, sent = plans[f][0][0]
        flying[f][0].wait_recv()
        pass_on(f, sent, size, 16)
    for copy in passed:
        copy.wait_recv()
    stored = pltpu.make_async_copy(result, summed, local.at[FLOWS + 3])
    stored.start()
    for copy in begun:
        copy.wait_send()
    save[0].wait()
    stored.wait()


def sum_all(parts, normed, first, last, weight):
    rows, cols, width = normed.shape
    bf, f32 = jnp.bfloat16, jnp.float32
    anywhere = pl.BlockSpec(memory_space=pl.ANY)
    inside = pl.BlockSpec(memory_space=pltpu.VMEM)
    piece = (PIECE_ROWS, 128)
    parts = parts.reshape((2, FLOWS, PIECES) + piece)
    return pl.pallas_call(
        sum_kernel,
        name="sum_all",
        out_shape=(jax.ShapeDtypeStruct(normed.shape, bf), jax.ShapeDtypeStruct(parts.shape, bf)),
        in_specs=[anywhere, anywhere, inside, inside, anywhere],
        out_specs=(anywhere, anywhere),
        scratch_shapes=[
            pltpu.VMEM((FLOWS, PIECES) + piece, bf),
            pltpu.VMEM((FLOWS, PIECES) + piece, bf),
            pltpu.VMEM((FLOWS, PIECES) + piece, f32),
            pltpu.VMEM((FLOWS, HALVED) + piece, bf),
            pltpu.VMEM((FLOWS, HALVED) + piece, bf),
            pltpu.VMEM((FLOWS, SIDE - 1) + piece, bf),
            pltpu.VMEM((FLOWS, SIDE - 1) + piece, bf),
            pltpu.VMEM((FLOWS, SIDE) + piece, bf),
            pltpu.VMEM((2, FLOWS, PIECES) + piece, bf),
            pltpu.VMEM((rows, cols, width), bf),
            pltpu.VMEM((rows + 2, cols, 3 * width), bf),
            pltpu.VMEM(weight.shape, bf),
            pltpu.VMEM((rows, cols, width), bf),
            pltpu.VMEM((cols, width), bf),
            pltpu.VMEM((cols, width), bf),
            pltpu.VMEM((rows + 2, 1, width), f32),
            pltpu.VMEM((rows + 2, 1, width), f32),
            pltpu.SemaphoreType.DMA((8,)),
            pltpu.SemaphoreType.DMA((8,)),
            pltpu.SemaphoreType.DMA((FLOWS, 17)),
            pltpu.SemaphoreType.DMA((FLOWS, 17)),
            pltpu.SemaphoreType.DMA((FLOWS + 4,)),
        ],
        compiler_params=pltpu.CompilerParams(
            collective_id=1, has_side_effects=True, vmem_limit_bytes=VMEM_LIMIT
        ),
    )(parts, normed, first, last, weight)


def finish_kernel(scale, summed, conv_grad, encoder_grad, gain_grad, held, taps, encoder, sems):
    count, width = taps.shape[0], taps.shape[2]
    lanes = width // 128
    channels = encoder.shape[0]
    size = lanes * width
    base = count * size
    rest = channels * lanes + 8 * lanes

    def load(tap):
        at = pl.ds(pl.multiple_of(tap * size, size), size)
        return pltpu.make_async_copy(summed.at[at], held.at[at], sems.at[0, tap])

    def save(tap):
        return pltpu.make_async_copy(taps.at[tap], conv_grad.at[tap], sems.at[1, tap])

    last = pl.ds(base, rest)
    load_rest = pltpu.make_async_copy(summed.at[last], held.at[last], sems.at[0, count])
    for tap in range(count):
        load(tap).start()
    load_rest.start()

    @pl.loop(0, count)
    def _(tap):
        load(tap).wait()
        for n in range(lanes):
            at = pl.ds(pl.multiple_of(tap * size + n * width, width), width)
            taps[tap, :, n * 128 : (n + 1) * 128] = held[at].astype(jnp.float32) * scale
        save(tap).start()

    load_rest.wait()
    for n in range(lanes):
        at = slice(n * 128, (n + 1) * 128)
        encoder[:, at] = held[base + n * channels : base + (n + 1) * channels].astype(jnp.float32) * scale
        start = base + channels * lanes + n * 8
        gain_grad[:, at] = jnp.sum(held[start : start + 8].astype(jnp.float32), axis=0, keepdims=True) * scale
    save_encoder = pltpu.make_async_copy(encoder, encoder_grad, sems.at[1, count])
    save_encoder.start()

    @pl.loop(0, count)
    def _(tap):
        save(tap).wait()

    save_encoder.wait()


def finish(summed, scale, channels, width):
    f32 = jnp.float32
    anywhere = pl.BlockSpec(memory_space=pl.ANY)
    return pl.pallas_call(
        lambda *refs: finish_kernel(scale, *refs),
        name="finish",
        out_shape=(
            jax.ShapeDtypeStruct((9, width, width), f32),
            jax.ShapeDtypeStruct((channels, width), f32),
            jax.ShapeDtypeStruct((1, width), f32),
        ),
        in_specs=[anywhere],
        out_specs=(anywhere, anywhere, pl.BlockSpec(memory_space=pltpu.VMEM)),
        scratch_shapes=[
            pltpu.VMEM(summed.shape, jnp.bfloat16),
            pltpu.VMEM((9, width, width), f32),
            pltpu.VMEM((channels, width), f32),
            pltpu.SemaphoreType.DMA((2, 10)),
        ],
        compiler_params=pltpu.CompilerParams(vmem_limit_bytes=VMEM_LIMIT),
    )(summed)


def shards(spectra, target, patch, kernel, encoder_weight, kernels, gain, conv_weight, cotangent):
    tiles, bands = lax.axis_size("lon"), lax.axis_size("lat")
    rows, cols, width = cotangent.shape
    channels = spectra.shape[1]
    loss_scale = 1.0 / math.sqrt(rows * bands * cols * tiles)
    send_a, send_b, meta, first, last = pack(target, patch, kernel, spectra.T, cotangent, kernels.shape[1], tiles)
    meta = meta.reshape(tiles, 1, 128)
    weight = conv_weight.reshape(9, width, width)
    got_a, got_b, got_meta, wide, back, encoded, slope, turned = exchange(
        send_a, send_b, meta, cotangent, first, last, weight, encoder_weight, kernels
    )
    part_rows = 192 * 112
    normed, first, last, parts = middle(
        got_meta.reshape(tiles, 128), send_a, send_b, got_a, got_b, turned, gain.reshape(1, width), wide, back,
        encoded, slope, channels, part_rows,
    )
    conv_out, summed = sum_all(parts, normed, first, last, conv_weight.reshape(3, 3 * width, width))
    conv_grad, encoder_grad, gain_grad = finish(summed.reshape(part_rows, 128), loss_scale, channels, width)
    return conv_out, conv_grad.reshape(3, 3, width, width), encoder_grad, gain_grad.reshape(width)


def solution(mesh):
    placed = (
        P(("lat", "lon"), None),
        P(("lat", "lon")),
        P(("lat", "lon")),
        P(("lat", "lon")),
        P(),
        P(),
        P(),
        P(),
        P("lat", "lon", None),
    )
    return jax.shard_map(
        shards,
        mesh=mesh,
        in_specs=placed,
        out_specs=(P("lat", "lon", None), P(), P(), P()),
        check_vma=False,
    )
```

```python
import math

import jax
import jax.numpy as jnp
from jax import lax
from jax.experimental import pallas as pl
from jax.experimental.pallas import tpu as pltpu
from jax.sharding import PartitionSpec as P

PH = 8
PW = 16
MOST = 3
SIDE = 4
MESH = pl.DeviceIdType.MESH
VMEM_LIMIT = 60 * 1024 * 1024
SOURCES = sorted(((dy, dz) for dy in range(SIDE) for dz in range(SIDE)), key=lambda o: (o.count(2), sum(o) if 2 in o else 0, o))
GROUPS = (0, 9, 11, 13, 15, 16)


def dot(a, b, ca, cb):
    return lax.dot_general(a, b, (((ca,), (cb,)), ((), ())), preferred_element_type=jnp.float32)


def pack_kernel(
    target, patch, kernel, spectra, cot, to_a, to_b, meta, first, last,
    held, blank, near, far, block_in, counts, in_sems, out_sems,
):
    slots = block_in.shape[0]
    high, block = to_a.shape[3:]
    low = to_b.shape[3]
    rows, cols, _ = cot.shape
    fetch = pltpu.make_async_copy(spectra, held, in_sems.at[0])
    fetch.start()
    edges = [
        pltpu.make_async_copy(cot.at[:, pl.ds(0, 8)], near, in_sems.at[1]),
        pltpu.make_async_copy(cot.at[:, pl.ds(cols - 8, 8)], far, in_sems.at[2]),
    ]
    for edge in edges:
        edge.start()
    blank[...] = jnp.zeros_like(blank)

    @pl.loop(0, slots // MOST)
    def _(tile):
        counts[tile] = 0
        for rank in range(MOST):
            block_in[tile * MOST + rank] = -1
            meta[tile, rank] = -1
            meta[tile, MOST + rank] = 0

    @pl.loop(0, target.shape[0])
    def _(which):
        tile = target[which]
        rank = counts[tile]
        counts[tile] = rank + 1
        block_in[tile * MOST + rank] = which
        meta[tile, rank] = kernel[which]
        meta[tile, MOST + rank] = patch[which]

    fetch.wait()

    def pieces(slot, source):
        tile = slot // MOST
        rank = slot - tile * MOST
        y, z = tile // SIDE, tile % SIDE
        return (
            pltpu.make_async_copy(source(0, high), to_a.at[z, y, rank], out_sems.at[slot, 0]),
            pltpu.make_async_copy(source(high, low), to_b.at[y, z, rank], out_sems.at[slot, 1]),
        )

    @pl.loop(0, slots)
    def _(slot):
        which = block_in[slot]

        @pl.when(which >= 0)
        def _():
            lanes = pl.ds(pl.multiple_of(which * block, block), block)
            for piece in pieces(slot, lambda base, size: held.at[pl.ds(base, size), lanes]):
                piece.start()

        @pl.when(which < 0)
        def _():
            for piece in pieces(slot, lambda base, size: blank.at[pl.ds(0, size)]):
                piece.start()

    for edge in edges:
        edge.wait()

    @pl.loop(0, rows)
    def _(row):
        first[row] = near[row].astype(jnp.float32)[:1]
        last[row] = far[row].astype(jnp.float32)[7:]

    @pl.loop(0, slots)
    def _(slot):
        for piece in pieces(slot, lambda base, size: blank.at[pl.ds(0, size)]):
            piece.wait()


def pack(target, patch, kernel, flipped_spectra, cotangent, block, tiles):
    channels = flipped_spectra.shape[0]
    rows, _, width = cotangent.shape
    high = channels // 32 * 16
    low = channels - high
    slots = tiles * MOST
    bf, f32 = jnp.bfloat16, jnp.float32
    outs = [jax.ShapeDtypeStruct((SIDE, SIDE, MOST, size, block), bf) for size in (high, low)]
    outs.append(jax.ShapeDtypeStruct((tiles, 128), jnp.int32))
    outs += [jax.ShapeDtypeStruct((rows, 1, width), f32)] * 2
    anywhere = pl.BlockSpec(memory_space=pl.ANY)
    scalars = pl.BlockSpec(memory_space=pltpu.SMEM)
    inside = pl.BlockSpec(memory_space=pltpu.VMEM)
    return pl.pallas_call(
        pack_kernel,
        name="pack",
        out_shape=outs,
        in_specs=[scalars] * 3 + [anywhere] * 2,
        out_specs=(anywhere, anywhere, scalars, inside, inside),
        scratch_shapes=[
            pltpu.VMEM(flipped_spectra.shape, bf),
            pltpu.VMEM((max(high, low), block), bf),
            pltpu.VMEM((rows, 8, width), bf),
            pltpu.VMEM((rows, 8, width), bf),
            pltpu.SMEM((slots,), jnp.int32),
            pltpu.SMEM((tiles,), jnp.int32),
            pltpu.SemaphoreType.DMA((3,)),
            pltpu.SemaphoreType.DMA((slots, 2)),
        ],
        compiler_params=pltpu.CompilerParams(vmem_limit_bytes=VMEM_LIMIT),
    )(target, patch, kernel, flipped_spectra, cotangent)


def position():
    lat, lon = lax.axis_index("lat"), lax.axis_index("lon")
    return lat, lon, lon // SIDE, lon % SIDE


def halo_peers():
    lat, lon = lax.axis_index("lat"), lax.axis_index("lon")
    lats, lons = lax.axis_size("lat"), lax.axis_size("lon")
    up, down = (lat + lats - 1) % lats, (lat + 1) % lats
    left, right = (lon + lons - 1) % lons, (lon + 1) % lons
    return lat, lon, up, down, left, right


def halo_copies(top, bottom, first, last, from_above, from_below, from_left, from_right, sends, recvs):
    lat, lon, up, down, left, right = halo_peers()
    rows = first.shape[0]
    body = pl.ds(1, rows)
    plan = [
        (top, from_below, (up, lon)),
        (bottom, from_above, (down, lon)),
        (last, from_left.at[body], (lat, right)),
        (first, from_right.at[body], (lat, left)),
        (last.at[0], from_left.at[rows + 1], (up, right)),
        (last.at[rows - 1], from_left.at[0], (down, right)),
        (first.at[0], from_right.at[rows + 1], (up, left)),
        (first.at[rows - 1], from_right.at[0], (down, left)),
    ]
    return [
        pltpu.make_async_remote_copy(
            src_ref=src, dst_ref=dst, send_sem=sends.at[n], recv_sem=recvs.at[n], device_id=to, device_id_type=MESH
        )
        for n, (src, dst, to) in enumerate(plan)
    ]


def lay_windows(tile, from_above, from_below, from_left, from_right, wide, reverse):
    lat, lats = lax.axis_index("lat"), lax.axis_size("lat")
    rows, cols, width = tile.shape
    index = lax.broadcasted_iota(jnp.int32, (cols, width), 0)

    def lay(at, center, keep):
        value = center.astype(jnp.float32)
        before = jnp.where(index == 0, from_left[at], pltpu.roll(value, 1, 0))
        after = jnp.where(index == cols - 1, from_right[at], pltpu.roll(value, cols - 1, 0))
        if keep is not None:
            before, value, after = (jnp.where(keep, v, 0.0) for v in (before, value, after))
        order = (after, value, before) if reverse else (before, value, after)
        for n, v in enumerate(order):
            wide[at, :, n * width : (n + 1) * width] = v.astype(jnp.bfloat16)

    @pl.loop(0, rows)
    def _(row):
        lay(row + 1, tile[row], None)

    lay(0, from_above[...], lat > 0)
    lay(rows + 1, from_below[...], lat < lats - 1)


def exchange_kernel(
    send_a, send_b, meta, cot, first, last, weight, encoder_in, kernels_in,
    got_a, got_b, got_meta, wide_out, back_out, encoded_out, slope_out, turned_out, mid_a, mid_b, relay_a, relay_b,
    tile, wide, held_weight, back, above, below, lefts, rights, encoder, flat, table, turned, x, encoded, slope,
    halo_send, halo_recv, meta_send, meta_recv, sends, recvs, local, x_sems, out_sems,
):
    lat, lon, y, z = position()
    lats = lax.axis_size("lat")
    count = lax.axis_size("lon")
    _, _, up, down, left, right = halo_peers()
    rows, cols, width = tile.shape
    high, block = send_a.shape[3:]
    channels = x.shape[1]

    barrier = pltpu.get_barrier_semaphore()
    for step in range(1, SIDE * SIDE):
        peer = (lon + step) % count
        pl.semaphore_signal(barrier, inc=1, device_id=(lat, peer), device_id_type=MESH)
    for other in (up, down):
        for peer in (left, lon, right):
            pl.semaphore_signal(barrier, inc=1, device_id=(other, peer), device_id_type=MESH)
    load_tile = pltpu.make_async_copy(cot, tile, local.at[0])
    load_weight = pltpu.make_async_copy(weight, held_weight, local.at[1])
    load_tile.start()
    load_weight.start()
    own_meta = pltpu.make_async_copy(meta.at[lon], got_meta.at[0], local.at[2])
    own_meta.start()
    load_encoder = pltpu.make_async_copy(encoder_in, flat, local.at[5])
    load_kernels = pltpu.make_async_copy(kernels_in, table, local.at[6])
    load_encoder.start()
    load_kernels.start()

    def fetch(at, rank, from_a, from_b):
        lanes = pl.ds(rank * block, block)
        return (
            pltpu.make_async_copy(from_a.at[rank], x.at[at, pl.ds(0, high), lanes], x_sems.at[at, rank, 0]),
            pltpu.make_async_copy(from_b.at[rank], x.at[at, pl.ds(high, channels - high), lanes], x_sems.at[at, rank, 1]),
        )

    def bring(at, from_a, from_b):
        for rank in range(MOST):
            for copy in fetch(at, rank, from_a, from_b):
                copy.start()

    bring(0, send_a.at[z, y], send_b.at[y, z])
    pl.semaphore_wait(barrier, SIDE * SIDE - 1 + 6)

    halo = halo_copies(
        cot.at[0], cot.at[rows - 1], first, last, above, below, lefts, rights, halo_send, halo_recv
    )
    for copy in halo:
        copy.start()
    notes = []
    for dy in range(SIDE):
        for dz in range(SIDE):
            if dy or dz:
                n = SOURCES.index((dy, dz))
                to = (y + dy) % SIDE * SIDE + (z + dz) % SIDE
                notes.append(
                    pltpu.make_async_remote_copy(
                        src_ref=meta.at[to], dst_ref=got_meta.at[n], send_sem=meta_send.at[n],
                        recv_sem=meta_recv.at[n], device_id=(lat, to), device_id_type=MESH,
                    )
                )
    for copy in notes:
        copy.start()

    flows = []
    for flow, (src, mid, relay, got, u, v) in enumerate(
        ((send_a, mid_a, relay_a, got_a, z, y), (send_b, mid_b, relay_b, got_b, y, z))
    ):
        made = []

        def make(src_ref, dst_ref, du, dv, flow=flow, made=made, u=u, v=v):
            n = len(made)
            uu, vv = (u + du) % SIDE, (v + dv) % SIDE
            to = vv * SIDE + uu if flow == 0 else uu * SIDE + vv
            copy = pltpu.make_async_remote_copy(
                src_ref=src_ref, dst_ref=dst_ref, send_sem=sends.at[flow, n], recv_sem=recvs.at[flow, n],
                device_id=(lat, to), device_id_type=MESH,
            )
            made.append(copy)
            return copy

        def land(g, e, mid=mid, got=got):
            return got.at[0, e] if g == 0 else mid.at[g, e]

        def part(g, e, src=src, mid=mid, u=u, v=v):
            return src.at[u, (v + g) % SIDE] if e == 0 else mid.at[g, e]

        f = {"made": made}
        for d, sign in ((0, 1), (1, -1)):
            for j in range(2):
                g = 2 * d + j
                f["q1", d, j] = make(src.at[(u + 2) % SIDE, (v + g) % SIDE], relay.at[0, d, j], sign, 0)
                f["r1", d, j] = make(relay.at[0, d, j], land(g, 2), sign, 0)
            for g in range(SIDE):
                f["d1", d, g] = make(src.at[(u + sign) % SIDE, (v + g) % SIDE], land(g, 1 if d == 0 else 3), sign, 0)
            for e in range(SIDE):
                g = 1 if d == 0 else 3
                f["d2", d, e] = make(part(g, e), got.at[g, e], 0, sign)
            for j in range(2):
                e = ((0, 1), (3, 2))[d][j]
                f["q2", d, j] = make(part(2, e), relay.at[1, d, j], 0, sign)
                f["r2", d, j] = make(relay.at[1, d, j], got.at[2, e], 0, sign)
        flows.append(f)

    def start(*keys):
        for key in keys:
            for f in flows:
                f[key].start()

    def arrived(*keys):
        for key in keys:
            for f in flows:
                f[key].wait_recv()

    start(("q1", 0, 1), ("q1", 1, 0), ("q1", 0, 0), ("q1", 1, 1))
    for g in (2, 1, 3, 0):
        start(("d1", 0, g), ("d1", 1, g))

    load_tile.wait()
    for copy in halo:
        copy.wait()
    lay_windows(tile, above, below, lefts, rights, wide, True)
    save_wide = pltpu.make_async_copy(wide, wide_out, local.at[3])
    save_wide.start()
    load_weight.wait()
    step_rows = 4

    @pl.loop(0, rows // step_rows)
    def _(chunk):
        total = jnp.zeros((step_rows * cols, width), jnp.float32)
        for a in range(3):
            for b in range(3):
                window = wide[pl.ds(chunk * step_rows + 2 - a, step_rows), :, b * width : (b + 1) * width]
                total += dot(window.reshape(step_rows * cols, width), held_weight[a * 3 + b], 1, 1)
        back[pl.ds(chunk * step_rows, step_rows)] = total.reshape(step_rows, cols, width)

    save_back = pltpu.make_async_copy(back, back_out, local.at[4])
    save_back.start()
    load_encoder.wait()
    encoder[...] = flat[...].T
    load_kernels.wait()
    for n in range(table.shape[0]):
        turned[n] = table[n].T
    save_turned = pltpu.make_async_copy(turned, turned_out, local.at[7])
    save_turned.start()

    def landed(f, stage, e):
        if stage == 0:
            return f[{1: ("d1", 0, 0), 3: ("d1", 1, 0), 2: ("r1", 0, 0)}[e]]
        if stage == 2:
            return f[{0: ("r2", 0, 0), 1: ("r2", 0, 1), 3: ("r2", 1, 0), 2: ("r2", 1, 1)}[e]]
        return f["d2", stage // 2, e]

    def save(at):
        return (
            pltpu.make_async_copy(encoded.at[at], encoded_out.at[at], out_sems.at[at, 0]),
            pltpu.make_async_copy(slope.at[at], slope_out.at[at], out_sems.at[at, 1]),
        )

    def encode(group):
        for at in range(GROUPS[group], GROUPS[group + 1]):
            dy, dz = SOURCES[at]
            if at:
                landed(flows[0], dy, dz).wait_recv()
                landed(flows[1], dz, dy).wait_recv()
                bring(at, got_a.at[dy, dz], got_b.at[dz, dy])

        @pl.loop(GROUPS[group], GROUPS[group + 1])
        def _(at):
            for rank in range(MOST):
                for copy in fetch(at, rank, got_a.at[0, 0], got_b.at[0, 0]):
                    copy.wait()
            pre = dot(encoder[...], x[at], 1, 0)
            logistic = 0.5 * jnp.tanh(0.5 * pre) + 0.5
            encoded[at] = (pre * logistic).astype(jnp.bfloat16)
            slope[at] = logistic * (1.0 + pre * (1.0 - logistic))
            for copy in save(at):
                copy.start()

    for d, j in ((0, 1), (1, 0), (0, 0), (1, 1)):
        arrived(("q1", d, j))
        start(("r1", d, j))
    start(("q2", 0, 0), ("d2", 0, 0), ("d2", 1, 0))
    for g in (2, 1, 3):
        arrived(("d1", 0, g), ("d1", 1, g))
        if g == 2:
            start(("q2", 0, 1), ("q2", 1, 0))
        if g == 1:
            start(("d2", 0, 1), ("d2", 0, 3))
        if g == 3:
            start(("d2", 1, 1), ("d2", 1, 3))
    arrived(("r1", 1, 0))
    start(("q2", 1, 1))
    arrived(("r1", 0, 1), ("r1", 1, 1))
    arrived(("q2", 0, 0))
    start(("r2", 0, 0))
    arrived(("q2", 0, 1), ("q2", 1, 0))
    start(("r2", 0, 1), ("r2", 1, 0))
    start(("d2", 0, 2), ("d2", 1, 2))
    arrived(("q2", 1, 1))
    start(("r2", 1, 1))
    for group in range(len(GROUPS) - 1):
        encode(group)
    for f in flows:
        for copy in f["made"]:
            copy.wait_send()
    for copy in notes:
        copy.wait()
    own_meta.wait()
    save_wide.wait()
    save_back.wait()
    save_turned.wait()

    @pl.loop(0, len(SOURCES))
    def _(at):
        for copy in save(at):
            copy.wait()


def exchange(send_a, send_b, meta, cotangent, first, last, weight, encoder, kernels):
    rows, cols, width = cotangent.shape
    lon = SIDE * SIDE
    channels = encoder.shape[0]
    observed = MOST * send_a.shape[4]
    bf, f32 = jnp.bfloat16, jnp.float32
    anywhere = pl.BlockSpec(memory_space=pl.ANY)
    whole = [jax.ShapeDtypeStruct(a.shape, bf) for a in (send_a, send_b)]
    relay = [jax.ShapeDtypeStruct((2, 2, 2) + a.shape[2:], bf) for a in (send_a, send_b)]
    out = pl.pallas_call(
        exchange_kernel,
        name="exchange",
        out_shape=(
            *whole, jax.ShapeDtypeStruct(meta.shape, meta.dtype),
            jax.ShapeDtypeStruct((rows + 2, cols, 3 * width), bf), jax.ShapeDtypeStruct((rows, cols, width), f32),
            jax.ShapeDtypeStruct((lon, width, observed), bf), jax.ShapeDtypeStruct((lon, width, observed), f32),
            jax.ShapeDtypeStruct(kernels.shape, bf),
            *whole, *relay,
        ),
        in_specs=[anywhere] * 9,
        out_specs=(anywhere,) * 12,
        scratch_shapes=[
            pltpu.VMEM((rows, cols, width), bf),
            pltpu.VMEM((rows + 2, cols, 3 * width), bf),
            pltpu.VMEM(weight.shape, bf),
            pltpu.VMEM((rows, cols, width), f32),
            pltpu.VMEM((cols, width), bf),
            pltpu.VMEM((cols, width), bf),
            pltpu.VMEM((rows + 2, 1, width), f32),
            pltpu.VMEM((rows + 2, 1, width), f32),
            pltpu.VMEM((width, channels), bf),
            pltpu.VMEM((channels, width), bf),
            pltpu.VMEM(kernels.shape, bf),
            pltpu.VMEM(kernels.shape, bf),
            pltpu.VMEM((lon, channels, observed), bf),
            pltpu.VMEM((lon, width, observed), bf),
            pltpu.VMEM((lon, width, observed), f32),
            pltpu.SemaphoreType.DMA((8,)),
            pltpu.SemaphoreType.DMA((8,)),
            pltpu.SemaphoreType.DMA((lon,)),
            pltpu.SemaphoreType.DMA((lon,)),
            pltpu.SemaphoreType.DMA((2, 32)),
            pltpu.SemaphoreType.DMA((2, 32)),
            pltpu.SemaphoreType.DMA((8,)),
            pltpu.SemaphoreType.DMA((lon, MOST, 2)),
            pltpu.SemaphoreType.DMA((lon, 2)),
        ],
        compiler_params=pltpu.CompilerParams(
            collective_id=0, has_side_effects=True, vmem_limit_bytes=VMEM_LIMIT
        ),
    )(send_a, send_b, meta, cotangent, first, last, weight, encoder, kernels)
    return out[:8]


def middle_kernel(
    channels, meta, turned, gain, wide_in, back_in, encoded_in,
    normed, first, last, d_spread, parts,
    encoded, spread, wide, back, flipped, gain_sum,
    pair_sems, local,
):
    rows, cols, width = normed.shape
    sources = SIDE * SIDE
    block = turned.shape[2]

    def load_encoded(n):
        return pltpu.make_async_copy(encoded_in.at[n], encoded.at[n], pair_sems.at[n])

    load_back = pltpu.make_async_copy(back_in, back, local.at[0])
    load_wide = pltpu.make_async_copy(wide_in, wide, local.at[1])
    for n in range(sources):
        load_encoded(n).start()
    load_back.start()
    load_wide.start()
    spread[...] = jnp.zeros_like(spread)

    @pl.loop(0, sources)
    def _(n):
        load_encoded(n).wait()
        for rank in range(MOST):
            which, patch = meta[n, rank], meta[n, MOST + rank]

            @pl.when(which >= 0)
            def _():
                spread[patch] += dot(turned[which], encoded[n, :, rank * block : (rank + 1) * block], 1, 1)

    load_back.wait()
    gain_sum[...] = jnp.zeros_like(gain_sum)
    across = cols // PW

    @pl.loop(0, spread.shape[0])
    def _(q):
        at = (pl.ds(q // across * PH, PH), pl.ds(pl.multiple_of(q % across * PW, PW), PW))
        value = spread[q]
        scale = lax.rsqrt(jnp.mean(value * value, axis=1, keepdims=True) + 1e-06)
        unit = value * scale
        weight = gain[...]
        normed[at] = (unit * weight).astype(jnp.bfloat16).reshape(PH, PW, width)
        given = back[at].reshape(PH * PW, width)
        product = given * unit
        gain_sum[...] += jnp.sum(product.reshape(PH * PW // 8, 8, width), axis=0)
        inner = jnp.mean(product * weight, axis=1, keepdims=True)
        d_spread[q] = (scale * (given * weight - unit * inner)).astype(jnp.bfloat16).T

    step_rows = 4

    @pl.loop(0, rows // step_rows)
    def _(n):
        some = normed[pl.ds(n * step_rows, step_rows)].reshape(step_rows * cols, width)
        flipped[:, pl.ds(pl.multiple_of(n * step_rows * cols, 128), step_rows * cols)] = some.T

    @pl.loop(0, rows)
    def _(row):
        some = normed[row].astype(jnp.float32)
        first[row] = some[:1]
        last[row] = some[cols - 1 :]

    load_wide.wait()
    for a in range(3):

        @pl.loop(0, 3 * width // 256)
        def _(j):
            window = wide[2 - a : 2 - a + rows, :, pl.ds(pl.multiple_of(j * 256, 256), 256)]
            got = dot(flipped[...], window.reshape(rows * cols, 256), 1, 0).astype(jnp.bfloat16)
            base = pl.multiple_of((a * (3 * width // 128) + 2 * j) * width, width)
            parts[pl.ds(base, width)] = got[:, :128]
            parts[pl.ds(pl.multiple_of(base + width, width), width)] = got[:, 128:]

    base = 9 * width * width // 128 + channels * width // 128
    for n in range(width // 128):
        parts[base + n * 8 : base + (n + 1) * 8] = gain_sum[:, n * 128 : (n + 1) * 128].astype(jnp.bfloat16)
    base += 8 * width // 128
    parts[base:] = jnp.zeros((parts.shape[0] - base, 128), jnp.bfloat16)


def middle(meta, turned, gain, wide, back, encoded, channels, part_rows):
    rows, cols, width = back.shape
    cells, block = turned.shape[1:]
    patches = rows * cols // cells
    sources = SIDE * SIDE
    bf, f32 = jnp.bfloat16, jnp.float32
    anywhere = pl.BlockSpec(memory_space=pl.ANY)
    local = pl.BlockSpec(memory_space=pltpu.VMEM)
    column = jax.ShapeDtypeStruct((rows, 1, width), f32)
    return pl.pallas_call(
        lambda *refs: middle_kernel(channels, *refs),
        name="middle",
        out_shape=(
            jax.ShapeDtypeStruct((rows, cols, width), bf), column, column,
            jax.ShapeDtypeStruct((patches, width, cells), bf), jax.ShapeDtypeStruct((part_rows, 128), bf),
        ),
        in_specs=[pl.BlockSpec(memory_space=pltpu.SMEM)] + [local] * 2 + [anywhere] * 3,
        out_specs=(local,) * 5,
        scratch_shapes=[
            pltpu.VMEM((sources, width, MOST * block), bf),
            pltpu.VMEM((patches, cells, width), f32),
            pltpu.VMEM(wide.shape, bf),
            pltpu.VMEM(back.shape, f32),
            pltpu.VMEM((width, rows * cols), bf),
            pltpu.VMEM((8, width), f32),
            pltpu.SemaphoreType.DMA((sources,)),
            pltpu.SemaphoreType.DMA((2,)),
        ],
        compiler_params=pltpu.CompilerParams(vmem_limit_bytes=VMEM_LIMIT),
    )(meta, turned, gain, wide, back, encoded)


PIECES = 16
PIECE_ROWS = 112
FLOWS = 6
EARLY, LATE = (0, 1, 2, 3), (4, 5)
HALVED = 12


def pairing(place, parity):
    near, far = place + 1 - 2 * (place % 2), (place + 3 - 2 * (place % 2)) % SIDE
    turn, high, low = (place + 1) // 2 % 2, place // 2, place % 2
    return ((near, turn), (far, high)) if parity == 0 else ((far, high), (near, low))


def sum_kernel(
    meta, parts, normed, first, last, weight, own_a, own_b, got_a, got_b, slope_in, turned_in, d_spread_in,
    conv_out, summed,
    own, late, other, total, outgoing, incoming, quarter_out, quarter_in, shared, result,
    tile, wide, held_weight, made, above, below, lefts, rights, observed, slope, turned, d_spread, d_rows, encoder_sum,
    halo_send, halo_recv, sends, recvs, local, x_sems, slope_sems,
):
    lat, lon, y, z = position()
    x, core = lat // 2, lat % 2
    twin = (lat + 1 - 2 * core, lon)
    rows, cols, width = tile.shape
    _, _, up, down, left, right = halo_peers()

    def at_place(axis, place):
        if axis == 0:
            return (place * 2 + core, lon)
        return (lat, place * SIDE + z) if axis == 1 else (lat, y * SIDE + place)

    barrier = pltpu.get_barrier_semaphore()
    peers = [twin]
    for axis, place in enumerate((x, y, z)):
        peers += [at_place(axis, (place + step) % SIDE) for step in range(1, SIDE)]
    peers += [(lat, left), (lat, right)]
    peers += [(a, b) for a in (up, down) for b in (left, lon, right)]
    for peer in peers:
        pl.semaphore_signal(barrier, inc=1, device_id=peer, device_id_type=MESH)
    load_own = [pltpu.make_async_copy(parts.at[core, f], own.at[f], local.at[f]) for f in EARLY]
    load_late = [
        pltpu.make_async_copy(parts.at[:, f], late.at[:, f - LATE[0]], local.at[f]) for f in LATE
    ]
    load_turned = pltpu.make_async_copy(turned_in, turned, local.at[FLOWS + 4])
    load_spread = pltpu.make_async_copy(d_spread_in, d_spread, local.at[FLOWS + 5])
    channels, high, block = observed.shape[1], own_a.shape[3], own_a.shape[4]

    def fetch(n, rank, from_a, from_b):
        lanes = pl.ds(rank * block, block)
        return (
            pltpu.make_async_copy(from_a.at[rank], observed.at[n, pl.ds(0, high), lanes], x_sems.at[n, rank, 0]),
            pltpu.make_async_copy(
                from_b.at[rank], observed.at[n, pl.ds(high, channels - high), lanes], x_sems.at[n, rank, 1]
            ),
        )

    def load_slope(n):
        return pltpu.make_async_copy(slope_in.at[n], slope.at[n], slope_sems.at[n])
    load_tile = pltpu.make_async_copy(normed, tile, local.at[FLOWS])
    load_weight = pltpu.make_async_copy(weight, held_weight, local.at[FLOWS + 1])
    for copy in (load_turned, load_spread, *load_own):
        copy.start()
    for n, (dy, dz) in enumerate(SOURCES):
        from_a = own_a.at[z, y] if n == 0 else got_a.at[dy, dz]
        from_b = own_b.at[y, z] if n == 0 else got_b.at[dz, dy]
        for rank in range(MOST):
            for copy in fetch(n, rank, from_a, from_b):
                copy.start()
        load_slope(n).start()
    for copy in (*load_late, load_tile, load_weight):
        copy.start()
    pl.semaphore_wait(barrier, len(peers))

    halo = halo_copies(
        normed.at[0], normed.at[rows - 1], first, last, above, below, lefts, rights, halo_send, halo_recv
    )
    for copy in halo:
        copy.start()

    begun = []

    def remote(src, dst, flow, n, to):
        copy = pltpu.make_async_remote_copy(
            src_ref=src, dst_ref=dst, send_sem=sends.at[flow, n], recv_sem=recvs.at[flow, n],
            device_id=to, device_id_type=MESH,
        )
        copy.start()
        begun.append(copy)
        return copy

    places = (x, y, z)
    plans = []
    for f in range(FLOWS):
        turn, parity = f // 2, f % 2
        steps, base = [], 0
        for k, (partner, keep) in enumerate(pairing(places[turn], parity)):
            size = PIECES >> (k + 1)
            kept, sent = base + keep * size, base + (1 - keep) * size
            base = kept
            steps.append((at_place(turn, partner), size, kept, sent))
        plans.append((steps, (turn + 1) % 3, (turn + 2) % 3))

    crossing = {f: remote(parts.at[1 - core, f], other.at[f], f, 0, twin) for f in EARLY}
    encoder_sum[...] = jnp.zeros_like(encoder_sum)
    load_turned.wait()
    load_spread.wait()

    def backward(low, high_end):
        @pl.loop(low, high_end)
        def _(n):
            for rank in range(MOST):
                for copy in fetch(n, rank, got_a.at[0, 0], got_b.at[0, 0]):
                    copy.wait()
            load_slope(n).wait()
            for rank in range(MOST):
                which, patch = jnp.maximum(meta[n, rank], 0), meta[n, MOST + rank]
                lanes = slice(rank * block, (rank + 1) * block)
                here = dot(d_spread[patch], turned[which], 1, 0).astype(jnp.bfloat16).astype(jnp.float32)
                d_rows[:, lanes] = (here * slope[n, :, lanes]).astype(jnp.bfloat16)
            encoder_sum[...] += dot(observed[n], d_rows[...], 1, 1)

    def place_encoder():
        flow_rows = PIECES * PIECE_ROWS
        begin = 9 * width * width // 128 - (FLOWS + LATE[0]) * flow_rows
        for n in range(width // 128):
            done = 0
            while done < channels:
                at = begin + n * channels + done
                flow, piece, row = at // flow_rows, at % flow_rows // PIECE_ROWS, at % PIECE_ROWS
                size = min(PIECE_ROWS - row, channels - done)
                some = encoder_sum[done : done + size, n * 128 : (n + 1) * 128]
                late[1, flow, piece, row : row + size] = some.astype(jnp.bfloat16)
                done += size

    step_rows = 4
    save = [pltpu.make_async_copy(made, conv_out, local.at[FLOWS + 2])]

    def convolve(chunk):
        value = jnp.zeros((step_rows * cols, width), jnp.float32)
        for a in range(3):
            window = wide[chunk * step_rows + a : chunk * step_rows + a + step_rows]
            value += dot(window.reshape(step_rows * cols, 3 * width), held_weight[a], 1, 0)
        made[chunk * step_rows : (chunk + 1) * step_rows] = value.astype(jnp.bfloat16).reshape(step_rows, cols, width)

    def halve(f, k):
        to, size, _, _ = plans[f][0][k]
        at = pl.ds((0, PIECES // 2)[k], size)
        return remote(outgoing.at[f, at], incoming.at[f, at], f, 1 + k, to)

    flying, passed = {}, []

    def pass_on(f, start, size, n):
        at = result.at[core, f, pl.ds(start, size)]
        passed.append(remote(at, at, f, n, twin))

    def half(f):
        _, size, kept, sent = plans[f][0][0]
        crossing[f].wait_recv()
        if f in EARLY:
            load_own[f].wait()

        def mine(i):
            return (own[f, i] if f in EARLY else late[core, f - LATE[0], i]).astype(jnp.float32)

        @pl.loop(0, size)
        def _(i):
            total[f, kept + i] = mine(kept + i) + other[f, kept + i].astype(jnp.float32)
            value = mine(sent + i) + other[f, sent + i].astype(jnp.float32)
            outgoing[f, i] = value.astype(jnp.bfloat16)

        flying[f] = halve(f, 0)

    def quarter(f):
        _, _, kept, _ = plans[f][0][0]
        _, size, keep_next, send_next = plans[f][0][1]
        flying[f].wait_recv()

        @pl.loop(0, size)
        def _(i):
            total[f, keep_next + i] += incoming[f, keep_next - kept + i].astype(jnp.float32)
            value = total[f, send_next + i] + incoming[f, send_next - kept + i].astype(jnp.float32)
            outgoing[f, PIECES // 2 + i] = value.astype(jnp.bfloat16)

        flying[f] = halve(f, 1)

    def second(f):
        steps, axis, _ = plans[f]
        base = steps[1][2]
        flying[f].wait_recv()
        flying[f] = []
        for step in range(1, SIDE):
            place = (places[axis] + step) % SIDE
            value = total[f, base + place] + incoming[f, PIECES // 2 + place].astype(jnp.float32)
            quarter_out[f, step - 1] = value.astype(jnp.bfloat16)
            flying[f].append(
                remote(quarter_out.at[f, step - 1], quarter_in.at[f, step - 1], f, 2 + step, at_place(axis, place))
            )

    def third(f):
        steps, axis, other_axis = plans[f]
        here, there = places[axis], places[other_axis]
        value = total[f, steps[1][2] + here] + incoming[f, PIECES // 2 + here].astype(jnp.float32)
        for step in range(1, SIDE):
            flying[f][step - 1].wait_recv()
            value += quarter_in[f, step - 1].astype(jnp.float32)
        shared[f, there] = value.astype(jnp.bfloat16)
        flying[f] = [
            remote(shared.at[f, there], shared.at[f, there], f, 5 + step, at_place(other_axis, (there + step) % SIDE))
            for step in range(1, SIDE)
        ]

    def settle(f):
        steps, axis, _ = plans[f]
        mine = steps[1][2] + places[axis]
        for copy in flying[f]:
            copy.wait_recv()
        value = shared[f, 0].astype(jnp.float32)
        for place in range(1, SIDE):
            value += shared[f, place].astype(jnp.float32)
        result[core, f, mine] = value.astype(jnp.bfloat16)
        at = result.at[core, f, mine]
        flying[f] = [
            remote(at, at, f, 8 + step, at_place(axis, (places[axis] + step) % SIDE)) for step in range(1, SIDE)
        ]

    def spread_out(f, k):
        to, size, kept, _ = plans[f][0][k]
        for copy in flying[f]:
            copy.wait_recv()
        at = result.at[core, f, pl.ds(kept, size)]
        flying[f] = [remote(at, at, f, 13 - k, to)]
        if k == 1:
            pass_on(f, kept, size, 14)
        else:
            pass_on(f, plans[f][0][1][3], plans[f][0][1][1], 15)

    def close(f):
        _, size, _, sent = plans[f][0][0]
        flying[f][0].wait_recv()
        pass_on(f, sent, size, 16)

    def each(group, act, *rest):
        for f in group:
            act(f, *rest)

    sources = len(SOURCES)
    backward(0, sources * 3 // 8)
    each(EARLY, half)
    backward(sources * 3 // 8, sources)
    for copy in load_late:
        copy.wait()
    place_encoder()
    for f in LATE:
        crossing[f] = remote(late.at[1 - core, f - LATE[0]], other.at[f], f, 0, twin)
    each(EARLY, quarter)
    load_tile.wait()
    for copy in halo:
        copy.wait()
    lay_windows(tile, above, below, lefts, rights, wide, False)
    load_weight.wait()
    each(LATE, half)
    each(EARLY, second)
    convolve(0)
    each(LATE, quarter)
    convolve(1)
    each(EARLY, third)
    convolve(2)
    each(LATE, second)
    convolve(3)
    each(EARLY, settle)
    each(LATE, third)
    convolve(4)
    each(EARLY, spread_out, 1)
    each(LATE, settle)
    convolve(5)
    save[0].start()
    each(EARLY, spread_out, 0)
    each(LATE, spread_out, 1)
    each(LATE, spread_out, 0)
    each(EARLY, close)
    each(LATE, close)
    for copy in passed:
        copy.wait_recv()
    stored = pltpu.make_async_copy(result, summed, local.at[FLOWS + 3])
    stored.start()
    for copy in begun:
        copy.wait_send()
    save[0].wait()
    stored.wait()


def sum_all(meta, parts, normed, first, last, weight, own_a, own_b, got_a, got_b, slope, turned, d_spread, channels):
    rows, cols, width = normed.shape
    bf, f32 = jnp.bfloat16, jnp.float32
    anywhere = pl.BlockSpec(memory_space=pl.ANY)
    inside = pl.BlockSpec(memory_space=pltpu.VMEM)
    piece = (PIECE_ROWS, 128)
    parts = parts.reshape((2, FLOWS, PIECES) + piece)
    sources = len(SOURCES)
    return pl.pallas_call(
        sum_kernel,
        name="sum_all",
        out_shape=(jax.ShapeDtypeStruct(normed.shape, bf), jax.ShapeDtypeStruct(parts.shape, bf)),
        in_specs=[pl.BlockSpec(memory_space=pltpu.SMEM), anywhere, anywhere, inside, inside] + [anywhere] * 8,
        out_specs=(anywhere, anywhere),
        scratch_shapes=[
            pltpu.VMEM((len(EARLY), PIECES) + piece, bf),
            pltpu.VMEM((2, len(LATE), PIECES) + piece, bf),
            pltpu.VMEM((FLOWS, PIECES) + piece, bf),
            pltpu.VMEM((FLOWS, PIECES) + piece, f32),
            pltpu.VMEM((FLOWS, HALVED) + piece, bf),
            pltpu.VMEM((FLOWS, HALVED) + piece, bf),
            pltpu.VMEM((FLOWS, SIDE - 1) + piece, bf),
            pltpu.VMEM((FLOWS, SIDE - 1) + piece, bf),
            pltpu.VMEM((FLOWS, SIDE) + piece, bf),
            pltpu.VMEM((2, FLOWS, PIECES) + piece, bf),
            pltpu.VMEM((rows, cols, width), bf),
            pltpu.VMEM((rows + 2, cols, 3 * width), bf),
            pltpu.VMEM(weight.shape, bf),
            pltpu.VMEM((rows, cols, width), bf),
            pltpu.VMEM((cols, width), bf),
            pltpu.VMEM((cols, width), bf),
            pltpu.VMEM((rows + 2, 1, width), f32),
            pltpu.VMEM((rows + 2, 1, width), f32),
            pltpu.VMEM((sources, channels, slope.shape[2]), bf),
            pltpu.VMEM(slope.shape, f32),
            pltpu.VMEM(turned.shape, bf),
            pltpu.VMEM(d_spread.shape, bf),
            pltpu.VMEM(slope.shape[1:], bf),
            pltpu.VMEM((channels, width), f32),
            pltpu.SemaphoreType.DMA((8,)),
            pltpu.SemaphoreType.DMA((8,)),
            pltpu.SemaphoreType.DMA((FLOWS, 17)),
            pltpu.SemaphoreType.DMA((FLOWS, 17)),
            pltpu.SemaphoreType.DMA((FLOWS + 6,)),
            pltpu.SemaphoreType.DMA((sources, MOST, 2)),
            pltpu.SemaphoreType.DMA((sources,)),
        ],
        compiler_params=pltpu.CompilerParams(
            collective_id=1, has_side_effects=True, vmem_limit_bytes=VMEM_LIMIT
        ),
    )(meta, parts, normed, first, last, weight, own_a, own_b, got_a, got_b, slope, turned, d_spread)


def finish_kernel(scale, summed, conv_grad, encoder_grad, gain_grad, held, taps, encoder, sems):
    count, width = taps.shape[0], taps.shape[2]
    lanes = width // 128
    channels = encoder.shape[0]
    size = lanes * width
    base = count * size
    rest = channels * lanes + 8 * lanes

    def load(tap):
        at = pl.ds(pl.multiple_of(tap * size, size), size)
        return pltpu.make_async_copy(summed.at[at], held.at[at], sems.at[0, tap])

    def save(tap):
        return pltpu.make_async_copy(taps.at[tap], conv_grad.at[tap], sems.at[1, tap])

    last = pl.ds(base, rest)
    load_rest = pltpu.make_async_copy(summed.at[last], held.at[last], sems.at[0, count])
    for tap in range(count):
        load(tap).start()
    load_rest.start()

    @pl.loop(0, count)
    def _(tap):
        load(tap).wait()
        for n in range(lanes):
            at = pl.ds(pl.multiple_of(tap * size + n * width, width), width)
            taps[tap, :, n * 128 : (n + 1) * 128] = held[at].astype(jnp.float32) * scale
        save(tap).start()

    load_rest.wait()
    for n in range(lanes):
        at = slice(n * 128, (n + 1) * 128)
        encoder[:, at] = held[base + n * channels : base + (n + 1) * channels].astype(jnp.float32) * scale
        start = base + channels * lanes + n * 8
        gain_grad[:, at] = jnp.sum(held[start : start + 8].astype(jnp.float32), axis=0, keepdims=True) * scale
    save_encoder = pltpu.make_async_copy(encoder, encoder_grad, sems.at[1, count])
    save_encoder.start()

    @pl.loop(0, count)
    def _(tap):
        save(tap).wait()

    save_encoder.wait()


def finish(summed, scale, channels, width):
    f32 = jnp.float32
    anywhere = pl.BlockSpec(memory_space=pl.ANY)
    return pl.pallas_call(
        lambda *refs: finish_kernel(scale, *refs),
        name="finish",
        out_shape=(
            jax.ShapeDtypeStruct((9, width, width), f32),
            jax.ShapeDtypeStruct((channels, width), f32),
            jax.ShapeDtypeStruct((1, width), f32),
        ),
        in_specs=[anywhere],
        out_specs=(anywhere, anywhere, pl.BlockSpec(memory_space=pltpu.VMEM)),
        scratch_shapes=[
            pltpu.VMEM(summed.shape, jnp.bfloat16),
            pltpu.VMEM((9, width, width), f32),
            pltpu.VMEM((channels, width), f32),
            pltpu.SemaphoreType.DMA((2, 10)),
        ],
        compiler_params=pltpu.CompilerParams(vmem_limit_bytes=VMEM_LIMIT),
    )(summed)


def shards(spectra, target, patch, kernel, encoder_weight, kernels, gain, conv_weight, cotangent):
    tiles, bands = lax.axis_size("lon"), lax.axis_size("lat")
    rows, cols, width = cotangent.shape
    channels = spectra.shape[1]
    loss_scale = 1.0 / math.sqrt(rows * bands * cols * tiles)
    send_a, send_b, meta, first, last = pack(target, patch, kernel, spectra.T, cotangent, kernels.shape[1], tiles)
    meta = meta.reshape(tiles, 1, 128)
    weight = conv_weight.reshape(9, width, width)
    got_a, got_b, got_meta, wide, back, encoded, slope, turned = exchange(
        send_a, send_b, meta, cotangent, first, last, weight, encoder_weight, kernels
    )
    part_rows = 192 * 112
    got_meta = got_meta.reshape(tiles, 128)
    normed, first, last, d_spread, parts = middle(
        got_meta, turned, gain.reshape(1, width), wide, back, encoded, channels, part_rows
    )
    conv_out, summed = sum_all(
        got_meta, parts, normed, first, last, conv_weight.reshape(3, 3 * width, width), send_a, send_b, got_a, got_b,
        slope, turned, d_spread, channels,
    )
    conv_grad, encoder_grad, gain_grad = finish(summed.reshape(part_rows, 128), loss_scale, channels, width)
    return conv_out, conv_grad.reshape(3, 3, width, width), encoder_grad, gain_grad.reshape(width)


def solution(mesh):
    placed = (
        P(("lat", "lon"), None),
        P(("lat", "lon")),
        P(("lat", "lon")),
        P(("lat", "lon")),
        P(),
        P(),
        P(),
        P(),
        P("lat", "lon", None),
    )
    return jax.shard_map(
        shards,
        mesh=mesh,
        in_specs=placed,
        out_specs=(P("lat", "lon", None), P(), P(), P()),
        check_vma=False,
    )
```
